32 devices in a mesh: section: 2 (over y), pen: 8 (over z, x), slab: 2 (over core).
Axes of the slice: x: 2, y: 2, z: 4, core: 2. Of those that a mesh axis runs over, the one named last changes fastest.
Arguments:
- velocity: float32 [3, 48, 48, 48], P(None, ('section', 'pen'), 'slab'), may hold values from -6 to 6
- vorticity: float32 [3, 48, 48, 48], P(None, ('section', 'pen'), 'slab'), may hold values from -6 to 6
- velocity_modes: float32 [3, 32, 32, 2, 32], P(None, None, ('section', 'pen'), None, 'slab'), may hold values from -6 to 6
Outputs:
- rhs_modes: float32 [3, 32, 32, 2, 32], P(None, None, ('section', 'pen'), None, 'slab')
The draws below stay inside these ranges and needn't reach their ends.
All inputs are finite; a program needn't handle non-finite values.
Results may differ from the reference program's by a relative error of at most 0.000057.
Values sent between devices are 32-bit elements; how exact they have to be, the bound alone decides.
A program may use at most 64 MiB of HBM per device.

```python
import jax
import jax.numpy as jnp
from jax import lax

N = 48
KEEP = 32


def block_levels(stream_key, shape, split, low, top_value):
    def one(position, blocks):
        steps = jax.random.uniform(jax.random.fold_in(jax.random.fold_in(stream_key, 6), position), (blocks,), jnp.float32, low / len(split), top_value / len(split))
        return jnp.repeat(jnp.exp(steps), shape[position] // blocks).reshape((-1,) + (1,) * (len(shape) - position - 1))

    loudness = one(*split[0])
    for cut in split[1:]:
        loudness = loudness * one(*cut)
    return loudness


def centred(stream_key, shape, deviation, most, split=(), kind=jnp.bfloat16):
    drawn = deviation * jax.random.normal(stream_key, shape, jnp.float32)
    if split:
        drawn = drawn * block_levels(stream_key, shape, split, -0.22, 0.18)
    return jnp.clip(drawn, -most, most).astype(kind)


def setup_inputs(seed: int = 0) -> dict:
    streams_of = jax.random.split(jax.random.key(seed), 4)
    return {
        "velocity": centred(streams_of[0], (3, N, N, N), 1.0, 6.0, ((1, 16), (2, 2)), jnp.float32),
        "vorticity": centred(streams_of[1], (3, N, N, N), 1.0, 6.0, ((1, 16), (2, 2)), jnp.float32),
        "velocity_modes": centred(streams_of[2], (3, KEEP, KEEP, 2, KEEP), 1.0, 6.0, ((2, 16), (4, 2)), jnp.float32),
    }


def signed_modes(index, count):
    return jnp.where(index < count // 2, index, index - count)


def reference(velocity, vorticity, velocity_modes):
    velocity_field = velocity
    vorticity_field = vorticity
    cross_product = jnp.stack([velocity_field[1] * vorticity_field[2] - velocity_field[2] * vorticity_field[1],
                         velocity_field[2] * vorticity_field[0] - velocity_field[0] * vorticity_field[2],
                         velocity_field[0] * vorticity_field[1] - velocity_field[1] * vorticity_field[0]])
    picked = jnp.concatenate([jnp.arange(KEEP // 2, dtype=jnp.int32),
                              jnp.arange(N - KEEP // 2, N, dtype=jnp.int32)])

    def transform(field):
        spec = jnp.fft.fft(field, axis=2, norm="ortho")[:, :, picked]
        spec = jnp.fft.fft(spec, axis=1, norm="ortho")[:, picked, :]
        spec = jnp.fft.fft(spec, axis=0, norm="ortho")[picked]
        return jnp.stack([jnp.real(spec), jnp.imag(spec)])

    spectrum = lax.map(transform, cross_product)
    modes = signed_modes(jnp.arange(KEEP, dtype=jnp.int32), KEEP)
    kz = modes[:, None, None]
    ky = modes[None, :, None]
    kx = modes[None, None, :]
    limit = -(KEEP // 2)
    mask = ((kx != limit) & (ky != limit) & (kz != limit)).astype(jnp.float32)
    waves = (kx.astype(jnp.float32), ky.astype(jnp.float32), kz.astype(jnp.float32))
    ksq = waves[0] * waves[0] + waves[1] * waves[1] + waves[2] * waves[2]
    denom = jnp.maximum(ksq, 1.0)
    parts = []
    for which in range(2):
        comp = [spectrum[c, which] for c in range(3)]
        inner = (waves[0] * comp[0] + waves[1] * comp[1] + waves[2] * comp[2]) / denom
        parts.append(jnp.stack([comp[c] - waves[c] * inner for c in range(3)]))
    projected = jnp.stack(parts, axis=3)
    visc = 0.5 / (KEEP // 2) ** 2
    return projected * mask[None, :, :, None, :] - visc * ksq[None, :, :, None, :] * velocity_modes
```

```python
import functools
import math

import jax
import jax.numpy as jnp
import numpy as np
from jax import lax
from jax.experimental import pallas as pl
from jax.experimental.pallas import tpu as pltpu
from jax.sharding import PartitionSpec as P

AXES = ("section", "pen", "slab")
highest = lax.Precision.HIGHEST


def signed_modes(index, count):
    return jnp.where(index < count // 2, index, index - count)


def discrete_fourier_tables(length, keep_count):
    modes = signed_modes(jnp.arange(keep_count, dtype=jnp.int32), keep_count)
    mode_positions = jnp.arange(length, dtype=jnp.int32)
    phase = jnp.remainder(modes[:, None] * mode_positions[None, :], length).astype(jnp.float32)
    angles = 2.0 * math.pi / length * phase
    factor = 1.0 / math.sqrt(length)
    return (jnp.cos(angles) * factor, jnp.sin(angles) * factor)


def complex_apply(form, cosine, sine, real_part, imag_part):
    out_real = jnp.einsum(form, cosine, real_part, precision=highest) + jnp.einsum(
        form, sine, imag_part, precision=highest
    )
    out_imag = jnp.einsum(form, cosine, imag_part, precision=highest) - jnp.einsum(
        form, sine, real_part, precision=highest
    )
    return (out_real, out_imag)


def per_device(velocity, vorticity, velocity_modes):
    grid_cells = velocity.shape[3]
    keep_count = velocity_modes.shape[1]
    cross_product = jnp.stack(
        [
            velocity[1] * vorticity[2] - velocity[2] * vorticity[1],
            velocity[2] * vorticity[0] - velocity[0] * vorticity[2],
            velocity[0] * vorticity[1] - velocity[1] * vorticity[0],
        ]
    )
    slabs = lax.axis_size("slab")
    block_modes = keep_count // slabs
    cosine_table, sine_table = discrete_fourier_tables(grid_cells, keep_count)
    cols_real = cosine_table.T.reshape(grid_cells, slabs, block_modes)
    cols_imag = (-sine_table).T.reshape(grid_cells, slabs, block_modes)
    column_table = jnp.stack([cols_real, cols_imag], axis=2).reshape(grid_cells, 2 * keep_count)
    first_pass = jnp.einsum("czyx,xj->czyj", cross_product, column_table, precision=highest)
    block = lax.all_to_all(first_pass, "slab", split_axis=3, concat_axis=2, tiled=True)
    out_real, out_imag = complex_apply(
        "ky,czyj->czkj",
        cosine_table,
        sine_table,
        block[..., :block_modes],
        block[..., block_modes:],
    )
    second_pass = jnp.concatenate([out_real, out_imag], axis=-1)
    halves = lax.axis_size("section")
    pens = lax.axis_size("pen")
    rows_ky = keep_count // (halves * pens)
    block = lax.all_to_all(second_pass, ("section", "pen"), split_axis=2, concat_axis=1, tiled=True)
    out_real, out_imag = complex_apply(
        "kz,czyj->ckyj",
        cosine_table,
        sine_table,
        block[..., :block_modes],
        block[..., block_modes:],
    )
    third_pass = jnp.concatenate([out_real, out_imag], axis=-1)
    group_index = lax.axis_index("section") * pens + lax.axis_index("pen")
    modes_z = signed_modes(jnp.arange(keep_count, dtype=jnp.int32), keep_count)[:, None, None]
    modes_y = signed_modes(
        group_index * rows_ky + jnp.arange(rows_ky, dtype=jnp.int32), keep_count
    )[None, :, None]
    modes_x = signed_modes(
        lax.axis_index("slab") * block_modes + jnp.arange(block_modes, dtype=jnp.int32), keep_count
    )[None, None, :]
    limit = -(keep_count // 2)
    keep_mask = ((modes_x != limit) & (modes_y != limit) & (modes_z != limit)).astype(jnp.float32)
    waves = (modes_x.astype(jnp.float32), modes_y.astype(jnp.float32), modes_z.astype(jnp.float32))
    ksq = waves[0] * waves[0] + waves[1] * waves[1] + waves[2] * waves[2]
    denom = jnp.maximum(ksq, 1.0)
    parts = []
    for which in range(2):
        chosen = third_pass[..., which * block_modes : (which + 1) * block_modes]
        comp = [chosen[c] for c in range(3)]
        inner = (waves[0] * comp[0] + waves[1] * comp[1] + waves[2] * comp[2]) / denom
        parts.append(jnp.stack([comp[c] - waves[c] * inner for c in range(3)]))
    projected = jnp.stack(parts, axis=3)
    visc = 0.5 / (keep_count // 2) ** 2
    return (
        projected * keep_mask[None, :, :, None, :]
        - visc * ksq[None, :, :, None, :] * velocity_modes
    )


def split_bf16(table):
    high = table.astype(jnp.bfloat16)
    low = (table - high.astype(np.float32)).astype(jnp.bfloat16)
    return high, low


def split_in_kernel(value):
    high = value.astype(jnp.bfloat16)
    low = (value - high.astype(jnp.float32)).astype(jnp.bfloat16)
    return high, low


def mm(a, b):
    return lax.dot_general(a, b, (((1,), (0,)), ((), ())), preferred_element_type=jnp.float32)


def split_dot(a, b):
    return mm(a[0], b[0]) + mm(a[1], b[0]) + mm(a[0], b[1])


def wave_numbers(count):
    index = np.arange(count)
    return np.where(index < count // 2, index, index - count)


def host_tables(cells, keep):
    phase = np.remainder(wave_numbers(keep)[:, None] * np.arange(cells)[None, :], cells)
    angles = 2.0 * np.pi / cells * phase
    factor = 1.0 / np.sqrt(cells)
    return np.cos(angles) * factor, np.sin(angles) * factor


class Plan:
    def __init__(self, mesh_shape, cells, keep, z_rows, y_rows):
        self.cells, self.keep, self.z_rows, self.y_rows = cells, keep, z_rows, y_rows
        self.halves, self.pens, self.slabs = (mesh_shape[a] for a in AXES)
        self.groups = self.halves * self.pens
        self.count = self.groups * self.slabs
        self.rows_ky = keep // self.groups
        self.block = keep // self.slabs
        self.width = self.rows_ky * self.block
        self.rows = 2 * z_rows
        self.wide = self.slabs * 128

    def fits(self):
        return (
            self.rows_ky * self.groups == self.keep
            and self.block * self.slabs == self.keep
            and 3 * self.width <= 128
            and 128 % self.width == 0
            and self.rows <= 8
            and self.cells <= 128
            and self.cells % 16 == 0
            and self.y_rows % 8 == 0
            and 6 * self.y_rows <= 256
            and self.groups % 8 == 0
            and self.keep % 8 == 0
            and self.block % 8 == 0
            and 3 * self.z_rows * self.y_rows <= 512
            and 2 <= self.count <= 64
        )

    def tables(self):
        cos, sin = host_tables(self.cells, self.keep)
        g, zl, yl, ky_n, bm = self.groups, self.z_rows, self.y_rows, self.rows_ky, self.block
        first = np.zeros((self.cells, 2, self.slabs, 128 // self.width, ky_n, bm), np.float32)
        for s in range(self.slabs):
            modes = slice(s * bm, (s + 1) * bm)
            first[:, 0, s, :3] = cos[modes].T[:, None, None]
            first[:, 1, s, :3] = -sin[modes].T[:, None, None]
        first = first.reshape(self.cells, 2 * self.wide)
        second = np.zeros((self.slabs, 2, ky_n, g, 2, yl), np.float32)
        for s in range(self.slabs):
            for k in range(ky_n):
                c = cos[k::ky_n, s * yl : (s + 1) * yl]
                n = sin[k::ky_n, s * yl : (s + 1) * yl]
                second[s, 0, k, :, 0], second[s, 0, k, :, 1] = c, n
                second[s, 1, k, :, 0], second[s, 1, k, :, 1] = -n, c
        second = second.reshape(self.slabs, 2 * self.keep, 2 * yl)
        third = np.zeros((2, self.keep, g, self.slabs, 8), np.float32)
        for z in range(zl):
            c, n = cos[:, z::zl][:, :, None], sin[:, z::zl][:, :, None]
            third[0, :, :, :, 2 * z], third[0, :, :, :, 2 * z + 1] = c, n
            third[1, :, :, :, 2 * z], third[1, :, :, :, 2 * z + 1] = -n, c
        third = third.reshape(2 * self.keep, self.count * 8)
        high, low = split_bf16(second)
        return (
            np.stack(split_bf16(first)),
            np.concatenate([high, high, low], axis=2),
            np.stack(split_bf16(third)),
        )


def kernel(
    plan, vel_hbm, vort_hbm, modes_hbm, first_hbm, second_hbm, third_hbm, out_ref,
    fields, modes, first, second, third, cross, send, recv,
    field_sem, table_sem, late_sem, send_sem, recv_sem,
):
    sec, pen, slab = (lax.axis_index(a) for a in AXES)
    group = sec * plan.pens + pen
    me = group * plan.slabs + slab
    cells, keep = plan.cells, plan.keep
    for i, source in enumerate((vel_hbm, vort_hbm)):
        for c in range(3):
            pltpu.make_async_copy(source.at[c], fields.at[i, c], field_sem).start()
    table_loads = [
        pltpu.make_async_copy(first_hbm.at[0], first.at[0, 0:cells], table_sem.at[0]),
        pltpu.make_async_copy(first_hbm.at[0], first.at[1, 0:cells], table_sem.at[1]),
        pltpu.make_async_copy(first_hbm.at[1], first.at[2, 0:cells], table_sem.at[2]),
        pltpu.make_async_copy(second_hbm.at[slab], second, table_sem.at[3]),
    ]
    late_loads = [
        pltpu.make_async_copy(third_hbm, third, late_sem.at[0]),
        pltpu.make_async_copy(modes_hbm, modes, late_sem.at[1]),
    ]
    for load in table_loads + late_loads:
        load.start()

    def spread(offset):
        a, b, c = offset
        return (
            lax.rem(sec + a, plan.halves),
            lax.rem(pen + b, plan.pens),
            lax.rem(slab + c, plan.slabs),
        )

    offsets = [
        (a, b, c)
        for b in sorted(range(plan.pens), key=lambda v: -min(v, plan.pens - v))
        for a in reversed(range(plan.halves))
        for c in reversed(range(plan.slabs))
    ]
    offsets.remove((0, 0, 0))
    barrier = pltpu.get_barrier_semaphore()
    for offset in offsets:
        pl.semaphore_signal(
            barrier, inc=1, device_id=spread(offset), device_id_type=pl.DeviceIdType.MESH
        )
    if plan.rows < 8:
        recv[:, plan.rows : 8] = jnp.zeros((plan.count, 8 - plan.rows, 128), jnp.float32)
    cross[...] = jnp.zeros_like(cross)
    if cells < 128:
        for i in range(3):
            first[i, cells:128] = jnp.zeros((128 - cells, first.shape[2]), jnp.bfloat16)

    pltpu.make_async_copy(fields, fields, field_sem).wait()
    zl, yl = plan.z_rows, plan.y_rows
    area = zl * yl
    v, w = ([fields[i, c].reshape(area, cells) for c in range(3)] for i in range(2))
    for c in range(3):
        p, q = (c + 1) % 3, (c + 2) % 3
        cross[c * area : (c + 1) * area, 0:cells] = v[p] * w[q] - v[q] * w[p]
    for load in table_loads:
        load.wait()
    high, low = split_in_kernel(cross[...])
    along_x = mm(
        jnp.concatenate([high, low], axis=1), jnp.concatenate([first[0], first[1]], axis=0)
    ) + mm(high, first[2])
    slot = lax.broadcasted_iota(jnp.int32, (area, 2 * plan.wide), 1) % 128 // plan.width
    along_x = [along_x[c * area : (c + 1) * area] for c in range(3)]
    along_x = jnp.where(slot == 0, along_x[0], jnp.where(slot == 1, along_x[1], along_x[2]))
    high = along_x.astype(jnp.bfloat16).astype(jnp.float32)
    low = along_x - high
    upper = lax.broadcasted_iota(jnp.int32, (plan.groups, plan.wide), 1) % plan.width // plan.block
    for z in range(zl):
        parts = []
        for part in (high, low):
            piece = part[z * yl : (z + 1) * yl]
            parts.append(
                jnp.concatenate([piece[:, : plan.wide], piece[:, plan.wide :]], axis=0)
            )
        stack = jnp.concatenate([parts[0], parts[1], parts[0]], axis=0).astype(jnp.bfloat16)
        planes = mm(second[...], stack)
        for k in range(2):
            total = None
            for i in range(plan.rows_ky):
                start = (k * plan.rows_ky + i) * plan.groups
                piece = planes[start : start + plan.groups]
                total = piece if total is None else jnp.where(upper == i, piece, total)
            for s in range(plan.slabs):
                send[s, :, 2 * z + k, :] = total[:, s * 128 : (s + 1) * 128]

    pl.semaphore_wait(barrier, plan.count - 1)
    used = pl.ds(0, plan.rows)
    for offset in offsets:
        to = spread(offset)
        pltpu.make_async_remote_copy(
            src_ref=send.at[to[2], to[0] * plan.pens + to[1], used],
            dst_ref=recv.at[me, used],
            send_sem=send_sem,
            recv_sem=recv_sem,
            device_id=to,
            device_id_type=pl.DeviceIdType.MESH,
        ).start()
    recv[me, 0 : plan.rows] = send[slab, group, 0 : plan.rows]

    bm, ky_n, width = plan.block, plan.rows_ky, plan.width

    def signed(index):
        return jnp.where(index < keep // 2, index, index - keep)

    row = lax.broadcasted_iota(jnp.int32, (width, keep), 0)
    kx = signed(row % bm + slab * bm)
    ky = signed(row // bm + group * ky_n)
    kz = signed(lax.broadcasted_iota(jnp.int32, (width, keep), 1))
    limit = -(keep // 2)
    mask = ((kx != limit) & (ky != limit) & (kz != limit)).astype(jnp.float32)
    waves = [k.astype(jnp.float32) for k in (kx, ky, kz)]
    ksq = waves[0] * waves[0] + waves[1] * waves[1] + waves[2] * waves[2]
    inverse = 1.0 / jnp.maximum(ksq, 1.0)
    damp = (0.5 / (keep // 2) ** 2) * ksq
    for load in late_loads:
        load.wait()
    damped = [
        [
            jnp.concatenate([modes[c, i, k] for i in range(ky_n)], axis=0) * damp
            for k in range(2)
        ]
        for c in range(3)
    ]

    arrived = recv.at[pl.ds(0, plan.count - 1), used]
    pltpu.make_async_copy(arrived, arrived, recv_sem).wait()
    got = split_in_kernel(recv[...].reshape(plan.count * 8, 128))
    out = split_dot((third[0], third[1]), got)
    for k in range(2):
        turned = jnp.transpose(out[k * keep : (k + 1) * keep])
        comp = [turned[c * width : (c + 1) * width] for c in range(3)]
        inner = (waves[0] * comp[0] + waves[1] * comp[1] + waves[2] * comp[2]) * inverse
        for c in range(3):
            result = (comp[c] - waves[c] * inner) * mask - damped[c][k]
            for i in range(ky_n):
                out_ref[c, i, k] = result[i * bm : (i + 1) * bm]
    pltpu.make_async_copy(arrived, arrived, send_sem).wait()


def direct(plan, tables, velocity, vorticity, velocity_modes):
    modes = jnp.transpose(velocity_modes, (0, 2, 3, 4, 1))
    first, second, third = tables
    hbm = pl.BlockSpec(memory_space=pltpu.HBM)
    out = pl.pallas_call(
        functools.partial(kernel, plan),
        out_shape=pltpu.VMEM(modes.shape, jnp.float32),
        in_specs=[hbm] * 6,
        out_specs=pl.BlockSpec(memory_space=pltpu.VMEM),
        scratch_shapes=[
            pltpu.VMEM((2,) + velocity.shape, jnp.float32),
            pltpu.VMEM(modes.shape, jnp.float32),
            pltpu.VMEM((3, 128, 2 * plan.wide), jnp.bfloat16),
            pltpu.VMEM(second.shape[1:], jnp.bfloat16),
            pltpu.VMEM(third.shape, jnp.bfloat16),
            pltpu.VMEM((3 * plan.z_rows * plan.y_rows, 128), jnp.float32),
            pltpu.VMEM((plan.slabs, plan.groups, 8, 128), jnp.float32),
            pltpu.VMEM((plan.count, 8, 128), jnp.float32),
            pltpu.SemaphoreType.DMA,
            pltpu.SemaphoreType.DMA((4,)),
            pltpu.SemaphoreType.DMA((2,)),
            pltpu.SemaphoreType.DMA,
            pltpu.SemaphoreType.DMA,
        ],
        compiler_params=pltpu.CompilerParams(collective_id=0, has_side_effects=True),
    )(velocity, vorticity, modes, first, second, third)
    return jnp.transpose(out, (0, 4, 1, 2, 3))


def solution(mesh):
    sizes = dict(mesh.shape)

    def run(velocity, vorticity, velocity_modes):
        _, z_rows, y_rows, cells = velocity.shape
        plan = Plan(sizes, cells, velocity_modes.shape[1], z_rows, y_rows)
        if not plan.fits():
            return per_device(velocity, vorticity, velocity_modes)
        return direct(plan, plan.tables(), velocity, vorticity, velocity_modes)

    return jax.shard_map(
        run,
        mesh=mesh,
        in_specs=(
            P(None, ("section", "pen"), "slab", None),
            P(None, ("section", "pen"), "slab", None),
            P(None, None, ("section", "pen"), None, "slab"),
        ),
        out_specs=P(None, None, ("section", "pen"), None, "slab"),
        check_vma=False,
    )
```

```python
import functools
import math

import jax
import jax.numpy as jnp
import numpy as np
from jax import lax
from jax.experimental import pallas as pl
from jax.experimental.pallas import tpu as pltpu
from jax.sharding import PartitionSpec as P

AXES = ("section", "pen", "slab")
highest = lax.Precision.HIGHEST


def signed_modes(index, count):
    return jnp.where(index < count // 2, index, index - count)


def discrete_fourier_tables(length, keep_count):
    modes = signed_modes(jnp.arange(keep_count, dtype=jnp.int32), keep_count)
    mode_positions = jnp.arange(length, dtype=jnp.int32)
    phase = jnp.remainder(modes[:, None] * mode_positions[None, :], length).astype(jnp.float32)
    angles = 2.0 * math.pi / length * phase
    factor = 1.0 / math.sqrt(length)
    return (jnp.cos(angles) * factor, jnp.sin(angles) * factor)


def complex_apply(form, cosine, sine, real_part, imag_part):
    out_real = jnp.einsum(form, cosine, real_part, precision=highest) + jnp.einsum(
        form, sine, imag_part, precision=highest
    )
    out_imag = jnp.einsum(form, cosine, imag_part, precision=highest) - jnp.einsum(
        form, sine, real_part, precision=highest
    )
    return (out_real, out_imag)


def per_device(velocity, vorticity, velocity_modes):
    grid_cells = velocity.shape[3]
    keep_count = velocity_modes.shape[1]
    cross_product = jnp.stack(
        [
            velocity[1] * vorticity[2] - velocity[2] * vorticity[1],
            velocity[2] * vorticity[0] - velocity[0] * vorticity[2],
            velocity[0] * vorticity[1] - velocity[1] * vorticity[0],
        ]
    )
    slabs = lax.axis_size("slab")
    block_modes = keep_count // slabs
    cosine_table, sine_table = discrete_fourier_tables(grid_cells, keep_count)
    cols_real = cosine_table.T.reshape(grid_cells, slabs, block_modes)
    cols_imag = (-sine_table).T.reshape(grid_cells, slabs, block_modes)
    column_table = jnp.stack([cols_real, cols_imag], axis=2).reshape(grid_cells, 2 * keep_count)
    first_pass = jnp.einsum("czyx,xj->czyj", cross_product, column_table, precision=highest)
    block = lax.all_to_all(first_pass, "slab", split_axis=3, concat_axis=2, tiled=True)
    out_real, out_imag = complex_apply(
        "ky,czyj->czkj",
        cosine_table,
        sine_table,
        block[..., :block_modes],
        block[..., block_modes:],
    )
    second_pass = jnp.concatenate([out_real, out_imag], axis=-1)
    halves = lax.axis_size("section")
    pens = lax.axis_size("pen")
    rows_ky = keep_count // (halves * pens)
    block = lax.all_to_all(second_pass, ("section", "pen"), split_axis=2, concat_axis=1, tiled=True)
    out_real, out_imag = complex_apply(
        "kz,czyj->ckyj",
        cosine_table,
        sine_table,
        block[..., :block_modes],
        block[..., block_modes:],
    )
    third_pass = jnp.concatenate([out_real, out_imag], axis=-1)
    group_index = lax.axis_index("section") * pens + lax.axis_index("pen")
    modes_z = signed_modes(jnp.arange(keep_count, dtype=jnp.int32), keep_count)[:, None, None]
    modes_y = signed_modes(
        group_index * rows_ky + jnp.arange(rows_ky, dtype=jnp.int32), keep_count
    )[None, :, None]
    modes_x = signed_modes(
        lax.axis_index("slab") * block_modes + jnp.arange(block_modes, dtype=jnp.int32), keep_count
    )[None, None, :]
    limit = -(keep_count // 2)
    keep_mask = ((modes_x != limit) & (modes_y != limit) & (modes_z != limit)).astype(jnp.float32)
    waves = (modes_x.astype(jnp.float32), modes_y.astype(jnp.float32), modes_z.astype(jnp.float32))
    ksq = waves[0] * waves[0] + waves[1] * waves[1] + waves[2] * waves[2]
    denom = jnp.maximum(ksq, 1.0)
    parts = []
    for which in range(2):
        chosen = third_pass[..., which * block_modes : (which + 1) * block_modes]
        comp = [chosen[c] for c in range(3)]
        inner = (waves[0] * comp[0] + waves[1] * comp[1] + waves[2] * comp[2]) / denom
        parts.append(jnp.stack([comp[c] - waves[c] * inner for c in range(3)]))
    projected = jnp.stack(parts, axis=3)
    visc = 0.5 / (keep_count // 2) ** 2
    return (
        projected * keep_mask[None, :, :, None, :]
        - visc * ksq[None, :, :, None, :] * velocity_modes
    )


def split_bf16(table):
    high = table.astype(jnp.bfloat16)
    low = (table - high.astype(np.float32)).astype(jnp.bfloat16)
    return high, low


def split_in_kernel(value):
    high = value.astype(jnp.bfloat16)
    low = (value - high.astype(jnp.float32)).astype(jnp.bfloat16)
    return high, low


def mm(a, b):
    return lax.dot_general(a, b, (((1,), (0,)), ((), ())), preferred_element_type=jnp.float32)


def split_dot(a, b):
    return mm(a[0], b[0]) + mm(a[1], b[0]) + mm(a[0], b[1])


def wave_numbers(count):
    index = np.arange(count)
    return np.where(index < count // 2, index, index - count)


def host_tables(cells, keep):
    phase = np.remainder(wave_numbers(keep)[:, None] * np.arange(cells)[None, :], cells)
    angles = 2.0 * np.pi / cells * phase
    factor = 1.0 / np.sqrt(cells)
    return np.cos(angles) * factor, np.sin(angles) * factor


def by_distance(devices):
    origin = getattr(devices.flat[0], "coords", ())

    def hops(index):
        return sum(abs(a - b) for a, b in zip(getattr(devices[index], "coords", ()), origin))

    return sorted(np.ndindex(devices.shape), key=lambda index: (hops(index), index))


class Plan:
    def __init__(self, mesh_shape, order, cells, keep, z_rows, y_rows):
        self.order = order
        self.cells, self.keep, self.z_rows, self.y_rows = cells, keep, z_rows, y_rows
        self.halves, self.pens, self.slabs = (mesh_shape[a] for a in AXES)
        self.groups = self.halves * self.pens
        self.count = self.groups * self.slabs
        self.rows_ky = keep // self.groups
        self.block = keep // self.slabs
        self.width = self.rows_ky * self.block
        self.rows = 2 * z_rows
        self.wide = self.slabs * 128

    def fits(self):
        return (
            self.rows_ky * self.groups == self.keep
            and self.block * self.slabs == self.keep
            and 3 * self.width <= 128
            and 128 % self.width == 0
            and self.rows <= 8
            and self.cells <= 128
            and self.cells % 16 == 0
            and self.y_rows % 8 == 0
            and 6 * self.y_rows <= 256
            and self.groups % 8 == 0
            and self.keep % 8 == 0
            and self.block % 8 == 0
            and 3 * self.z_rows * self.y_rows <= 512
            and 2 <= self.count <= 64
        )

    def tables(self):
        cos, sin = host_tables(self.cells, self.keep)
        g, zl, yl, ky_n, bm = self.groups, self.z_rows, self.y_rows, self.rows_ky, self.block
        first = np.zeros((self.cells, 2, self.slabs, 128 // self.width, ky_n, bm), np.float32)
        for s in range(self.slabs):
            modes = slice(s * bm, (s + 1) * bm)
            first[:, 0, s, :3] = cos[modes].T[:, None, None]
            first[:, 1, s, :3] = -sin[modes].T[:, None, None]
        first = first.reshape(self.cells, 2 * self.wide)
        second = np.zeros((self.slabs, 2, ky_n, g, 2, yl), np.float32)
        for s in range(self.slabs):
            for k in range(ky_n):
                c = cos[k::ky_n, s * yl : (s + 1) * yl]
                n = sin[k::ky_n, s * yl : (s + 1) * yl]
                second[s, 0, k, :, 0], second[s, 0, k, :, 1] = c, n
                second[s, 1, k, :, 0], second[s, 1, k, :, 1] = -n, c
        second = second.reshape(self.slabs, 2 * self.keep, 2 * yl)
        third = np.zeros((2, self.keep, g, self.slabs, 8), np.float32)
        for z in range(zl):
            c, n = cos[:, z::zl][:, :, None], sin[:, z::zl][:, :, None]
            third[0, :, :, :, 2 * z], third[0, :, :, :, 2 * z + 1] = c, n
            third[1, :, :, :, 2 * z], third[1, :, :, :, 2 * z + 1] = -n, c
        third = third.reshape(2 * self.keep, self.count * 8)
        high, low = split_bf16(second)
        return (
            np.stack(split_bf16(first)),
            np.concatenate([high, high, low], axis=2),
            np.stack(split_bf16(third)),
        )


def kernel(
    plan, vel_hbm, vort_hbm, modes_hbm, first_hbm, second_hbm, third_hbm, out_ref,
    fields, modes, first, second, third, cross, send, recv,
    field_sem, table_sem, late_sem, send_sem, recv_sem,
):
    sec, pen, slab = (lax.axis_index(a) for a in AXES)
    group = sec * plan.pens + pen
    me = group * plan.slabs + slab
    cells, keep = plan.cells, plan.keep
    for i, source in enumerate((vel_hbm, vort_hbm)):
        for c in range(3):
            pltpu.make_async_copy(source.at[c], fields.at[i, c], field_sem).start()
    table_loads = [
        pltpu.make_async_copy(first_hbm.at[0], first.at[0, 0:cells], table_sem.at[0]),
        pltpu.make_async_copy(first_hbm.at[0], first.at[1, 0:cells], table_sem.at[1]),
        pltpu.make_async_copy(first_hbm.at[1], first.at[2, 0:cells], table_sem.at[2]),
        pltpu.make_async_copy(second_hbm.at[slab], second, table_sem.at[3]),
    ]
    late_loads = [
        pltpu.make_async_copy(third_hbm, third, late_sem.at[0]),
        pltpu.make_async_copy(modes_hbm, modes, late_sem.at[1]),
    ]
    for load in table_loads + late_loads:
        load.start()

    barrier = pltpu.get_barrier_semaphore()

    def place(to):
        return (to[0] * plan.pens + to[1]) * plan.slabs + to[2]

    for to in reversed(plan.order):

        @pl.when(me != place(to))
        def _(to=to):
            pl.semaphore_signal(
                barrier, inc=1, device_id=to, device_id_type=pl.DeviceIdType.MESH
            )

    if plan.rows < 8:
        recv[:, plan.rows : 8] = jnp.zeros((plan.count, 8 - plan.rows, 128), jnp.float32)
    cross[...] = jnp.zeros_like(cross)
    if cells < 128:
        for i in range(3):
            first[i, cells:128] = jnp.zeros((128 - cells, first.shape[2]), jnp.bfloat16)

    pltpu.make_async_copy(fields, fields, field_sem).wait()
    zl, yl = plan.z_rows, plan.y_rows
    area = zl * yl
    v, w = ([fields[i, c].reshape(area, cells) for c in range(3)] for i in range(2))
    for c in range(3):
        p, q = (c + 1) % 3, (c + 2) % 3
        cross[c * area : (c + 1) * area, 0:cells] = v[p] * w[q] - v[q] * w[p]
    for load in table_loads:
        load.wait()
    high, low = split_in_kernel(cross[...])
    along_x = mm(
        jnp.concatenate([high, low], axis=1), jnp.concatenate([first[0], first[1]], axis=0)
    ) + mm(high, first[2])
    slot = lax.broadcasted_iota(jnp.int32, (area, 2 * plan.wide), 1) % 128 // plan.width
    along_x = [along_x[c * area : (c + 1) * area] for c in range(3)]
    along_x = jnp.where(slot == 0, along_x[0], jnp.where(slot == 1, along_x[1], along_x[2]))
    high = along_x.astype(jnp.bfloat16).astype(jnp.float32)
    low = along_x - high
    upper = lax.broadcasted_iota(jnp.int32, (plan.groups, plan.wide), 1) % plan.width // plan.block
    for z in range(zl):
        parts = []
        for part in (high, low):
            piece = part[z * yl : (z + 1) * yl]
            parts.append(
                jnp.concatenate([piece[:, : plan.wide], piece[:, plan.wide :]], axis=0)
            )
        stack = jnp.concatenate([parts[0], parts[1], parts[0]], axis=0).astype(jnp.bfloat16)
        planes = mm(second[...], stack)
        for k in range(2):
            total = None
            for i in range(plan.rows_ky):
                start = (k * plan.rows_ky + i) * plan.groups
                piece = planes[start : start + plan.groups]
                total = piece if total is None else jnp.where(upper == i, piece, total)
            for s in range(plan.slabs):
                rows = pl.ds(s * plan.groups * 8 + 2 * z + k, plan.groups, stride=8)
                send[rows, :] = total[:, s * 128 : (s + 1) * 128]

    pl.semaphore_wait(barrier, plan.count - 1)
    used = pl.ds(0, plan.rows)

    def slot_of(s, g):
        return (s * plan.groups + g) * 8

    for to in plan.order:

        @pl.when(me != place(to))
        def _(to=to):
            pltpu.make_async_remote_copy(
                src_ref=send.at[pl.ds(slot_of(to[2], to[0] * plan.pens + to[1]), plan.rows)],
                dst_ref=recv.at[me, used],
                send_sem=send_sem,
                recv_sem=recv_sem,
                device_id=to,
                device_id_type=pl.DeviceIdType.MESH,
            ).start()

    own = pl.multiple_of(slot_of(slab, group), 8)
    recv[me, 0 : plan.rows] = send[pl.ds(own, plan.rows)]

    bm, ky_n, width = plan.block, plan.rows_ky, plan.width

    def signed(index):
        return jnp.where(index < keep // 2, index, index - keep)

    row = lax.broadcasted_iota(jnp.int32, (width, keep), 0)
    kx = signed(row % bm + slab * bm)
    ky = signed(row // bm + group * ky_n)
    kz = signed(lax.broadcasted_iota(jnp.int32, (width, keep), 1))
    limit = -(keep // 2)
    mask = ((kx != limit) & (ky != limit) & (kz != limit)).astype(jnp.float32)
    waves = [k.astype(jnp.float32) for k in (kx, ky, kz)]
    ksq = waves[0] * waves[0] + waves[1] * waves[1] + waves[2] * waves[2]
    inverse = 1.0 / jnp.maximum(ksq, 1.0)
    damp = (0.5 / (keep // 2) ** 2) * ksq
    for load in late_loads:
        load.wait()
    damped = [
        [
            jnp.concatenate([modes[c, i, k] for i in range(ky_n)], axis=0) * damp
            for k in range(2)
        ]
        for c in range(3)
    ]

    arrived = recv.at[pl.ds(0, plan.count - 1), used]
    pltpu.make_async_copy(arrived, arrived, recv_sem).wait()
    got = split_in_kernel(recv[...].reshape(plan.count * 8, 128))
    out = split_dot((third[0], third[1]), got)
    for k in range(2):
        turned = jnp.transpose(out[k * keep : (k + 1) * keep])
        comp = [turned[c * width : (c + 1) * width] for c in range(3)]
        inner = (waves[0] * comp[0] + waves[1] * comp[1] + waves[2] * comp[2]) * inverse
        for c in range(3):
            result = (comp[c] - waves[c] * inner) * mask - damped[c][k]
            for i in range(ky_n):
                out_ref[c, i, k] = result[i * bm : (i + 1) * bm]
    pltpu.make_async_copy(arrived, arrived, send_sem).wait()


def direct(plan, tables, velocity, vorticity, velocity_modes):
    modes = jnp.transpose(velocity_modes, (0, 2, 3, 4, 1))
    first, second, third = tables
    hbm = pl.BlockSpec(memory_space=pltpu.HBM)
    out = pl.pallas_call(
        functools.partial(kernel, plan),
        out_shape=pltpu.VMEM(modes.shape, jnp.float32),
        in_specs=[hbm] * 6,
        out_specs=pl.BlockSpec(memory_space=pltpu.VMEM),
        scratch_shapes=[
            pltpu.VMEM((2,) + velocity.shape, jnp.float32),
            pltpu.VMEM(modes.shape, jnp.float32),
            pltpu.VMEM((3, 128, 2 * plan.wide), jnp.bfloat16),
            pltpu.VMEM(second.shape[1:], jnp.bfloat16),
            pltpu.VMEM(third.shape, jnp.bfloat16),
            pltpu.VMEM((3 * plan.z_rows * plan.y_rows, 128), jnp.float32),
            pltpu.VMEM((plan.slabs * plan.groups * 8, 128), jnp.float32),
            pltpu.VMEM((plan.count, 8, 128), jnp.float32),
            pltpu.SemaphoreType.DMA,
            pltpu.SemaphoreType.DMA((4,)),
            pltpu.SemaphoreType.DMA((2,)),
            pltpu.SemaphoreType.DMA,
            pltpu.SemaphoreType.DMA,
        ],
        compiler_params=pltpu.CompilerParams(collective_id=0, has_side_effects=True),
    )(velocity, vorticity, modes, first, second, third)
    return jnp.transpose(out, (0, 4, 1, 2, 3))


def solution(mesh):
    sizes = dict(mesh.shape)
    order = by_distance(mesh.devices)

    def run(velocity, vorticity, velocity_modes):
        _, z_rows, y_rows, cells = velocity.shape
        plan = Plan(sizes, order, cells, velocity_modes.shape[1], z_rows, y_rows)
        if not plan.fits():
            return per_device(velocity, vorticity, velocity_modes)
        return direct(plan, plan.tables(), velocity, vorticity, velocity_modes)

    return jax.shard_map(
        run,
        mesh=mesh,
        in_specs=(
            P(None, ("section", "pen"), "slab", None),
            P(None, ("section", "pen"), "slab", None),
            P(None, None, ("section", "pen"), None, "slab"),
        ),
        out_specs=P(None, None, ("section", "pen"), None, "slab"),
        check_vma=False,
    )
```

```python
import functools
import math

import jax
import jax.numpy as jnp
import numpy as np
from jax import lax
from jax.experimental import pallas as pl
from jax.experimental.pallas import tpu as pltpu
from jax.sharding import PartitionSpec as P

AXES = ("section", "pen", "slab")
highest = lax.Precision.HIGHEST


def signed_modes(index, count):
    return jnp.where(index < count // 2, index, index - count)


def discrete_fourier_tables(length, keep_count):
    modes = signed_modes(jnp.arange(keep_count, dtype=jnp.int32), keep_count)
    mode_positions = jnp.arange(length, dtype=jnp.int32)
    phase = jnp.remainder(modes[:, None] * mode_positions[None, :], length).astype(jnp.float32)
    angles = 2.0 * math.pi / length * phase
    factor = 1.0 / math.sqrt(length)
    return (jnp.cos(angles) * factor, jnp.sin(angles) * factor)


def complex_apply(form, cosine, sine, real_part, imag_part):
    out_real = jnp.einsum(form, cosine, real_part, precision=highest) + jnp.einsum(
        form, sine, imag_part, precision=highest
    )
    out_imag = jnp.einsum(form, cosine, imag_part, precision=highest) - jnp.einsum(
        form, sine, real_part, precision=highest
    )
    return (out_real, out_imag)


def per_device(velocity, vorticity, velocity_modes):
    grid_cells = velocity.shape[3]
    keep_count = velocity_modes.shape[1]
    cross_product = jnp.stack(
        [
            velocity[1] * vorticity[2] - velocity[2] * vorticity[1],
            velocity[2] * vorticity[0] - velocity[0] * vorticity[2],
            velocity[0] * vorticity[1] - velocity[1] * vorticity[0],
        ]
    )
    slabs = lax.axis_size("slab")
    block_modes = keep_count // slabs
    cosine_table, sine_table = discrete_fourier_tables(grid_cells, keep_count)
    cols_real = cosine_table.T.reshape(grid_cells, slabs, block_modes)
    cols_imag = (-sine_table).T.reshape(grid_cells, slabs, block_modes)
    column_table = jnp.stack([cols_real, cols_imag], axis=2).reshape(grid_cells, 2 * keep_count)
    first_pass = jnp.einsum("czyx,xj->czyj", cross_product, column_table, precision=highest)
    block = lax.all_to_all(first_pass, "slab", split_axis=3, concat_axis=2, tiled=True)
    out_real, out_imag = complex_apply(
        "ky,czyj->czkj",
        cosine_table,
        sine_table,
        block[..., :block_modes],
        block[..., block_modes:],
    )
    second_pass = jnp.concatenate([out_real, out_imag], axis=-1)
    halves = lax.axis_size("section")
    pens = lax.axis_size("pen")
    rows_ky = keep_count // (halves * pens)
    block = lax.all_to_all(second_pass, ("section", "pen"), split_axis=2, concat_axis=1, tiled=True)
    out_real, out_imag = complex_apply(
        "kz,czyj->ckyj",
        cosine_table,
        sine_table,
        block[..., :block_modes],
        block[..., block_modes:],
    )
    third_pass = jnp.concatenate([out_real, out_imag], axis=-1)
    group_index = lax.axis_index("section") * pens + lax.axis_index("pen")
    modes_z = signed_modes(jnp.arange(keep_count, dtype=jnp.int32), keep_count)[:, None, None]
    modes_y = signed_modes(
        group_index * rows_ky + jnp.arange(rows_ky, dtype=jnp.int32), keep_count
    )[None, :, None]
    modes_x = signed_modes(
        lax.axis_index("slab") * block_modes + jnp.arange(block_modes, dtype=jnp.int32), keep_count
    )[None, None, :]
    limit = -(keep_count // 2)
    keep_mask = ((modes_x != limit) & (modes_y != limit) & (modes_z != limit)).astype(jnp.float32)
    waves = (modes_x.astype(jnp.float32), modes_y.astype(jnp.float32), modes_z.astype(jnp.float32))
    ksq = waves[0] * waves[0] + waves[1] * waves[1] + waves[2] * waves[2]
    denom = jnp.maximum(ksq, 1.0)
    parts = []
    for which in range(2):
        chosen = third_pass[..., which * block_modes : (which + 1) * block_modes]
        comp = [chosen[c] for c in range(3)]
        inner = (waves[0] * comp[0] + waves[1] * comp[1] + waves[2] * comp[2]) / denom
        parts.append(jnp.stack([comp[c] - waves[c] * inner for c in range(3)]))
    projected = jnp.stack(parts, axis=3)
    visc = 0.5 / (keep_count // 2) ** 2
    return (
        projected * keep_mask[None, :, :, None, :]
        - visc * ksq[None, :, :, None, :] * velocity_modes
    )


def split_bf16(table):
    high = table.astype(jnp.bfloat16)
    low = (table - high.astype(np.float32)).astype(jnp.bfloat16)
    return high, low


def split_in_kernel(value):
    high = value.astype(jnp.bfloat16)
    low = (value - high.astype(jnp.float32)).astype(jnp.bfloat16)
    return high, low


def mm(a, b):
    return lax.dot_general(a, b, (((1,), (0,)), ((), ())), preferred_element_type=jnp.float32)


def split_dot(a, b):
    return mm(a[0], b[0]) + mm(a[1], b[0]) + mm(a[0], b[1])


def wave_numbers(count):
    index = np.arange(count)
    return np.where(index < count // 2, index, index - count)


def host_tables(cells, keep):
    phase = np.remainder(wave_numbers(keep)[:, None] * np.arange(cells)[None, :], cells)
    angles = 2.0 * np.pi / cells * phase
    factor = 1.0 / np.sqrt(cells)
    return np.cos(angles) * factor, np.sin(angles) * factor


def by_distance(devices):
    origin = getattr(devices.flat[0], "coords", ())

    def hops(index):
        return sum(abs(a - b) for a, b in zip(getattr(devices[index], "coords", ()), origin))

    return sorted(np.ndindex(devices.shape), key=lambda index: (hops(index), index))


class Plan:
    def __init__(self, mesh_shape, order, cells, keep, z_rows, y_rows):
        self.order = order
        self.cells, self.keep, self.z_rows, self.y_rows = cells, keep, z_rows, y_rows
        self.halves, self.pens, self.slabs = (mesh_shape[a] for a in AXES)
        self.groups = self.halves * self.pens
        self.count = self.groups * self.slabs
        self.rows_ky = keep // self.groups
        self.block = keep // self.slabs
        self.width = self.rows_ky * self.block
        self.rows = 2 * z_rows
        self.wide = self.slabs * 128

    def fits(self):
        return (
            self.rows_ky * self.groups == self.keep
            and self.block * self.slabs == self.keep
            and 3 * self.width <= 128
            and 128 % self.width == 0
            and self.rows <= 8
            and self.cells <= 128
            and self.cells % 16 == 0
            and self.y_rows % 8 == 0
            and 6 * self.y_rows <= 256
            and self.groups % 8 == 0
            and self.keep % 8 == 0
            and self.block % 8 == 0
            and 3 * self.z_rows * self.y_rows <= 512
            and 2 <= self.count <= 64
        )

    def tables(self):
        cos, sin = host_tables(self.cells, self.keep)
        g, zl, yl, ky_n, bm = self.groups, self.z_rows, self.y_rows, self.rows_ky, self.block
        first = np.zeros((self.cells, 2, self.slabs, 128 // self.width, ky_n, bm), np.float32)
        for s in range(self.slabs):
            modes = slice(s * bm, (s + 1) * bm)
            first[:, 0, s, :3] = cos[modes].T[:, None, None]
            first[:, 1, s, :3] = -sin[modes].T[:, None, None]
        first = first.reshape(self.cells, 2 * self.wide)
        second = np.zeros((self.slabs, 2, ky_n, g, 2, yl), np.float32)
        for s in range(self.slabs):
            for k in range(ky_n):
                c = cos[k::ky_n, s * yl : (s + 1) * yl]
                n = sin[k::ky_n, s * yl : (s + 1) * yl]
                second[s, 0, k, :, 0], second[s, 0, k, :, 1] = c, n
                second[s, 1, k, :, 0], second[s, 1, k, :, 1] = -n, c
        second = second.reshape(self.slabs, 2 * self.keep, 2 * yl)
        third = np.zeros((2, self.keep, g, self.slabs, 8), np.float32)
        for z in range(zl):
            c, n = cos[:, z::zl][:, :, None], sin[:, z::zl][:, :, None]
            third[0, :, :, :, 2 * z], third[0, :, :, :, 2 * z + 1] = c, n
            third[1, :, :, :, 2 * z], third[1, :, :, :, 2 * z + 1] = -n, c
        third = third.reshape(2 * self.keep, self.count * 8)
        high, low = split_bf16(second)
        kept = (self.order[0][0] * self.pens + self.order[0][1]) * ky_n
        near = np.zeros((self.slabs, ky_n, 2, yl, 128), np.float32)
        for s in range(self.slabs):
            for k in range(ky_n):
                near[s, k, 0] = cos[kept + k, s * yl : (s + 1) * yl, None]
                near[s, k, 1] = sin[kept + k, s * yl : (s + 1) * yl, None]
        return (
            np.stack(split_bf16(first)),
            np.concatenate([high, high, low], axis=2),
            np.stack(split_bf16(third)),
            near,
        )


def kernel(
    plan, vel_hbm, vort_hbm, modes_hbm, first_hbm, second_hbm, third_hbm, near_hbm, out_ref,
    fields, modes, first, second, third, near, cross, quick, send, recv,
    field_sem, table_sem, late_sem, send_sem, recv_sem,
):
    sec, pen, slab = (lax.axis_index(a) for a in AXES)
    group = sec * plan.pens + pen
    me = group * plan.slabs + slab
    cells, keep = plan.cells, plan.keep
    for i, source in enumerate((vel_hbm, vort_hbm)):
        for c in range(3):
            pltpu.make_async_copy(source.at[c], fields.at[i, c], field_sem).start()
    table_loads = [
        pltpu.make_async_copy(first_hbm.at[0], first.at[0, 0:cells], table_sem.at[0]),
        pltpu.make_async_copy(first_hbm.at[1], first.at[1, 0:cells], table_sem.at[1]),
        pltpu.make_async_copy(second_hbm.at[slab], second, table_sem.at[2]),
        pltpu.make_async_copy(near_hbm.at[slab], near, table_sem.at[3]),
    ]
    late_loads = [
        pltpu.make_async_copy(third_hbm, third, late_sem.at[0]),
        pltpu.make_async_copy(modes_hbm, modes, late_sem.at[1]),
    ]
    for load in table_loads:
        load.start()

    barrier = pltpu.get_barrier_semaphore()

    def place(to):
        return (to[0] * plan.pens + to[1]) * plan.slabs + to[2]

    for to in reversed(plan.order):

        @pl.when(me != place(to))
        def _(to=to):
            pl.semaphore_signal(
                barrier, inc=1, device_id=to, device_id_type=pl.DeviceIdType.MESH
            )

    if plan.rows < 8:
        recv[:, plan.rows : 8] = jnp.zeros((plan.count, 8 - plan.rows, 128), jnp.float32)
    cross[...] = jnp.zeros_like(cross)
    if cells < 128:
        for i in range(2):
            first[i, cells:128] = jnp.zeros((128 - cells, first.shape[2]), jnp.bfloat16)

    pltpu.make_async_copy(fields, fields, field_sem).wait()
    for load in late_loads:
        load.start()
    zl, yl = plan.z_rows, plan.y_rows
    area = zl * yl
    v, w = ([fields[i, c].reshape(area, cells) for c in range(3)] for i in range(2))
    for c in range(3):
        p, q = (c + 1) % 3, (c + 2) % 3
        cross[c * area : (c + 1) * area, 0:cells] = v[p] * w[q] - v[q] * w[p]
    for load in table_loads:
        load.wait()
    sub = lax.broadcasted_iota(jnp.int32, (8, 128), 0)
    blocks = []
    for i in range(plan.rows_ky):
        for c in range(3):
            block = None
            for z in range(zl):
                start = (c * zl + z) * yl
                pair = []
                for k in range(2):
                    terms = cross[start : start + yl] * near[i, k]
                    part = terms[0:8]
                    for r in range(8, yl, 8):
                        part = part + terms[r : r + 8]
                    pair.append(part)
                part = jnp.where(sub < 4, pair[0], pair[1]) + pltpu.roll(
                    jnp.where(sub < 4, pair[1], pair[0]), 4, 0
                )
                part = part + pltpu.roll(part, 6, 0)
                part = part + pltpu.roll(part, 7, 0)
                if z == 0:
                    block = part
                else:
                    block = jnp.where(sub % 4 == z, pltpu.roll(part, z, 0), block)
            blocks.append(block)
    high, low = split_in_kernel(jnp.concatenate(blocks, axis=0))
    doubled = jnp.concatenate([first[0], first[0]], axis=0)
    planes = mm(jnp.concatenate([high, low], axis=1), doubled) + mm(high, first[1])
    cell = lax.broadcasted_iota(jnp.int32, (8, 2 * plan.wide), 1) % 128 // plan.block
    total = planes[0:8]
    for i in range(plan.rows_ky):
        for c in range(3):
            start = (i * 3 + c) * 8
            total = jnp.where(cell == c * plan.rows_ky + i, planes[start : start + 8], total)
    real, imag = total[:, : plan.wide], total[:, plan.wide :]
    parts = (real + pltpu.roll(imag, 4, 0), imag - pltpu.roll(real, 4, 0))
    for k in range(2):
        for s in range(plan.slabs):
            quick[pl.ds(s * 8 + k, zl, stride=2), :] = parts[k][0:zl, s * 128 : (s + 1) * 128]

    pl.semaphore_wait(barrier, plan.count - 1)
    used = pl.ds(0, plan.rows)

    def slot_of(s, g):
        return (s * plan.groups + g) * 8

    for s in range(plan.slabs):
        to = (*plan.order[0][:2], s)

        @pl.when(me != place(to))
        def _(to=to):
            pltpu.make_async_remote_copy(
                src_ref=quick.at[pl.ds(to[2] * 8, plan.rows)],
                dst_ref=recv.at[me, used],
                send_sem=send_sem,
                recv_sem=recv_sem,
                device_id=to,
                device_id_type=pl.DeviceIdType.MESH,
            ).start()

    high, low = split_in_kernel(cross[...])
    along_x = mm(
        jnp.concatenate([high, low], axis=1), jnp.concatenate([first[0], first[0]], axis=0)
    ) + mm(high, first[1])
    slot = lax.broadcasted_iota(jnp.int32, (area, 2 * plan.wide), 1) % 128 // plan.width
    along_x = [along_x[c * area : (c + 1) * area] for c in range(3)]
    along_x = jnp.where(slot == 0, along_x[0], jnp.where(slot == 1, along_x[1], along_x[2]))
    high = along_x.astype(jnp.bfloat16).astype(jnp.float32)
    low = along_x - high
    upper = lax.broadcasted_iota(jnp.int32, (plan.groups, plan.wide), 1) % plan.width // plan.block
    for z in range(zl):
        parts = []
        for part in (high, low):
            piece = part[z * yl : (z + 1) * yl]
            parts.append(
                jnp.concatenate([piece[:, : plan.wide], piece[:, plan.wide :]], axis=0)
            )
        stack = jnp.concatenate([parts[0], parts[1], parts[0]], axis=0).astype(jnp.bfloat16)
        planes = mm(second[...], stack)
        for k in range(2):
            total = None
            for i in range(plan.rows_ky):
                start = (k * plan.rows_ky + i) * plan.groups
                piece = planes[start : start + plan.groups]
                total = piece if total is None else jnp.where(upper == i, piece, total)
            for s in range(plan.slabs):
                rows = pl.ds(s * plan.groups * 8 + 2 * z + k, plan.groups, stride=8)
                send[rows, :] = total[:, s * 128 : (s + 1) * 128]

    for to in plan.order[plan.slabs :]:

        @pl.when(me != place(to))
        def _(to=to):
            pltpu.make_async_remote_copy(
                src_ref=send.at[pl.ds(slot_of(to[2], to[0] * plan.pens + to[1]), plan.rows)],
                dst_ref=recv.at[me, used],
                send_sem=send_sem,
                recv_sem=recv_sem,
                device_id=to,
                device_id_type=pl.DeviceIdType.MESH,
            ).start()

    own = pl.multiple_of(slot_of(slab, group), 8)
    recv[me, 0 : plan.rows] = send[pl.ds(own, plan.rows)]

    bm, ky_n, width = plan.block, plan.rows_ky, plan.width

    def signed(index):
        return jnp.where(index < keep // 2, index, index - keep)

    row = lax.broadcasted_iota(jnp.int32, (width, keep), 0)
    kx = signed(row % bm + slab * bm)
    ky = signed(row // bm + group * ky_n)
    kz = signed(lax.broadcasted_iota(jnp.int32, (width, keep), 1))
    limit = -(keep // 2)
    mask = ((kx != limit) & (ky != limit) & (kz != limit)).astype(jnp.float32)
    waves = [k.astype(jnp.float32) for k in (kx, ky, kz)]
    ksq = waves[0] * waves[0] + waves[1] * waves[1] + waves[2] * waves[2]
    inverse = 1.0 / jnp.maximum(ksq, 1.0)
    damp = (0.5 / (keep // 2) ** 2) * ksq
    for load in late_loads:
        load.wait()
    damped = [
        [
            jnp.concatenate([modes[c, i, k] for i in range(ky_n)], axis=0) * damp
            for k in range(2)
        ]
        for c in range(3)
    ]

    arrived = recv.at[pl.ds(0, plan.count - 1), used]
    pltpu.make_async_copy(arrived, arrived, recv_sem).wait()
    got = split_in_kernel(recv[...].reshape(plan.count * 8, 128))
    wide_ = mm(third[0], jnp.concatenate([got[0], got[1]], axis=1))
    out = wide_[:, :128] + wide_[:, 128:] + mm(third[1], got[0])
    for k in range(2):
        turned = jnp.transpose(out[k * keep : (k + 1) * keep])
        comp = [turned[c * width : (c + 1) * width] for c in range(3)]
        inner = (waves[0] * comp[0] + waves[1] * comp[1] + waves[2] * comp[2]) * inverse
        for c in range(3):
            result = (comp[c] - waves[c] * inner) * mask - damped[c][k]
            for i in range(ky_n):
                out_ref[c, i, k] = result[i * bm : (i + 1) * bm]
    pltpu.make_async_copy(arrived, arrived, send_sem).wait()


def direct(plan, tables, velocity, vorticity, velocity_modes):
    modes = jnp.transpose(velocity_modes, (0, 2, 3, 4, 1))
    first, second, third, near = tables
    hbm = pl.BlockSpec(memory_space=pltpu.HBM)
    out = pl.pallas_call(
        functools.partial(kernel, plan),
        out_shape=pltpu.VMEM(modes.shape, jnp.float32),
        in_specs=[hbm] * 7,
        out_specs=pl.BlockSpec(memory_space=pltpu.VMEM),
        scratch_shapes=[
            pltpu.VMEM((2,) + velocity.shape, jnp.float32),
            pltpu.VMEM(modes.shape, jnp.float32),
            pltpu.VMEM((2, 128, 2 * plan.wide), jnp.bfloat16),
            pltpu.VMEM(second.shape[1:], jnp.bfloat16),
            pltpu.VMEM(third.shape, jnp.bfloat16),
            pltpu.VMEM(near.shape[1:], jnp.float32),
            pltpu.VMEM((3 * plan.z_rows * plan.y_rows, 128), jnp.float32),
            pltpu.VMEM((plan.slabs * 8, 128), jnp.float32),
            pltpu.VMEM((plan.slabs * plan.groups * 8, 128), jnp.float32),
            pltpu.VMEM((plan.count, 8, 128), jnp.float32),
            pltpu.SemaphoreType.DMA,
            pltpu.SemaphoreType.DMA((4,)),
            pltpu.SemaphoreType.DMA((2,)),
            pltpu.SemaphoreType.DMA,
            pltpu.SemaphoreType.DMA,
        ],
        compiler_params=pltpu.CompilerParams(collective_id=0, has_side_effects=True),
    )(velocity, vorticity, modes, first, second, third, near)
    return jnp.transpose(out, (0, 4, 1, 2, 3))


def solution(mesh):
    sizes = dict(mesh.shape)
    order = by_distance(mesh.devices)

    def run(velocity, vorticity, velocity_modes):
        _, z_rows, y_rows, cells = velocity.shape
        plan = Plan(sizes, order, cells, velocity_modes.shape[1], z_rows, y_rows)
        if not plan.fits():
            return per_device(velocity, vorticity, velocity_modes)
        return direct(plan, plan.tables(), velocity, vorticity, velocity_modes)

    return jax.shard_map(
        run,
        mesh=mesh,
        in_specs=(
            P(None, ("section", "pen"), "slab", None),
            P(None, ("section", "pen"), "slab", None),
            P(None, None, ("section", "pen"), None, "slab"),
        ),
        out_specs=P(None, None, ("section", "pen"), None, "slab"),
        check_vma=False,
    )
```

```python
import functools
import math

import jax
import jax.numpy as jnp
import numpy as np
from jax import lax
from jax.experimental import pallas as pl
from jax.experimental.pallas import tpu as pltpu
from jax.sharding import PartitionSpec as P

AXES = ("section", "pen", "slab")
highest = lax.Precision.HIGHEST


def signed_modes(index, count):
    return jnp.where(index < count // 2, index, index - count)


def discrete_fourier_tables(length, keep_count):
    modes = signed_modes(jnp.arange(keep_count, dtype=jnp.int32), keep_count)
    mode_positions = jnp.arange(length, dtype=jnp.int32)
    phase = jnp.remainder(modes[:, None] * mode_positions[None, :], length).astype(jnp.float32)
    angles = 2.0 * math.pi / length * phase
    factor = 1.0 / math.sqrt(length)
    return (jnp.cos(angles) * factor, jnp.sin(angles) * factor)


def complex_apply(form, cosine, sine, real_part, imag_part):
    out_real = jnp.einsum(form, cosine, real_part, precision=highest) + jnp.einsum(
        form, sine, imag_part, precision=highest
    )
    out_imag = jnp.einsum(form, cosine, imag_part, precision=highest) - jnp.einsum(
        form, sine, real_part, precision=highest
    )
    return (out_real, out_imag)


def per_device(velocity, vorticity, velocity_modes):
    grid_cells = velocity.shape[3]
    keep_count = velocity_modes.shape[1]
    cross_product = jnp.stack(
        [
            velocity[1] * vorticity[2] - velocity[2] * vorticity[1],
            velocity[2] * vorticity[0] - velocity[0] * vorticity[2],
            velocity[0] * vorticity[1] - velocity[1] * vorticity[0],
        ]
    )
    slabs = lax.axis_size("slab")
    block_modes = keep_count // slabs
    cosine_table, sine_table = discrete_fourier_tables(grid_cells, keep_count)
    cols_real = cosine_table.T.reshape(grid_cells, slabs, block_modes)
    cols_imag = (-sine_table).T.reshape(grid_cells, slabs, block_modes)
    column_table = jnp.stack([cols_real, cols_imag], axis=2).reshape(grid_cells, 2 * keep_count)
    first_pass = jnp.einsum("czyx,xj->czyj", cross_product, column_table, precision=highest)
    block = lax.all_to_all(first_pass, "slab", split_axis=3, concat_axis=2, tiled=True)
    out_real, out_imag = complex_apply(
        "ky,czyj->czkj",
        cosine_table,
        sine_table,
        block[..., :block_modes],
        block[..., block_modes:],
    )
    second_pass = jnp.concatenate([out_real, out_imag], axis=-1)
    halves = lax.axis_size("section")
    pens = lax.axis_size("pen")
    rows_ky = keep_count // (halves * pens)
    block = lax.all_to_all(second_pass, ("section", "pen"), split_axis=2, concat_axis=1, tiled=True)
    out_real, out_imag = complex_apply(
        "kz,czyj->ckyj",
        cosine_table,
        sine_table,
        block[..., :block_modes],
        block[..., block_modes:],
    )
    third_pass = jnp.concatenate([out_real, out_imag], axis=-1)
    group_index = lax.axis_index("section") * pens + lax.axis_index("pen")
    modes_z = signed_modes(jnp.arange(keep_count, dtype=jnp.int32), keep_count)[:, None, None]
    modes_y = signed_modes(
        group_index * rows_ky + jnp.arange(rows_ky, dtype=jnp.int32), keep_count
    )[None, :, None]
    modes_x = signed_modes(
        lax.axis_index("slab") * block_modes + jnp.arange(block_modes, dtype=jnp.int32), keep_count
    )[None, None, :]
    limit = -(keep_count // 2)
    keep_mask = ((modes_x != limit) & (modes_y != limit) & (modes_z != limit)).astype(jnp.float32)
    waves = (modes_x.astype(jnp.float32), modes_y.astype(jnp.float32), modes_z.astype(jnp.float32))
    ksq = waves[0] * waves[0] + waves[1] * waves[1] + waves[2] * waves[2]
    denom = jnp.maximum(ksq, 1.0)
    parts = []
    for which in range(2):
        chosen = third_pass[..., which * block_modes : (which + 1) * block_modes]
        comp = [chosen[c] for c in range(3)]
        inner = (waves[0] * comp[0] + waves[1] * comp[1] + waves[2] * comp[2]) / denom
        parts.append(jnp.stack([comp[c] - waves[c] * inner for c in range(3)]))
    projected = jnp.stack(parts, axis=3)
    visc = 0.5 / (keep_count // 2) ** 2
    return (
        projected * keep_mask[None, :, :, None, :]
        - visc * ksq[None, :, :, None, :] * velocity_modes
    )


def split_bf16(table):
    high = table.astype(jnp.bfloat16)
    low = (table - high.astype(np.float32)).astype(jnp.bfloat16)
    return high, low


def split_in_kernel(value):
    high = value.astype(jnp.bfloat16)
    low = (value - high.astype(jnp.float32)).astype(jnp.bfloat16)
    return high, low


def mm(a, b):
    return lax.dot_general(a, b, (((1,), (0,)), ((), ())), preferred_element_type=jnp.float32)


def split_dot(a, b):
    return mm(a[0], b[0]) + mm(a[1], b[0]) + mm(a[0], b[1])


def wave_numbers(count):
    index = np.arange(count)
    return np.where(index < count // 2, index, index - count)


def host_tables(cells, keep):
    phase = np.remainder(wave_numbers(keep)[:, None] * np.arange(cells)[None, :], cells)
    angles = 2.0 * np.pi / cells * phase
    factor = 1.0 / np.sqrt(cells)
    return np.cos(angles) * factor, np.sin(angles) * factor


def by_distance(devices):
    origin = getattr(devices.flat[0], "coords", ())

    def hops(index):
        return [abs(a - b) for a, b in zip(getattr(devices[index], "coords", ()), origin)]

    every = list(np.ndindex(devices.shape))
    spans = [max(far) for far in zip(*map(hops, every))]

    def key(index):
        far = hops(index)
        if sum(far) == 0:
            return -1, 0, index
        return (far[spans.index(max(spans))], -sum(far), index) if far else (0, 0, index)

    return sorted(every, key=key)


class Plan:
    def __init__(self, mesh_shape, order, cells, keep, z_rows, y_rows):
        self.order = order
        self.cells, self.keep, self.z_rows, self.y_rows = cells, keep, z_rows, y_rows
        self.halves, self.pens, self.slabs = (mesh_shape[a] for a in AXES)
        self.groups = self.halves * self.pens
        self.count = self.groups * self.slabs
        self.rows_ky = keep // self.groups
        self.block = keep // self.slabs
        self.width = self.rows_ky * self.block
        self.rows = 2 * z_rows
        self.wide = self.slabs * 128

    def fits(self):
        return (
            self.rows_ky * self.groups == self.keep
            and self.block * self.slabs == self.keep
            and 3 * self.width <= 128
            and 128 % self.width == 0
            and self.rows <= 8
            and self.cells <= 128
            and self.cells % 16 == 0
            and self.y_rows % 8 == 0
            and 6 * self.y_rows <= 256
            and self.groups % 8 == 0
            and self.keep % 8 == 0
            and self.block % 8 == 0
            and 3 * self.z_rows * self.y_rows <= 512
            and 2 <= self.count <= 64
        )

    def tables(self):
        cos, sin = host_tables(self.cells, self.keep)
        g, zl, yl, ky_n, bm = self.groups, self.z_rows, self.y_rows, self.rows_ky, self.block
        first = np.zeros((self.cells, 2, self.slabs, 128 // self.width, ky_n, bm), np.float32)
        for s in range(self.slabs):
            modes = slice(s * bm, (s + 1) * bm)
            first[:, 0, s, :3] = cos[modes].T[:, None, None]
            first[:, 1, s, :3] = -sin[modes].T[:, None, None]
        first = first.reshape(self.cells, 2 * self.wide)
        second = np.zeros((self.slabs, 2, ky_n, g, 2, yl), np.float32)
        for s in range(self.slabs):
            for k in range(ky_n):
                c = cos[k::ky_n, s * yl : (s + 1) * yl]
                n = sin[k::ky_n, s * yl : (s + 1) * yl]
                second[s, 0, k, :, 0], second[s, 0, k, :, 1] = c, n
                second[s, 1, k, :, 0], second[s, 1, k, :, 1] = -n, c
        second = second.reshape(self.slabs, 2 * self.keep, 2 * yl)
        third = np.zeros((2, self.keep, g, self.slabs, 8), np.float32)
        for z in range(zl):
            c, n = cos[:, z::zl][:, :, None], sin[:, z::zl][:, :, None]
            third[0, :, :, :, 2 * z], third[0, :, :, :, 2 * z + 1] = c, n
            third[1, :, :, :, 2 * z], third[1, :, :, :, 2 * z + 1] = -n, c
        final = third[:, :, g - 1, 0, : self.rows].reshape(2 * self.keep, self.rows)
        final = np.ascontiguousarray(np.broadcast_to(final.T[:, :, None], (*final.T.shape, 128)))
        third = third.reshape(2 * self.keep, self.count * 8)
        high, low = split_bf16(second)
        third = np.zeros((2, self.keep, g, self.slabs, 8), np.float32)
        for z in range(zl):
            c, n = cos[:, z::zl][:, :, None], sin[:, z::zl][:, :, None]
            third[0, :, :, :, 2 * z], third[0, :, :, :, 2 * z + 1] = c, n
            third[1, :, :, :, 2 * z], third[1, :, :, :, 2 * z + 1] = -n, c
        final = third[:, :, g - 1, 0, : self.rows].reshape(2 * self.keep, self.rows)
        final = np.ascontiguousarray(np.broadcast_to(final.T[:, :, None], (*final.T.shape, 128)))
        third = third.reshape(2 * self.keep, self.count * 8)
        high, low = split_bf16(second)
        kept = (self.order[0][0] * self.pens + self.order[0][1]) * ky_n
        near = np.zeros((self.slabs, ky_n, 2, yl, 128), np.float32)
        for s in range(self.slabs):
            for k in range(ky_n):
                near[s, k, 0] = cos[kept + k, s * yl : (s + 1) * yl, None]
                near[s, k, 1] = sin[kept + k, s * yl : (s + 1) * yl, None]
        return (
            np.stack(split_bf16(first)),
            np.concatenate([high, high, low], axis=2),
            np.stack(split_bf16(third[:, : (g - 1) * self.slabs * 8])),
            final,
        )


def kernel(
    plan, vel_hbm, vort_hbm, modes_hbm, first_hbm, second_hbm, third_hbm, final_hbm, out_ref,
    fields, modes, first, second, third, near, final, cross, quick, send, recv,
    field_sem, table_sem, late_sem, send_sem, recv_sem,
):
    sec, pen, slab = (lax.axis_index(a) for a in AXES)
    group = sec * plan.pens + pen
    me = group * plan.slabs + slab
    kind = group // (plan.groups - 1)
    is_last = kind == 1
    cells, keep = plan.cells, plan.keep
    for i, source in enumerate((vel_hbm, vort_hbm)):
        for c in range(3):
            pltpu.make_async_copy(source.at[c], fields.at[i, c], field_sem).start()
    table_loads = [
        pltpu.make_async_copy(first_hbm.at[0], first.at[0, 0:cells], table_sem.at[0]),
        pltpu.make_async_copy(first_hbm.at[1], first.at[1, 0:cells], table_sem.at[1]),
    ]
    late_loads = [
        pltpu.make_async_copy(second_hbm.at[slab], second, late_sem.at[0]),
        pltpu.make_async_copy(third_hbm, third, late_sem.at[1]),
        pltpu.make_async_copy(modes_hbm, modes, late_sem.at[2]),
        pltpu.make_async_copy(final_hbm, final, late_sem.at[3]),
    ]
    for load in table_loads:
        load.start()

    barrier = pltpu.get_barrier_semaphore()

    def place(to):
        return (to[0] * plan.pens + to[1]) * plan.slabs + to[2]

    for to in reversed(plan.order):

        @pl.when(me != place(to))
        def _(to=to):
            pl.semaphore_signal(
                barrier, inc=1, device_id=to, device_id_type=pl.DeviceIdType.MESH
            )

    if plan.rows < 8:
        recv[:, plan.rows : 8] = jnp.zeros((plan.count, 8 - plan.rows, 128), jnp.float32)
    cross[...] = jnp.zeros_like(cross)
    kept = plan.order[0][0] * plan.pens + plan.order[0][1]
    line = lax.broadcasted_iota(jnp.int32, (plan.y_rows, 128), 0) + slab * plan.y_rows
    for i in range(plan.rows_ky):
        wave = int(wave_numbers(keep)[kept * plan.rows_ky + i])
        angle = (wave * line % cells).astype(jnp.float32) * (2.0 * math.pi / cells)
        near[i, 0] = jnp.cos(angle) * (1.0 / math.sqrt(cells))
        near[i, 1] = jnp.sin(angle) * (1.0 / math.sqrt(cells))
    if cells < 128:
        for i in range(2):
            first[i, cells:128] = jnp.zeros((128 - cells, first.shape[2]), jnp.bfloat16)

    pltpu.make_async_copy(fields, fields, field_sem).wait()
    for load in late_loads:
        load.start()
    zl, yl = plan.z_rows, plan.y_rows
    area = zl * yl
    v, w = ([fields[i, c].reshape(area, cells) for c in range(3)] for i in range(2))
    for c in range(3):
        p, q = (c + 1) % 3, (c + 2) % 3
        cross[c * area : (c + 1) * area, 0:cells] = v[p] * w[q] - v[q] * w[p]
    for load in table_loads:
        load.wait()
    sub = lax.broadcasted_iota(jnp.int32, (8, 128), 0)
    blocks = []
    for i in range(plan.rows_ky):
        for c in range(3):
            block = None
            for z in range(zl):
                start = (c * zl + z) * yl
                pair = []
                for k in range(2):
                    terms = cross[start : start + yl] * near[i, k]
                    part = terms[0:8]
                    for r in range(8, yl, 8):
                        part = part + terms[r : r + 8]
                    pair.append(part)
                part = jnp.where(sub < 4, pair[0], pair[1]) + pltpu.roll(
                    jnp.where(sub < 4, pair[1], pair[0]), 4, 0
                )
                part = part + pltpu.roll(part, 6, 0)
                part = part + pltpu.roll(part, 7, 0)
                if z == 0:
                    block = part
                else:
                    block = jnp.where(sub % 4 == z, pltpu.roll(part, z, 0), block)
            blocks.append(block)
    high, low = split_in_kernel(jnp.concatenate(blocks, axis=0))
    planes = mm(
        jnp.concatenate([high, low, high], axis=1),
        jnp.concatenate([first[0], first[0], first[1]], axis=0),
    )
    cell = lax.broadcasted_iota(jnp.int32, (8, 2 * plan.wide), 1) % 128 // plan.block
    total = planes[0:8]
    for i in range(plan.rows_ky):
        for c in range(3):
            start = (i * 3 + c) * 8
            total = jnp.where(cell == c * plan.rows_ky + i, planes[start : start + 8], total)
    real, imag = total[:, : plan.wide], total[:, plan.wide :]
    parts = (real + pltpu.roll(imag, 4, 0), imag - pltpu.roll(real, 4, 0))
    for k in range(2):
        for s in range(plan.slabs):
            quick[pl.ds(s * 8 + k, zl, stride=2), :] = parts[k][0:zl, s * 128 : (s + 1) * 128]

    pl.semaphore_wait(barrier, plan.count - 1)
    used = pl.ds(0, plan.rows)

    def slot_of(s, g):
        return (s * plan.groups + g) * 8

    for s in range(plan.slabs):
        to = (*plan.order[0][:2], s)

        @pl.when(me != place(to))
        def _(to=to):
            pltpu.make_async_remote_copy(
                src_ref=quick.at[pl.ds(to[2] * 8, plan.rows)],
                dst_ref=recv.at[me, used],
                send_sem=send_sem,
                recv_sem=recv_sem.at[kind],
                device_id=to,
                device_id_type=pl.DeviceIdType.MESH,
            ).start()

    high, low = split_in_kernel(cross[...])
    along_x = mm(
        jnp.concatenate([high, low], axis=1), jnp.concatenate([first[0], first[0]], axis=0)
    ) + mm(high, first[1])
    late_loads[0].wait()
    slot = lax.broadcasted_iota(jnp.int32, (area, 2 * plan.wide), 1) % 128 // plan.width
    along_x = [along_x[c * area : (c + 1) * area] for c in range(3)]
    along_x = jnp.where(slot == 0, along_x[0], jnp.where(slot == 1, along_x[1], along_x[2]))
    high = along_x.astype(jnp.bfloat16).astype(jnp.float32)
    low = along_x - high
    upper = lax.broadcasted_iota(jnp.int32, (plan.groups, plan.wide), 1) % plan.width // plan.block
    for z in range(zl):
        parts = []
        for part in (high, low):
            piece = part[z * yl : (z + 1) * yl]
            parts.append(
                jnp.concatenate([piece[:, : plan.wide], piece[:, plan.wide :]], axis=0)
            )
        stack = jnp.concatenate([parts[0], parts[1], parts[0]], axis=0).astype(jnp.bfloat16)
        planes = mm(second[...], stack)
        for k in range(2):
            total = None
            for i in range(plan.rows_ky):
                start = (k * plan.rows_ky + i) * plan.groups
                piece = planes[start : start + plan.groups]
                total = piece if total is None else jnp.where(upper == i, piece, total)
            for s in range(plan.slabs):
                rows = pl.ds(s * plan.groups * 8 + 2 * z + k, plan.groups, stride=8)
                send[rows, :] = total[:, s * 128 : (s + 1) * 128]

    for to in plan.order[plan.slabs :]:

        @pl.when(me != place(to))
        def _(to=to):
            pltpu.make_async_remote_copy(
                src_ref=send.at[pl.ds(slot_of(to[2], to[0] * plan.pens + to[1]), plan.rows)],
                dst_ref=recv.at[me, used],
                send_sem=send_sem,
                recv_sem=recv_sem.at[kind],
                device_id=to,
                device_id_type=pl.DeviceIdType.MESH,
            ).start()

    own = pl.multiple_of(slot_of(slab, group), 8)
    recv[me, 0 : plan.rows] = send[pl.ds(own, plan.rows)]

    bm, ky_n, width = plan.block, plan.rows_ky, plan.width

    def signed(index):
        return jnp.where(index < keep // 2, index, index - keep)

    row = lax.broadcasted_iota(jnp.int32, (width, keep), 0)
    kx = signed(row % bm + slab * bm)
    ky = signed(row // bm + group * ky_n)
    kz = signed(lax.broadcasted_iota(jnp.int32, (width, keep), 1))
    limit = -(keep // 2)
    mask = ((kx != limit) & (ky != limit) & (kz != limit)).astype(jnp.float32)
    waves = [k.astype(jnp.float32) for k in (kx, ky, kz)]
    ksq = waves[0] * waves[0] + waves[1] * waves[1] + waves[2] * waves[2]
    inverse = 1.0 / jnp.maximum(ksq, 1.0)
    damp = (0.5 / (keep // 2) ** 2) * ksq
    for load in late_loads[1:]:
        load.wait()
    damped = [
        [
            jnp.concatenate([modes[c, i, k] for i in range(ky_n)], axis=0) * damp
            for k in range(2)
        ]
        for c in range(3)
    ]

    def landed(messages, sem):
        part = recv.at[pl.ds(0, messages), used]
        pltpu.make_async_copy(part, part, sem).wait()

    early = plan.count - plan.slabs

    @pl.when(is_last)
    def _():
        landed(early, recv_sem.at[0])

    @pl.when(jnp.logical_not(is_last))
    def _():
        landed(early - 1, recv_sem.at[0])

    got = split_in_kernel(recv[0:early].reshape(early * 8, 128))
    out = mm(third[0], jnp.concatenate(got, axis=1))
    out = out[:, :128] + out[:, 128:] + mm(third[1], got[0])

    @pl.when(is_last)
    def _():
        if plan.slabs > 1:
            landed(plan.slabs - 1, recv_sem.at[1])

    @pl.when(jnp.logical_not(is_last))
    def _():
        landed(plan.slabs, recv_sem.at[1])

    tail = recv[early]
    for s in range(1, plan.slabs):
        tail = tail + recv[early + s]
    for r in range(plan.rows):
        out = out + final[r] * tail[r : r + 1]
    for k in range(2):
        turned = jnp.transpose(out[k * keep : (k + 1) * keep])
        comp = [turned[c * width : (c + 1) * width] for c in range(3)]
        inner = (waves[0] * comp[0] + waves[1] * comp[1] + waves[2] * comp[2]) * inverse
        for c in range(3):
            result = (comp[c] - waves[c] * inner) * mask - damped[c][k]
            for i in range(ky_n):
                out_ref[c, i, k] = result[i * bm : (i + 1) * bm]
    landed(plan.count - 1, send_sem)


def direct(plan, tables, velocity, vorticity, velocity_modes):
    modes = jnp.transpose(velocity_modes, (0, 2, 3, 4, 1))
    first, second, third, final = tables
    hbm = pl.BlockSpec(memory_space=pltpu.HBM)
    out = pl.pallas_call(
        functools.partial(kernel, plan),
        out_shape=pltpu.VMEM(modes.shape, jnp.float32),
        in_specs=[hbm] * 7,
        out_specs=pl.BlockSpec(memory_space=pltpu.VMEM),
        scratch_shapes=[
            pltpu.VMEM((2,) + velocity.shape, jnp.float32),
            pltpu.VMEM(modes.shape, jnp.float32),
            pltpu.VMEM((2, 128, 2 * plan.wide), jnp.bfloat16),
            pltpu.VMEM(second.shape[1:], jnp.bfloat16),
            pltpu.VMEM(third.shape, jnp.bfloat16),
            pltpu.VMEM((plan.rows_ky, 2, plan.y_rows, 128), jnp.float32),
            pltpu.VMEM(final.shape, jnp.float32),
            pltpu.VMEM((3 * plan.z_rows * plan.y_rows, 128), jnp.float32),
            pltpu.VMEM((plan.slabs * 8, 128), jnp.float32),
            pltpu.VMEM((plan.slabs * plan.groups * 8, 128), jnp.float32),
            pltpu.VMEM((plan.count, 8, 128), jnp.float32),
            pltpu.SemaphoreType.DMA,
            pltpu.SemaphoreType.DMA((2,)),
            pltpu.SemaphoreType.DMA((4,)),
            pltpu.SemaphoreType.DMA,
            pltpu.SemaphoreType.DMA((2,)),
        ],
        compiler_params=pltpu.CompilerParams(collective_id=0, has_side_effects=True),
    )(velocity, vorticity, modes, first, second, third, final)
    return jnp.transpose(out, (0, 4, 1, 2, 3))


def solution(mesh):
    sizes = dict(mesh.shape)
    order = by_distance(mesh.devices)

    def run(velocity, vorticity, velocity_modes):
        _, z_rows, y_rows, cells = velocity.shape
        plan = Plan(sizes, order, cells, velocity_modes.shape[1], z_rows, y_rows)
        if not plan.fits():
            return per_device(velocity, vorticity, velocity_modes)
        return direct(plan, plan.tables(), velocity, vorticity, velocity_modes)

    return jax.shard_map(
        run,
        mesh=mesh,
        in_specs=(
            P(None, ("section", "pen"), "slab", None),
            P(None, ("section", "pen"), "slab", None),
            P(None, None, ("section", "pen"), None, "slab"),
        ),
        out_specs=P(None, None, ("section", "pen"), None, "slab"),
        check_vma=False,
    )
```

```python
import functools
import math

import jax
import jax.numpy as jnp
import numpy as np
from jax import lax
from jax.experimental import pallas as pl
from jax.experimental.pallas import tpu as pltpu
from jax.sharding import PartitionSpec as P

AXES = ("section", "pen", "slab")
highest = lax.Precision.HIGHEST


def signed_modes(index, count):
    return jnp.where(index < count // 2, index, index - count)


def discrete_fourier_tables(length, keep_count):
    modes = signed_modes(jnp.arange(keep_count, dtype=jnp.int32), keep_count)
    mode_positions = jnp.arange(length, dtype=jnp.int32)
    phase = jnp.remainder(modes[:, None] * mode_positions[None, :], length).astype(jnp.float32)
    angles = 2.0 * math.pi / length * phase
    factor = 1.0 / math.sqrt(length)
    return (jnp.cos(angles) * factor, jnp.sin(angles) * factor)


def complex_apply(form, cosine, sine, real_part, imag_part):
    out_real = jnp.einsum(form, cosine, real_part, precision=highest) + jnp.einsum(
        form, sine, imag_part, precision=highest
    )
    out_imag = jnp.einsum(form, cosine, imag_part, precision=highest) - jnp.einsum(
        form, sine, real_part, precision=highest
    )
    return (out_real, out_imag)


def per_device(velocity, vorticity, velocity_modes):
    grid_cells = velocity.shape[3]
    keep_count = velocity_modes.shape[1]
    cross_product = jnp.stack(
        [
            velocity[1] * vorticity[2] - velocity[2] * vorticity[1],
            velocity[2] * vorticity[0] - velocity[0] * vorticity[2],
            velocity[0] * vorticity[1] - velocity[1] * vorticity[0],
        ]
    )
    slabs = lax.axis_size("slab")
    block_modes = keep_count // slabs
    cosine_table, sine_table = discrete_fourier_tables(grid_cells, keep_count)
    cols_real = cosine_table.T.reshape(grid_cells, slabs, block_modes)
    cols_imag = (-sine_table).T.reshape(grid_cells, slabs, block_modes)
    column_table = jnp.stack([cols_real, cols_imag], axis=2).reshape(grid_cells, 2 * keep_count)
    first_pass = jnp.einsum("czyx,xj->czyj", cross_product, column_table, precision=highest)
    block = lax.all_to_all(first_pass, "slab", split_axis=3, concat_axis=2, tiled=True)
    out_real, out_imag = complex_apply(
        "ky,czyj->czkj",
        cosine_table,
        sine_table,
        block[..., :block_modes],
        block[..., block_modes:],
    )
    second_pass = jnp.concatenate([out_real, out_imag], axis=-1)
    halves = lax.axis_size("section")
    pens = lax.axis_size("pen")
    rows_ky = keep_count // (halves * pens)
    block = lax.all_to_all(second_pass, ("section", "pen"), split_axis=2, concat_axis=1, tiled=True)
    out_real, out_imag = complex_apply(
        "kz,czyj->ckyj",
        cosine_table,
        sine_table,
        block[..., :block_modes],
        block[..., block_modes:],
    )
    third_pass = jnp.concatenate([out_real, out_imag], axis=-1)
    group_index = lax.axis_index("section") * pens + lax.axis_index("pen")
    modes_z = signed_modes(jnp.arange(keep_count, dtype=jnp.int32), keep_count)[:, None, None]
    modes_y = signed_modes(
        group_index * rows_ky + jnp.arange(rows_ky, dtype=jnp.int32), keep_count
    )[None, :, None]
    modes_x = signed_modes(
        lax.axis_index("slab") * block_modes + jnp.arange(block_modes, dtype=jnp.int32), keep_count
    )[None, None, :]
    limit = -(keep_count // 2)
    keep_mask = ((modes_x != limit) & (modes_y != limit) & (modes_z != limit)).astype(jnp.float32)
    waves = (modes_x.astype(jnp.float32), modes_y.astype(jnp.float32), modes_z.astype(jnp.float32))
    ksq = waves[0] * waves[0] + waves[1] * waves[1] + waves[2] * waves[2]
    denom = jnp.maximum(ksq, 1.0)
    parts = []
    for which in range(2):
        chosen = third_pass[..., which * block_modes : (which + 1) * block_modes]
        comp = [chosen[c] for c in range(3)]
        inner = (waves[0] * comp[0] + waves[1] * comp[1] + waves[2] * comp[2]) / denom
        parts.append(jnp.stack([comp[c] - waves[c] * inner for c in range(3)]))
    projected = jnp.stack(parts, axis=3)
    visc = 0.5 / (keep_count // 2) ** 2
    return (
        projected * keep_mask[None, :, :, None, :]
        - visc * ksq[None, :, :, None, :] * velocity_modes
    )


def split_bf16(table):
    high = table.astype(jnp.bfloat16)
    low = (table - high.astype(np.float32)).astype(jnp.bfloat16)
    return high, low


def split_in_kernel(value):
    high = value.astype(jnp.bfloat16)
    low = (value - high.astype(jnp.float32)).astype(jnp.bfloat16)
    return high, low


def mm(a, b):
    return lax.dot_general(a, b, (((1,), (0,)), ((), ())), preferred_element_type=jnp.float32)


def split_dot(a, b):
    return mm(a[0], b[0]) + mm(a[1], b[0]) + mm(a[0], b[1])


def wave_numbers(count):
    index = np.arange(count)
    return np.where(index < count // 2, index, index - count)


def host_tables(cells, keep):
    phase = np.remainder(wave_numbers(keep)[:, None] * np.arange(cells)[None, :], cells)
    angles = 2.0 * np.pi / cells * phase
    factor = 1.0 / np.sqrt(cells)
    return np.cos(angles) * factor, np.sin(angles) * factor


def by_distance(devices):
    origin = getattr(devices.flat[0], "coords", ())

    def hops(index):
        return [abs(a - b) for a, b in zip(getattr(devices[index], "coords", ()), origin)]

    every = list(np.ndindex(devices.shape))
    spans = [max(far) for far in zip(*map(hops, every))]

    def key(index):
        far = hops(index)
        if sum(far) == 0:
            return -1, 0, index
        return (far[spans.index(max(spans))], -sum(far), index) if far else (0, 0, index)

    return sorted(every, key=key)


class Plan:
    def __init__(self, mesh_shape, order, cells, keep, z_rows, y_rows):
        self.order = order
        self.cells, self.keep, self.z_rows, self.y_rows = cells, keep, z_rows, y_rows
        self.halves, self.pens, self.slabs = (mesh_shape[a] for a in AXES)
        self.groups = self.halves * self.pens
        self.count = self.groups * self.slabs
        self.rows_ky = keep // self.groups
        self.block = keep // self.slabs
        self.width = self.rows_ky * self.block
        self.rows = 2 * z_rows
        self.wide = self.slabs * 128

    def fits(self):
        return (
            self.rows_ky * self.groups == self.keep
            and self.block * self.slabs == self.keep
            and 3 * self.width <= 128
            and 128 % self.width == 0
            and self.rows <= 8
            and self.cells <= 128
            and self.cells % 16 == 0
            and self.y_rows % 8 == 0
            and 6 * self.y_rows <= 256
            and self.groups % 8 == 0
            and self.keep % 8 == 0
            and self.block % 8 == 0
            and 3 * self.z_rows * self.y_rows <= 512
            and 2 <= self.count <= 64
        )

    def tables(self):
        cos, sin = host_tables(self.cells, self.keep)
        g, zl, yl, ky_n = self.groups, self.z_rows, self.y_rows, self.rows_ky
        second = np.zeros((self.slabs, 2, ky_n, g, 2, yl), np.float32)
        for s in range(self.slabs):
            for k in range(ky_n):
                c = cos[k::ky_n, s * yl : (s + 1) * yl]
                n = sin[k::ky_n, s * yl : (s + 1) * yl]
                second[s, 0, k, :, 0], second[s, 0, k, :, 1] = c, n
                second[s, 1, k, :, 0], second[s, 1, k, :, 1] = -n, c
        second = second.reshape(self.slabs, 2 * self.keep, 2 * yl)
        third = np.zeros((2, self.keep, g, self.slabs, 8), np.float32)
        for z in range(zl):
            c, n = cos[:, z::zl][:, :, None], sin[:, z::zl][:, :, None]
            third[0, :, :, :, 2 * z], third[0, :, :, :, 2 * z + 1] = c, n
            third[1, :, :, :, 2 * z], third[1, :, :, :, 2 * z + 1] = -n, c
        final = third[:, :, g - 1, 0, : self.rows].reshape(2 * self.keep, self.rows)
        final = np.ascontiguousarray(np.broadcast_to(final.T[:, :, None], (*final.T.shape, 128)))
        third = third.reshape(2 * self.keep, self.count * 8)
        high, low = split_bf16(second)
        third = np.zeros((2, self.keep, g, self.slabs, 8), np.float32)
        for z in range(zl):
            c, n = cos[:, z::zl][:, :, None], sin[:, z::zl][:, :, None]
            third[0, :, :, :, 2 * z], third[0, :, :, :, 2 * z + 1] = c, n
            third[1, :, :, :, 2 * z], third[1, :, :, :, 2 * z + 1] = -n, c
        final = third[:, :, g - 1, 0, : self.rows].reshape(2 * self.keep, self.rows)
        final = np.ascontiguousarray(np.broadcast_to(final.T[:, :, None], (*final.T.shape, 128)))
        third = third.reshape(2 * self.keep, self.count * 8)
        high, low = split_bf16(second)
        kept = (self.order[0][0] * self.pens + self.order[0][1]) * ky_n
        near = np.zeros((self.slabs, ky_n, 2, yl, 128), np.float32)
        for s in range(self.slabs):
            for k in range(ky_n):
                near[s, k, 0] = cos[kept + k, s * yl : (s + 1) * yl, None]
                near[s, k, 1] = sin[kept + k, s * yl : (s + 1) * yl, None]
        return (
            np.concatenate([high, high, low], axis=2),
            np.stack(split_bf16(third[:, : (g - 1) * self.slabs * 8])),
            final,
        )


def kernel(
    plan, vel_hbm, vort_hbm, modes_hbm, second_hbm, third_hbm, final_hbm, out_ref,
    fields, modes, first, second, third, near, final, cross, quick, send, recv,
    field_sem, late_sem, send_sem, recv_sem,
):
    sec, pen, slab = (lax.axis_index(a) for a in AXES)
    group = sec * plan.pens + pen
    me = group * plan.slabs + slab
    kind = group // (plan.groups - 1)
    is_last = kind == 1
    cells, keep = plan.cells, plan.keep
    for i, source in enumerate((vel_hbm, vort_hbm)):
        for c in range(3):
            pltpu.make_async_copy(source.at[c], fields.at[i, c], field_sem).start()
    late_loads = [
        pltpu.make_async_copy(second_hbm.at[slab], second, late_sem.at[0]),
        pltpu.make_async_copy(third_hbm, third, late_sem.at[1]),
        pltpu.make_async_copy(modes_hbm, modes, late_sem.at[2]),
        pltpu.make_async_copy(final_hbm, final, late_sem.at[3]),
    ]

    barrier = pltpu.get_barrier_semaphore()

    def signed(index):
        return jnp.where(index < keep // 2, index, index - keep)

    def place(to):
        return (to[0] * plan.pens + to[1]) * plan.slabs + to[2]

    for to in plan.order:

        @pl.when(me != place(to))
        def _(to=to):
            pl.semaphore_signal(
                barrier, inc=1, device_id=to, device_id_type=pl.DeviceIdType.MESH
            )

    if plan.rows < 8:
        recv[:, plan.rows : 8] = jnp.zeros((plan.count, 8 - plan.rows, 128), jnp.float32)
    cross[...] = jnp.zeros_like(cross)
    scale = 1.0 / math.sqrt(cells)

    def turn(wave, cell):
        product = wave * cell
        product = product - cells * jnp.floor(product * (1.0 / cells) + 0.5)
        angle = product * (2.0 * math.pi / cells)
        return jnp.cos(angle) * scale, jnp.sin(angle) * scale

    def ramp(shape, axis):
        return lax.broadcasted_iota(jnp.int32, shape, axis)

    kept = plan.order[0][0] * plan.pens + plan.order[0][1]
    line = (ramp((plan.y_rows, 128), 0) + slab * plan.y_rows).astype(jnp.float32)
    waves_near = [float(wave_numbers(keep)[kept * plan.rows_ky + i]) for i in range(plan.rows_ky)]
    for i in range(plan.rows_ky):
        if waves_near[i] != 0:
            near[i, 0], near[i, 1] = turn(waves_near[i], line)
    lane = ramp((cells, 128), 1)
    line = ramp((cells, 128), 0).astype(jnp.float32)
    for s in range(plan.slabs):
        wave = signed(lane % plan.block + s * plan.block).astype(jnp.float32)
        cosine, sine = turn(wave, line)
        for k, table in enumerate((cosine, -sine)):
            table = split_in_kernel(jnp.where(lane < 3 * plan.width, table, 0.0))
            start = k * plan.wide + s * 128
            for i in range(2):
                first[i, 0:cells, start : start + 128] = table[i]
    if cells < 128:
        for i in range(2):
            first[i, cells:128] = jnp.zeros((128 - cells, first.shape[2]), jnp.bfloat16)

    pltpu.make_async_copy(fields, fields, field_sem).wait()
    for load in late_loads:
        load.start()
    zl, yl = plan.z_rows, plan.y_rows
    area = zl * yl
    v, w = ([fields[i, c].reshape(area, cells) for c in range(3)] for i in range(2))
    for c in range(3):
        p, q = (c + 1) % 3, (c + 2) % 3
        cross[c * area : (c + 1) * area, 0:cells] = v[p] * w[q] - v[q] * w[p]
    sub = lax.broadcasted_iota(jnp.int32, (8, 128), 0)

    def folded(terms):
        part = terms[0:8]
        for r in range(8, yl, 8):
            part = part + terms[r : r + 8]
        return part

    blocks = []
    for i in range(plan.rows_ky):
        for c in range(3):
            sums = []
            for z in range(zl):
                start = (c * zl + z) * yl
                line = cross[start : start + yl]
                if waves_near[i] == 0:
                    part = folded(line)
                    part = part + pltpu.roll(part, 4, 0)
                else:
                    pair = [folded(line * near[i, k]) for k in range(2)]
                    part = jnp.where(sub < 4, pair[0], pair[1]) + pltpu.roll(
                        jnp.where(sub < 4, pair[1], pair[0]), 4, 0
                    )
                sums.append(part + pltpu.roll(part, 2 if z // 2 % 2 else 6, 0))
            even, odd = None, None
            for z in range(0, zl, 2):
                even = sums[z] if even is None else jnp.where(sub % 4 < 2, even, sums[z])
            for z in range(1, zl, 2):
                odd = sums[z] if odd is None else jnp.where(sub % 4 < 2, odd, sums[z])
            block = even + pltpu.roll(even, 7, 0)
            if odd is not None:
                block = jnp.where(sub % 2 == 0, block, odd + pltpu.roll(odd, 1, 0))
            if waves_near[i] == 0:
                block = jnp.where(sub < 4, block * scale, 0.0)
            blocks.append(block)
    high, low = split_in_kernel(jnp.concatenate(blocks, axis=0))
    planes = mm(
        jnp.concatenate([high, low, high], axis=1),
        jnp.concatenate([first[0], first[0], first[1]], axis=0),
    )
    cell = lax.broadcasted_iota(jnp.int32, (8, 2 * plan.wide), 1) % 128 // plan.block
    total = planes[0:8]
    for i in range(plan.rows_ky):
        for c in range(3):
            start = (i * 3 + c) * 8
            total = jnp.where(cell == c * plan.rows_ky + i, planes[start : start + 8], total)
    real, imag = total[:, : plan.wide], total[:, plan.wide :]
    parts = (real + pltpu.roll(imag, 4, 0), imag - pltpu.roll(real, 4, 0))
    for k in range(2):
        for s in range(plan.slabs):
            quick[pl.ds(s * 8 + k, zl, stride=2), :] = parts[k][0:zl, s * 128 : (s + 1) * 128]

    used = pl.ds(0, plan.rows)

    def slot_of(s, g):
        return (s * plan.groups + g) * 8

    def open_with_near():
        pl.semaphore_wait(barrier, plan.count - 1)
        for s in range(plan.slabs):
            to = (*plan.order[0][:2], s)

            @pl.when(me != place(to))
            def _(to=to):
                pltpu.make_async_remote_copy(
                    src_ref=quick.at[pl.ds(to[2] * 8, plan.rows)],
                    dst_ref=recv.at[me, used],
                    send_sem=send_sem,
                    recv_sem=recv_sem.at[kind],
                    device_id=to,
                    device_id_type=pl.DeviceIdType.MESH,
                ).start()

    @pl.when(is_last)
    def _():
        open_with_near()

    high, low = split_in_kernel(cross[...])
    along_x = mm(
        jnp.concatenate([high, low], axis=1), jnp.concatenate([first[0], first[0]], axis=0)
    ) + mm(high, first[1])
    late_loads[0].wait()
    slot = lax.broadcasted_iota(jnp.int32, (area, 2 * plan.wide), 1) % 128 // plan.width
    along_x = [along_x[c * area : (c + 1) * area] for c in range(3)]
    along_x = jnp.where(slot == 0, along_x[0], jnp.where(slot == 1, along_x[1], along_x[2]))
    high = along_x.astype(jnp.bfloat16).astype(jnp.float32)
    low = along_x - high
    upper = lax.broadcasted_iota(jnp.int32, (plan.groups, plan.wide), 1) % plan.width // plan.block
    for z in range(zl):
        parts = []
        for part in (high, low):
            piece = part[z * yl : (z + 1) * yl]
            parts.append(
                jnp.concatenate([piece[:, : plan.wide], piece[:, plan.wide :]], axis=0)
            )
        stack = jnp.concatenate([parts[0], parts[1], parts[0]], axis=0).astype(jnp.bfloat16)
        planes = mm(second[...], stack)
        for k in range(2):
            total = None
            for i in range(plan.rows_ky):
                start = (k * plan.rows_ky + i) * plan.groups
                piece = planes[start : start + plan.groups]
                total = piece if total is None else jnp.where(upper == i, piece, total)
            for s in range(plan.slabs):
                rows = pl.ds(s * plan.groups * 8 + 2 * z + k, plan.groups, stride=8)
                send[rows, :] = total[:, s * 128 : (s + 1) * 128]

    @pl.when(jnp.logical_not(is_last))
    def _():
        open_with_near()

    for to in plan.order[plan.slabs :]:

        @pl.when(me != place(to))
        def _(to=to):
            pltpu.make_async_remote_copy(
                src_ref=send.at[pl.ds(slot_of(to[2], to[0] * plan.pens + to[1]), plan.rows)],
                dst_ref=recv.at[me, used],
                send_sem=send_sem,
                recv_sem=recv_sem.at[kind],
                device_id=to,
                device_id_type=pl.DeviceIdType.MESH,
            ).start()

    own = pl.multiple_of(slot_of(slab, group), 8)
    recv[me, 0 : plan.rows] = send[pl.ds(own, plan.rows)]

    bm, ky_n, width = plan.block, plan.rows_ky, plan.width

    row = lax.broadcasted_iota(jnp.int32, (width, keep), 0)
    kx = signed(row % bm + slab * bm)
    ky = signed(row // bm + group * ky_n)
    kz = signed(lax.broadcasted_iota(jnp.int32, (width, keep), 1))
    limit = -(keep // 2)
    mask = ((kx != limit) & (ky != limit) & (kz != limit)).astype(jnp.float32)
    waves = [k.astype(jnp.float32) for k in (kx, ky, kz)]
    ksq = waves[0] * waves[0] + waves[1] * waves[1] + waves[2] * waves[2]
    inverse = 1.0 / jnp.maximum(ksq, 1.0)
    damp = (0.5 / (keep // 2) ** 2) * ksq
    for load in late_loads[1:]:
        load.wait()
    damped = [
        [
            jnp.concatenate([modes[c, i, k] for i in range(ky_n)], axis=0) * damp
            for k in range(2)
        ]
        for c in range(3)
    ]

    def landed(messages, sem):
        part = recv.at[pl.ds(0, messages), used]
        pltpu.make_async_copy(part, part, sem).wait()

    early = plan.count - plan.slabs

    @pl.when(is_last)
    def _():
        landed(early, recv_sem.at[0])

    @pl.when(jnp.logical_not(is_last))
    def _():
        landed(early - 1, recv_sem.at[0])

    got = split_in_kernel(recv[0:early].reshape(early * 8, 128))
    out = mm(third[0], jnp.concatenate(got, axis=1))
    out = out[:, :128] + out[:, 128:] + mm(third[1], got[0])

    @pl.when(is_last)
    def _():
        if plan.slabs > 1:
            landed(plan.slabs - 1, recv_sem.at[1])

    @pl.when(jnp.logical_not(is_last))
    def _():
        landed(plan.slabs, recv_sem.at[1])

    tail = recv[early]
    for s in range(1, plan.slabs):
        tail = tail + recv[early + s]
    for r in range(plan.rows):
        out = out + final[r] * tail[r : r + 1]
    for k in range(2):
        turned = jnp.transpose(out[k * keep : (k + 1) * keep])
        comp = [turned[c * width : (c + 1) * width] for c in range(3)]
        inner = (waves[0] * comp[0] + waves[1] * comp[1] + waves[2] * comp[2]) * inverse
        for c in range(3):
            result = (comp[c] - waves[c] * inner) * mask - damped[c][k]
            for i in range(ky_n):
                out_ref[c, i, k] = result[i * bm : (i + 1) * bm]
    landed(plan.count - 1, send_sem)


def direct(plan, tables, velocity, vorticity, velocity_modes):
    modes = jnp.transpose(velocity_modes, (0, 2, 3, 4, 1))
    second, third, final = tables
    hbm = pl.BlockSpec(memory_space=pltpu.HBM)
    out = pl.pallas_call(
        functools.partial(kernel, plan),
        out_shape=pltpu.VMEM(modes.shape, jnp.float32),
        in_specs=[hbm] * 6,
        out_specs=pl.BlockSpec(memory_space=pltpu.VMEM),
        scratch_shapes=[
            pltpu.VMEM((2,) + velocity.shape, jnp.float32),
            pltpu.VMEM(modes.shape, jnp.float32),
            pltpu.VMEM((2, 128, 2 * plan.wide), jnp.bfloat16),
            pltpu.VMEM(second.shape[1:], jnp.bfloat16),
            pltpu.VMEM(third.shape, jnp.bfloat16),
            pltpu.VMEM((plan.rows_ky, 2, plan.y_rows, 128), jnp.float32),
            pltpu.VMEM(final.shape, jnp.float32),
            pltpu.VMEM((3 * plan.z_rows * plan.y_rows, 128), jnp.float32),
            pltpu.VMEM((plan.slabs * 8, 128), jnp.float32),
            pltpu.VMEM((plan.slabs * plan.groups * 8, 128), jnp.float32),
            pltpu.VMEM((plan.count, 8, 128), jnp.float32),
            pltpu.SemaphoreType.DMA,
            pltpu.SemaphoreType.DMA((4,)),
            pltpu.SemaphoreType.DMA,
            pltpu.SemaphoreType.DMA((2,)),
        ],
        compiler_params=pltpu.CompilerParams(collective_id=0, has_side_effects=True),
    )(velocity, vorticity, modes, second, third, final)
    return jnp.transpose(out, (0, 4, 1, 2, 3))


def solution(mesh):
    sizes = dict(mesh.shape)
    order = by_distance(mesh.devices)

    def run(velocity, vorticity, velocity_modes):
        _, z_rows, y_rows, cells = velocity.shape
        plan = Plan(sizes, order, cells, velocity_modes.shape[1], z_rows, y_rows)
        if not plan.fits():
            return per_device(velocity, vorticity, velocity_modes)
        return direct(plan, plan.tables(), velocity, vorticity, velocity_modes)

    return jax.shard_map(
        run,
        mesh=mesh,
        in_specs=(
            P(None, ("section", "pen"), "slab", None),
            P(None, ("section", "pen"), "slab", None),
            P(None, None, ("section", "pen"), None, "slab"),
        ),
        out_specs=P(None, None, ("section", "pen"), None, "slab"),
        check_vma=False,
    )
```

```python
import functools
import math

import jax
import jax.numpy as jnp
import numpy as np
from jax import lax
from jax.experimental import pallas as pl
from jax.experimental.pallas import tpu as pltpu
from jax.sharding import PartitionSpec as P

AXES = ("section", "pen", "slab")
highest = lax.Precision.HIGHEST


def signed_modes(index, count):
    return jnp.where(index < count // 2, index, index - count)


def discrete_fourier_tables(length, keep_count):
    modes = signed_modes(jnp.arange(keep_count, dtype=jnp.int32), keep_count)
    mode_positions = jnp.arange(length, dtype=jnp.int32)
    phase = jnp.remainder(modes[:, None] * mode_positions[None, :], length).astype(jnp.float32)
    angles = 2.0 * math.pi / length * phase
    factor = 1.0 / math.sqrt(length)
    return (jnp.cos(angles) * factor, jnp.sin(angles) * factor)


def complex_apply(form, cosine, sine, real_part, imag_part):
    out_real = jnp.einsum(form, cosine, real_part, precision=highest) + jnp.einsum(
        form, sine, imag_part, precision=highest
    )
    out_imag = jnp.einsum(form, cosine, imag_part, precision=highest) - jnp.einsum(
        form, sine, real_part, precision=highest
    )
    return (out_real, out_imag)


def per_device(velocity, vorticity, velocity_modes):
    grid_cells = velocity.shape[3]
    keep_count = velocity_modes.shape[1]
    cross_product = jnp.stack(
        [
            velocity[1] * vorticity[2] - velocity[2] * vorticity[1],
            velocity[2] * vorticity[0] - velocity[0] * vorticity[2],
            velocity[0] * vorticity[1] - velocity[1] * vorticity[0],
        ]
    )
    slabs = lax.axis_size("slab")
    block_modes = keep_count // slabs
    cosine_table, sine_table = discrete_fourier_tables(grid_cells, keep_count)
    cols_real = cosine_table.T.reshape(grid_cells, slabs, block_modes)
    cols_imag = (-sine_table).T.reshape(grid_cells, slabs, block_modes)
    column_table = jnp.stack([cols_real, cols_imag], axis=2).reshape(grid_cells, 2 * keep_count)
    first_pass = jnp.einsum("czyx,xj->czyj", cross_product, column_table, precision=highest)
    block = lax.all_to_all(first_pass, "slab", split_axis=3, concat_axis=2, tiled=True)
    out_real, out_imag = complex_apply(
        "ky,czyj->czkj",
        cosine_table,
        sine_table,
        block[..., :block_modes],
        block[..., block_modes:],
    )
    second_pass = jnp.concatenate([out_real, out_imag], axis=-1)
    halves = lax.axis_size("section")
    pens = lax.axis_size("pen")
    rows_ky = keep_count // (halves * pens)
    block = lax.all_to_all(second_pass, ("section", "pen"), split_axis=2, concat_axis=1, tiled=True)
    out_real, out_imag = complex_apply(
        "kz,czyj->ckyj",
        cosine_table,
        sine_table,
        block[..., :block_modes],
        block[..., block_modes:],
    )
    third_pass = jnp.concatenate([out_real, out_imag], axis=-1)
    group_index = lax.axis_index("section") * pens + lax.axis_index("pen")
    modes_z = signed_modes(jnp.arange(keep_count, dtype=jnp.int32), keep_count)[:, None, None]
    modes_y = signed_modes(
        group_index * rows_ky + jnp.arange(rows_ky, dtype=jnp.int32), keep_count
    )[None, :, None]
    modes_x = signed_modes(
        lax.axis_index("slab") * block_modes + jnp.arange(block_modes, dtype=jnp.int32), keep_count
    )[None, None, :]
    limit = -(keep_count // 2)
    keep_mask = ((modes_x != limit) & (modes_y != limit) & (modes_z != limit)).astype(jnp.float32)
    waves = (modes_x.astype(jnp.float32), modes_y.astype(jnp.float32), modes_z.astype(jnp.float32))
    ksq = waves[0] * waves[0] + waves[1] * waves[1] + waves[2] * waves[2]
    denom = jnp.maximum(ksq, 1.0)
    parts = []
    for which in range(2):
        chosen = third_pass[..., which * block_modes : (which + 1) * block_modes]
        comp = [chosen[c] for c in range(3)]
        inner = (waves[0] * comp[0] + waves[1] * comp[1] + waves[2] * comp[2]) / denom
        parts.append(jnp.stack([comp[c] - waves[c] * inner for c in range(3)]))
    projected = jnp.stack(parts, axis=3)
    visc = 0.5 / (keep_count // 2) ** 2
    return (
        projected * keep_mask[None, :, :, None, :]
        - visc * ksq[None, :, :, None, :] * velocity_modes
    )


def split_bf16(table):
    high = table.astype(jnp.bfloat16)
    low = (table - high.astype(np.float32)).astype(jnp.bfloat16)
    return high, low


def split_in_kernel(value):
    high = value.astype(jnp.bfloat16)
    low = (value - high.astype(jnp.float32)).astype(jnp.bfloat16)
    return high, low


def mm(a, b):
    return lax.dot_general(a, b, (((1,), (0,)), ((), ())), preferred_element_type=jnp.float32)


def split_dot(a, b):
    return mm(a[0], b[0]) + mm(a[1], b[0]) + mm(a[0], b[1])


def wave_numbers(count):
    index = np.arange(count)
    return np.where(index < count // 2, index, index - count)


def host_tables(cells, keep):
    phase = np.remainder(wave_numbers(keep)[:, None] * np.arange(cells)[None, :], cells)
    angles = 2.0 * np.pi / cells * phase
    factor = 1.0 / np.sqrt(cells)
    return np.cos(angles) * factor, np.sin(angles) * factor


def by_distance(devices):
    origin = getattr(devices.flat[0], "coords", ())

    def hops(index):
        return [abs(a - b) for a, b in zip(getattr(devices[index], "coords", ()), origin)]

    every = list(np.ndindex(devices.shape))
    spans = [max(far) for far in zip(*map(hops, every))]

    def key(index):
        far = hops(index)
        if sum(far) == 0:
            return -1, 0, index
        return (far[spans.index(max(spans))], -sum(far), index) if far else (0, 0, index)

    return sorted(every, key=key)


class Plan:
    def __init__(self, mesh_shape, order, cells, keep, z_rows, y_rows):
        self.order = order
        self.cells, self.keep, self.z_rows, self.y_rows = cells, keep, z_rows, y_rows
        self.halves, self.pens, self.slabs = (mesh_shape[a] for a in AXES)
        self.groups = self.halves * self.pens
        self.count = self.groups * self.slabs
        self.rows_ky = keep // self.groups
        self.block = keep // self.slabs
        self.width = self.rows_ky * self.block
        self.rows = 2 * z_rows
        self.wide = self.slabs * 128

    def fits(self):
        return (
            self.rows_ky * self.groups == self.keep
            and self.block * self.slabs == self.keep
            and 3 * self.width <= 128
            and 128 % self.width == 0
            and self.rows <= 8
            and self.cells <= 128
            and self.cells % 16 == 0
            and self.y_rows % 8 == 0
            and 6 * self.y_rows <= 256
            and self.groups % 8 == 0
            and self.keep % 8 == 0
            and self.block % 8 == 0
            and 3 * self.z_rows * self.y_rows <= 512
            and 2 <= self.count <= 64
        )

    def tables(self):
        cos, sin = host_tables(self.cells, self.keep)
        g, zl = self.groups, self.z_rows
        table = np.zeros((2, self.keep, g, self.slabs, 8), np.float32)
        for z in range(zl):
            c, n = cos[:, z::zl][:, :, None], sin[:, z::zl][:, :, None]
            table[0, :, :, :, 2 * z], table[0, :, :, :, 2 * z + 1] = c, n
            table[1, :, :, :, 2 * z], table[1, :, :, :, 2 * z + 1] = -n, c
        early = table[:, :, : g - 1].reshape(2 * self.keep, (g - 1) * self.slabs * 8)
        last = table[:, :, g - 1, 0, : self.rows].reshape(2 * self.keep, self.rows).T
        last = np.broadcast_to(last[:, :, None], (*last.shape, 128))
        return np.stack(split_bf16(early)), np.ascontiguousarray(last)


def kernel(
    plan, vel_hbm, vort_hbm, modes_hbm, third_hbm, final_hbm, out_ref,
    fields, modes, first, second, third, near, final, cross, quick, send, recv,
    field_sem, late_sem, send_sem, recv_sem,
):
    sec, pen, slab = (lax.axis_index(a) for a in AXES)
    group = sec * plan.pens + pen
    me = group * plan.slabs + slab
    kind = group // (plan.groups - 1)
    is_last = kind == 1
    cells, keep = plan.cells, plan.keep
    for i, source in enumerate((vel_hbm, vort_hbm)):
        for c in range(3):
            pltpu.make_async_copy(source.at[c], fields.at[i, c], field_sem).start()
    late_loads = [
        pltpu.make_async_copy(third_hbm, third, late_sem.at[0]),
        pltpu.make_async_copy(modes_hbm, modes, late_sem.at[1]),
        pltpu.make_async_copy(final_hbm, final, late_sem.at[2]),
    ]

    barrier = pltpu.get_barrier_semaphore()

    def signed(index):
        return jnp.where(index < keep // 2, index, index - keep)

    def place(to):
        return (to[0] * plan.pens + to[1]) * plan.slabs + to[2]

    for to in plan.order:

        @pl.when(me != place(to))
        def _(to=to):
            pl.semaphore_signal(
                barrier, inc=1, device_id=to, device_id_type=pl.DeviceIdType.MESH
            )

    if plan.rows < 8:
        recv[:, plan.rows : 8] = jnp.zeros((plan.count, 8 - plan.rows, 128), jnp.float32)
    cross[...] = jnp.zeros_like(cross)
    scale = 1.0 / math.sqrt(cells)

    def turn(wave, cell):
        product = wave * cell
        product = product - cells * jnp.floor(product * (1.0 / cells) + 0.5)
        angle = product * (2.0 * math.pi / cells)
        return jnp.cos(angle) * scale, jnp.sin(angle) * scale

    def ramp(shape, axis):
        return lax.broadcasted_iota(jnp.int32, shape, axis)

    kept = plan.order[0][0] * plan.pens + plan.order[0][1]
    line = (ramp((plan.y_rows, 128), 0) + slab * plan.y_rows).astype(jnp.float32)
    waves_near = [float(wave_numbers(keep)[kept * plan.rows_ky + i]) for i in range(plan.rows_ky)]
    for i in range(plan.rows_ky):
        if waves_near[i] != 0:
            near[i, 0], near[i, 1] = turn(waves_near[i], line)
    lane = ramp((cells, 128), 1)
    line = ramp((cells, 128), 0).astype(jnp.float32)
    for s in range(plan.slabs):
        wave = signed(lane % plan.block + s * plan.block).astype(jnp.float32)
        cosine, sine = turn(wave, line)
        for k, table in enumerate((cosine, -sine)):
            table = split_in_kernel(jnp.where(lane < 3 * plan.width, table, 0.0))
            start = k * plan.wide + s * 128
            for i in range(2):
                first[i, 0:cells, start : start + 128] = table[i]
    shape = (keep, 6 * plan.y_rows)
    row = ramp(shape, 0)
    wave = signed(row % plan.groups * plan.rows_ky + row // plan.groups).astype(jnp.float32)
    line = ramp(shape, 1).astype(jnp.float32)
    part = jnp.floor((line + 0.5) * (1.0 / plan.y_rows))
    line = line - part * plan.y_rows
    cosine, sine = turn(wave, line + (slab * plan.y_rows).astype(jnp.float32))
    real = (part == 0) | (part == 2) | (part == 4)
    for k, table in enumerate((jnp.where(real, cosine, sine), jnp.where(real, -sine, cosine))):
        table_high = table.astype(jnp.bfloat16).astype(jnp.float32)
        table = jnp.where(part < 4, table_high, table - table_high)
        second[k * keep : (k + 1) * keep] = table.astype(jnp.bfloat16)
    if cells < 128:
        for i in range(2):
            first[i, cells:128] = jnp.zeros((128 - cells, first.shape[2]), jnp.bfloat16)

    pltpu.make_async_copy(fields, fields, field_sem).wait()
    for load in late_loads:
        load.start()
    zl, yl = plan.z_rows, plan.y_rows
    area = zl * yl
    v, w = ([fields[i, c].reshape(area, cells) for c in range(3)] for i in range(2))
    for c in range(3):
        p, q = (c + 1) % 3, (c + 2) % 3
        cross[c * area : (c + 1) * area, 0:cells] = v[p] * w[q] - v[q] * w[p]
    sub = lax.broadcasted_iota(jnp.int32, (8, 128), 0)

    def folded(terms):
        part = terms[0:8]
        for r in range(8, yl, 8):
            part = part + terms[r : r + 8]
        return part

    blocks = []
    for i in range(plan.rows_ky):
        for c in range(3):
            sums = []
            for z in range(zl):
                start = (c * zl + z) * yl
                line = cross[start : start + yl]
                if waves_near[i] == 0:
                    part = folded(line)
                    part = part + pltpu.roll(part, 4, 0)
                else:
                    pair = [folded(line * near[i, k]) for k in range(2)]
                    part = jnp.where(sub < 4, pair[0], pair[1]) + pltpu.roll(
                        jnp.where(sub < 4, pair[1], pair[0]), 4, 0
                    )
                sums.append(part + pltpu.roll(part, 2 if z // 2 % 2 else 6, 0))
            even, odd = None, None
            for z in range(0, zl, 2):
                even = sums[z] if even is None else jnp.where(sub % 4 < 2, even, sums[z])
            for z in range(1, zl, 2):
                odd = sums[z] if odd is None else jnp.where(sub % 4 < 2, odd, sums[z])
            block = even + pltpu.roll(even, 7, 0)
            if odd is not None:
                block = jnp.where(sub % 2 == 0, block, odd + pltpu.roll(odd, 1, 0))
            if waves_near[i] == 0:
                block = jnp.where(sub < 4, block * scale, 0.0)
            blocks.append(block)
    high, low = split_in_kernel(jnp.concatenate(blocks, axis=0))
    planes = mm(
        jnp.concatenate([high, low, high], axis=1),
        jnp.concatenate([first[0], first[0], first[1]], axis=0),
    )
    cell = lax.broadcasted_iota(jnp.int32, (8, 2 * plan.wide), 1) % 128 // plan.block
    total = planes[0:8]
    for i in range(plan.rows_ky):
        for c in range(3):
            start = (i * 3 + c) * 8
            total = jnp.where(cell == c * plan.rows_ky + i, planes[start : start + 8], total)
    real, imag = total[:, : plan.wide], total[:, plan.wide :]
    parts = (real + pltpu.roll(imag, 4, 0), imag - pltpu.roll(real, 4, 0))
    for k in range(2):
        for s in range(plan.slabs):
            quick[pl.ds(s * 8 + k, zl, stride=2), :] = parts[k][0:zl, s * 128 : (s + 1) * 128]

    used = pl.ds(0, plan.rows)

    def slot_of(s, g):
        return (s * plan.groups + g) * 8

    def open_with_near():
        pl.semaphore_wait(barrier, plan.count - 1)
        for s in range(plan.slabs):
            to = (*plan.order[0][:2], s)

            @pl.when(me != place(to))
            def _(to=to):
                pltpu.make_async_remote_copy(
                    src_ref=quick.at[pl.ds(to[2] * 8, plan.rows)],
                    dst_ref=recv.at[me, used],
                    send_sem=send_sem,
                    recv_sem=recv_sem.at[kind],
                    device_id=to,
                    device_id_type=pl.DeviceIdType.MESH,
                ).start()

    @pl.when(is_last)
    def _():
        open_with_near()

    high, low = split_in_kernel(cross[...])
    along_x = mm(
        jnp.concatenate([high, low], axis=1), jnp.concatenate([first[0], first[0]], axis=0)
    ) + mm(high, first[1])
    slot = lax.broadcasted_iota(jnp.int32, (area, 2 * plan.wide), 1) % 128 // plan.width
    along_x = [along_x[c * area : (c + 1) * area] for c in range(3)]
    along_x = jnp.where(slot == 0, along_x[0], jnp.where(slot == 1, along_x[1], along_x[2]))
    high = along_x.astype(jnp.bfloat16).astype(jnp.float32)
    low = along_x - high
    upper = lax.broadcasted_iota(jnp.int32, (plan.groups, plan.wide), 1) % plan.width // plan.block
    for z in range(zl):
        parts = []
        for part in (high, low):
            piece = part[z * yl : (z + 1) * yl]
            parts.append(
                jnp.concatenate([piece[:, : plan.wide], piece[:, plan.wide :]], axis=0)
            )
        stack = jnp.concatenate([parts[0], parts[1], parts[0]], axis=0).astype(jnp.bfloat16)
        planes = mm(second[...], stack)
        for k in range(2):
            total = None
            for i in range(plan.rows_ky):
                start = (k * plan.rows_ky + i) * plan.groups
                piece = planes[start : start + plan.groups]
                total = piece if total is None else jnp.where(upper == i, piece, total)
            for s in range(plan.slabs):
                rows = pl.ds(s * plan.groups * 8 + 2 * z + k, plan.groups, stride=8)
                send[rows, :] = total[:, s * 128 : (s + 1) * 128]

    @pl.when(jnp.logical_not(is_last))
    def _():
        open_with_near()

    for to in plan.order[plan.slabs :]:

        @pl.when(me != place(to))
        def _(to=to):
            pltpu.make_async_remote_copy(
                src_ref=send.at[pl.ds(slot_of(to[2], to[0] * plan.pens + to[1]), plan.rows)],
                dst_ref=recv.at[me, used],
                send_sem=send_sem,
                recv_sem=recv_sem.at[kind],
                device_id=to,
                device_id_type=pl.DeviceIdType.MESH,
            ).start()

    own = pl.multiple_of(slot_of(slab, group), 8)
    recv[me, 0 : plan.rows] = send[pl.ds(own, plan.rows)]

    bm, ky_n, width = plan.block, plan.rows_ky, plan.width

    row = lax.broadcasted_iota(jnp.int32, (width, keep), 0)
    kx = signed(row % bm + slab * bm)
    ky = signed(row // bm + group * ky_n)
    kz = signed(lax.broadcasted_iota(jnp.int32, (width, keep), 1))
    limit = -(keep // 2)
    mask = ((kx != limit) & (ky != limit) & (kz != limit)).astype(jnp.float32)
    waves = [k.astype(jnp.float32) for k in (kx, ky, kz)]
    ksq = waves[0] * waves[0] + waves[1] * waves[1] + waves[2] * waves[2]
    inverse = 1.0 / jnp.maximum(ksq, 1.0)
    damp = (0.5 / (keep // 2) ** 2) * ksq
    for load in late_loads:
        load.wait()
    damped = [
        [
            jnp.concatenate([modes[c, i, k] for i in range(ky_n)], axis=0) * damp
            for k in range(2)
        ]
        for c in range(3)
    ]

    def landed(messages, sem):
        part = recv.at[pl.ds(0, messages), used]
        pltpu.make_async_copy(part, part, sem).wait()

    early = plan.count - plan.slabs

    @pl.when(is_last)
    def _():
        landed(early, recv_sem.at[0])

    @pl.when(jnp.logical_not(is_last))
    def _():
        landed(early - 1, recv_sem.at[0])

    got = split_in_kernel(recv[0:early].reshape(early * 8, 128))
    out = mm(third[0], jnp.concatenate(got, axis=1))
    out = out[:, :128] + out[:, 128:] + mm(third[1], got[0])

    @pl.when(is_last)
    def _():
        if plan.slabs > 1:
            landed(plan.slabs - 1, recv_sem.at[1])

    @pl.when(jnp.logical_not(is_last))
    def _():
        landed(plan.slabs, recv_sem.at[1])

    tail = recv[early]
    for s in range(1, plan.slabs):
        tail = tail + recv[early + s]
    for r in range(plan.rows):
        out = out + final[r] * tail[r : r + 1]
    for k in range(2):
        turned = jnp.transpose(out[k * keep : (k + 1) * keep])
        comp = [turned[c * width : (c + 1) * width] for c in range(3)]
        inner = (waves[0] * comp[0] + waves[1] * comp[1] + waves[2] * comp[2]) * inverse
        for c in range(3):
            result = (comp[c] - waves[c] * inner) * mask - damped[c][k]
            for i in range(ky_n):
                out_ref[c, i, k] = result[i * bm : (i + 1) * bm]
    landed(plan.count - 1, send_sem)


def direct(plan, tables, velocity, vorticity, velocity_modes):
    modes = jnp.transpose(velocity_modes, (0, 2, 3, 4, 1))
    third, final = tables
    hbm = pl.BlockSpec(memory_space=pltpu.HBM)
    out = pl.pallas_call(
        functools.partial(kernel, plan),
        out_shape=pltpu.VMEM(modes.shape, jnp.float32),
        in_specs=[hbm] * 5,
        out_specs=pl.BlockSpec(memory_space=pltpu.VMEM),
        scratch_shapes=[
            pltpu.VMEM((2,) + velocity.shape, jnp.float32),
            pltpu.VMEM(modes.shape, jnp.float32),
            pltpu.VMEM((2, 128, 2 * plan.wide), jnp.bfloat16),
            pltpu.VMEM((2 * plan.keep, 6 * plan.y_rows), jnp.bfloat16),
            pltpu.VMEM(third.shape, jnp.bfloat16),
            pltpu.VMEM((plan.rows_ky, 2, plan.y_rows, 128), jnp.float32),
            pltpu.VMEM(final.shape, jnp.float32),
            pltpu.VMEM((3 * plan.z_rows * plan.y_rows, 128), jnp.float32),
            pltpu.VMEM((plan.slabs * 8, 128), jnp.float32),
            pltpu.VMEM((plan.slabs * plan.groups * 8, 128), jnp.float32),
            pltpu.VMEM((plan.count, 8, 128), jnp.float32),
            pltpu.SemaphoreType.DMA,
            pltpu.SemaphoreType.DMA((3,)),
            pltpu.SemaphoreType.DMA,
            pltpu.SemaphoreType.DMA((2,)),
        ],
        compiler_params=pltpu.CompilerParams(collective_id=0, has_side_effects=True),
    )(velocity, vorticity, modes, third, final)
    return jnp.transpose(out, (0, 4, 1, 2, 3))


def solution(mesh):
    sizes = dict(mesh.shape)
    order = by_distance(mesh.devices)

    def run(velocity, vorticity, velocity_modes):
        _, z_rows, y_rows, cells = velocity.shape
        plan = Plan(sizes, order, cells, velocity_modes.shape[1], z_rows, y_rows)
        if not plan.fits():
            return per_device(velocity, vorticity, velocity_modes)
        return direct(plan, plan.tables(), velocity, vorticity, velocity_modes)

    return jax.shard_map(
        run,
        mesh=mesh,
        in_specs=(
            P(None, ("section", "pen"), "slab", None),
            P(None, ("section", "pen"), "slab", None),
            P(None, None, ("section", "pen"), None, "slab"),
        ),
        out_specs=P(None, None, ("section", "pen"), None, "slab"),
        check_vma=False,
    )
```

```python
import functools
import math

import jax
import jax.numpy as jnp
import numpy as np
from jax import lax
from jax.experimental import pallas as pl
from jax.experimental.pallas import tpu as pltpu
from jax.sharding import PartitionSpec as P

AXES = ("section", "pen", "slab")
highest = lax.Precision.HIGHEST


def signed_modes(index, count):
    return jnp.where(index < count // 2, index, index - count)


def discrete_fourier_tables(length, keep_count):
    modes = signed_modes(jnp.arange(keep_count, dtype=jnp.int32), keep_count)
    mode_positions = jnp.arange(length, dtype=jnp.int32)
    phase = jnp.remainder(modes[:, None] * mode_positions[None, :], length).astype(jnp.float32)
    angles = 2.0 * math.pi / length * phase
    factor = 1.0 / math.sqrt(length)
    return (jnp.cos(angles) * factor, jnp.sin(angles) * factor)


def complex_apply(form, cosine, sine, real_part, imag_part):
    out_real = jnp.einsum(form, cosine, real_part, precision=highest) + jnp.einsum(
        form, sine, imag_part, precision=highest
    )
    out_imag = jnp.einsum(form, cosine, imag_part, precision=highest) - jnp.einsum(
        form, sine, real_part, precision=highest
    )
    return (out_real, out_imag)


def per_device(velocity, vorticity, velocity_modes):
    grid_cells = velocity.shape[3]
    keep_count = velocity_modes.shape[1]
    cross_product = jnp.stack(
        [
            velocity[1] * vorticity[2] - velocity[2] * vorticity[1],
            velocity[2] * vorticity[0] - velocity[0] * vorticity[2],
            velocity[0] * vorticity[1] - velocity[1] * vorticity[0],
        ]
    )
    slabs = lax.axis_size("slab")
    block_modes = keep_count // slabs
    cosine_table, sine_table = discrete_fourier_tables(grid_cells, keep_count)
    cols_real = cosine_table.T.reshape(grid_cells, slabs, block_modes)
    cols_imag = (-sine_table).T.reshape(grid_cells, slabs, block_modes)
    column_table = jnp.stack([cols_real, cols_imag], axis=2).reshape(grid_cells, 2 * keep_count)
    first_pass = jnp.einsum("czyx,xj->czyj", cross_product, column_table, precision=highest)
    block = lax.all_to_all(first_pass, "slab", split_axis=3, concat_axis=2, tiled=True)
    out_real, out_imag = complex_apply(
        "ky,czyj->czkj",
        cosine_table,
        sine_table,
        block[..., :block_modes],
        block[..., block_modes:],
    )
    second_pass = jnp.concatenate([out_real, out_imag], axis=-1)
    halves = lax.axis_size("section")
    pens = lax.axis_size("pen")
    rows_ky = keep_count // (halves * pens)
    block = lax.all_to_all(second_pass, ("section", "pen"), split_axis=2, concat_axis=1, tiled=True)
    out_real, out_imag = complex_apply(
        "kz,czyj->ckyj",
        cosine_table,
        sine_table,
        block[..., :block_modes],
        block[..., block_modes:],
    )
    third_pass = jnp.concatenate([out_real, out_imag], axis=-1)
    group_index = lax.axis_index("section") * pens + lax.axis_index("pen")
    modes_z = signed_modes(jnp.arange(keep_count, dtype=jnp.int32), keep_count)[:, None, None]
    modes_y = signed_modes(
        group_index * rows_ky + jnp.arange(rows_ky, dtype=jnp.int32), keep_count
    )[None, :, None]
    modes_x = signed_modes(
        lax.axis_index("slab") * block_modes + jnp.arange(block_modes, dtype=jnp.int32), keep_count
    )[None, None, :]
    limit = -(keep_count // 2)
    keep_mask = ((modes_x != limit) & (modes_y != limit) & (modes_z != limit)).astype(jnp.float32)
    waves = (modes_x.astype(jnp.float32), modes_y.astype(jnp.float32), modes_z.astype(jnp.float32))
    ksq = waves[0] * waves[0] + waves[1] * waves[1] + waves[2] * waves[2]
    denom = jnp.maximum(ksq, 1.0)
    parts = []
    for which in range(2):
        chosen = third_pass[..., which * block_modes : (which + 1) * block_modes]
        comp = [chosen[c] for c in range(3)]
        inner = (waves[0] * comp[0] + waves[1] * comp[1] + waves[2] * comp[2]) / denom
        parts.append(jnp.stack([comp[c] - waves[c] * inner for c in range(3)]))
    projected = jnp.stack(parts, axis=3)
    visc = 0.5 / (keep_count // 2) ** 2
    return (
        projected * keep_mask[None, :, :, None, :]
        - visc * ksq[None, :, :, None, :] * velocity_modes
    )


def split_bf16(table):
    high = table.astype(jnp.bfloat16)
    low = (table - high.astype(np.float32)).astype(jnp.bfloat16)
    return high, low


def split_in_kernel(value):
    high = value.astype(jnp.bfloat16)
    low = (value - high.astype(jnp.float32)).astype(jnp.bfloat16)
    return high, low


def mm(a, b):
    return lax.dot_general(a, b, (((1,), (0,)), ((), ())), preferred_element_type=jnp.float32)


def split_dot(a, b):
    return mm(a[0], b[0]) + mm(a[1], b[0]) + mm(a[0], b[1])


def wave_numbers(count):
    index = np.arange(count)
    return np.where(index < count // 2, index, index - count)


def host_tables(cells, keep):
    phase = np.remainder(wave_numbers(keep)[:, None] * np.arange(cells)[None, :], cells)
    angles = 2.0 * np.pi / cells * phase
    factor = 1.0 / np.sqrt(cells)
    return np.cos(angles) * factor, np.sin(angles) * factor


def by_distance(devices):
    origin = getattr(devices.flat[0], "coords", ())

    def hops(index):
        return [abs(a - b) for a, b in zip(getattr(devices[index], "coords", ()), origin)]

    every = list(np.ndindex(devices.shape))
    spans = [max(far) for far in zip(*map(hops, every))]

    def key(index):
        far = hops(index)
        if sum(far) == 0:
            return -1, 0, index
        return (far[spans.index(max(spans))], -sum(far), index) if far else (0, 0, index)

    return sorted(every, key=key)


class Plan:
    def __init__(self, mesh_shape, order, cells, keep, z_rows, y_rows):
        self.order = order
        self.cells, self.keep, self.z_rows, self.y_rows = cells, keep, z_rows, y_rows
        self.halves, self.pens, self.slabs = (mesh_shape[a] for a in AXES)
        self.groups = self.halves * self.pens
        self.count = self.groups * self.slabs
        self.rows_ky = keep // self.groups
        self.block = keep // self.slabs
        self.width = self.rows_ky * self.block
        self.rows = 2 * z_rows
        self.wide = self.slabs * 128

    def fits(self):
        return (
            self.rows_ky * self.groups == self.keep
            and self.block * self.slabs == self.keep
            and 3 * self.width <= 128
            and 128 % self.width == 0
            and self.rows <= 8
            and self.cells <= 128
            and self.cells % 16 == 0
            and self.y_rows % 8 == 0
            and 6 * self.y_rows <= 256
            and self.groups % 8 == 0
            and self.keep % 8 == 0
            and self.block % 8 == 0
            and 3 * self.z_rows * self.y_rows <= 512
            and 2 <= self.count <= 64
        )

    def tables(self):
        cos, sin = host_tables(self.cells, self.keep)
        g, zl = self.groups, self.z_rows
        table = np.zeros((2, self.keep, g, self.slabs, 8), np.float32)
        for z in range(zl):
            c, n = cos[:, z::zl][:, :, None], sin[:, z::zl][:, :, None]
            table[0, :, :, :, 2 * z], table[0, :, :, :, 2 * z + 1] = c, n
            table[1, :, :, :, 2 * z], table[1, :, :, :, 2 * z + 1] = -n, c
        early = table[:, :, : g - 1].reshape(2 * self.keep, (g - 1) * self.slabs * 8)
        last = table[:, :, g - 1, 0, : self.rows].reshape(2 * self.keep, self.rows).T
        last = np.broadcast_to(last[:, :, None], (*last.shape, 128))
        return np.stack(split_bf16(early)), np.ascontiguousarray(last)


def kernel(
    plan, vel_hbm, vort_hbm, modes_hbm, third_hbm, final_hbm, out_ref,
    fields, modes, first, second, third, near, final, cross, quick, send, recv,
    field_sem, late_sem, send_sem, recv_sem,
):
    sec, pen, slab = (lax.axis_index(a) for a in AXES)
    group = sec * plan.pens + pen
    me = group * plan.slabs + slab
    kind = group // (plan.groups - 1)
    is_last = kind == 1
    cells, keep = plan.cells, plan.keep
    for i, source in enumerate((vel_hbm, vort_hbm)):
        for c in range(3):
            pltpu.make_async_copy(source.at[c], fields.at[i, c], field_sem).start()
    late_loads = [
        pltpu.make_async_copy(third_hbm, third, late_sem.at[0]),
        pltpu.make_async_copy(modes_hbm, modes, late_sem.at[1]),
        pltpu.make_async_copy(final_hbm, final, late_sem.at[2]),
    ]

    barrier = pltpu.get_barrier_semaphore()

    def signed(index):
        return jnp.where(index < keep // 2, index, index - keep)

    def place(to):
        return (to[0] * plan.pens + to[1]) * plan.slabs + to[2]

    for to in plan.order:

        @pl.when(me != place(to))
        def _(to=to):
            pl.semaphore_signal(
                barrier, inc=1, device_id=to, device_id_type=pl.DeviceIdType.MESH
            )

    if plan.rows < 8:
        recv[:, plan.rows : 8] = jnp.zeros((plan.count, 8 - plan.rows, 128), jnp.float32)
    cross[...] = jnp.zeros_like(cross)
    scale = 1.0 / math.sqrt(cells)

    def turn(wave, cell):
        product = wave * cell
        product = product - cells * jnp.floor(product * (1.0 / cells) + 0.5)
        angle = product * (2.0 * math.pi / cells)
        return jnp.cos(angle) * scale, jnp.sin(angle) * scale

    def ramp(shape, axis):
        return lax.broadcasted_iota(jnp.int32, shape, axis)

    kept = plan.order[0][0] * plan.pens + plan.order[0][1]
    line = (ramp((plan.y_rows, 128), 0) + slab * plan.y_rows).astype(jnp.float32)
    waves_near = [float(wave_numbers(keep)[kept * plan.rows_ky + i]) for i in range(plan.rows_ky)]
    for i in range(plan.rows_ky):
        if waves_near[i] != 0:
            near[i, 0], near[i, 1] = turn(waves_near[i], line)
    lane = ramp((cells, 128), 1)
    line = ramp((cells, 128), 0).astype(jnp.float32)
    for s in range(plan.slabs):
        wave = signed(lane % plan.block + s * plan.block).astype(jnp.float32)
        cosine, sine = turn(wave, line)
        for k, table in enumerate((cosine, -sine)):
            table = split_in_kernel(jnp.where(lane < 3 * plan.width, table, 0.0))
            start = k * plan.wide + s * 128
            for i in range(2):
                first[i, 0:cells, start : start + 128] = table[i]
    shape = (keep, 6 * plan.y_rows)
    row = ramp(shape, 0)
    wave = signed(row % plan.groups * plan.rows_ky + row // plan.groups).astype(jnp.float32)
    line = ramp(shape, 1).astype(jnp.float32)
    part = jnp.floor((line + 0.5) * (1.0 / plan.y_rows))
    line = line - part * plan.y_rows
    cosine, sine = turn(wave, line + (slab * plan.y_rows).astype(jnp.float32))
    real = (part == 0) | (part == 2) | (part == 4)
    for k, table in enumerate((jnp.where(real, cosine, sine), jnp.where(real, -sine, cosine))):
        table_high = table.astype(jnp.bfloat16).astype(jnp.float32)
        table = jnp.where(part < 4, table_high, table - table_high)
        second[k * keep : (k + 1) * keep] = table.astype(jnp.bfloat16)
    if cells < 128:
        for i in range(2):
            first[i, cells:128] = jnp.zeros((128 - cells, first.shape[2]), jnp.bfloat16)

    pltpu.make_async_copy(fields, fields, field_sem).wait()
    zl, yl = plan.z_rows, plan.y_rows
    area = zl * yl
    v, w = ([fields[i, c].reshape(area, cells) for c in range(3)] for i in range(2))
    for c in range(3):
        p, q = (c + 1) % 3, (c + 2) % 3
        cross[c * area : (c + 1) * area, 0:cells] = v[p] * w[q] - v[q] * w[p]
    sub = lax.broadcasted_iota(jnp.int32, (8, 128), 0)

    def folded(terms):
        part = terms[0:8]
        for r in range(8, yl, 8):
            part = part + terms[r : r + 8]
        return part

    blocks = []
    for i in range(plan.rows_ky):
        for c in range(3):
            sums = []
            for z in range(zl):
                start = (c * zl + z) * yl
                line = cross[start : start + yl]
                if waves_near[i] == 0:
                    part = folded(line)
                    part = part + pltpu.roll(part, 4, 0)
                else:
                    pair = [folded(line * near[i, k]) for k in range(2)]
                    part = jnp.where(sub < 4, pair[0], pair[1]) + pltpu.roll(
                        jnp.where(sub < 4, pair[1], pair[0]), 4, 0
                    )
                sums.append(part + pltpu.roll(part, 2 if z // 2 % 2 else 6, 0))
            even, odd = None, None
            for z in range(0, zl, 2):
                even = sums[z] if even is None else jnp.where(sub % 4 < 2, even, sums[z])
            for z in range(1, zl, 2):
                odd = sums[z] if odd is None else jnp.where(sub % 4 < 2, odd, sums[z])
            block = even + pltpu.roll(even, 7, 0)
            if odd is not None:
                block = jnp.where(sub % 2 == 0, block, odd + pltpu.roll(odd, 1, 0))
            if waves_near[i] == 0:
                block = jnp.where(sub < 4, block * scale, 0.0)
            blocks.append(block)
    high, low = split_in_kernel(jnp.concatenate(blocks, axis=0))
    planes = mm(
        jnp.concatenate([high, low, high], axis=1),
        jnp.concatenate([first[0], first[0], first[1]], axis=0),
    )
    cell = lax.broadcasted_iota(jnp.int32, (8, 2 * plan.wide), 1) % 128 // plan.block
    total = planes[0:8]
    for i in range(plan.rows_ky):
        for c in range(3):
            start = (i * 3 + c) * 8
            total = jnp.where(cell == c * plan.rows_ky + i, planes[start : start + 8], total)
    real, imag = total[:, : plan.wide], total[:, plan.wide :]
    parts = (real + pltpu.roll(imag, 4, 0), imag - pltpu.roll(real, 4, 0))
    for k in range(2):
        for s in range(plan.slabs):
            quick[pl.ds(s * 8 + k, zl, stride=2), :] = parts[k][0:zl, s * 128 : (s + 1) * 128]

    used = pl.ds(0, plan.rows)

    def slot_of(s, g):
        return (s * plan.groups + g) * 8

    def open_with_near():
        pl.semaphore_wait(barrier, plan.count - 1)
        for s in range(plan.slabs):
            to = (*plan.order[0][:2], s)

            @pl.when(me != place(to))
            def _(to=to):
                pltpu.make_async_remote_copy(
                    src_ref=quick.at[pl.ds(to[2] * 8, plan.rows)],
                    dst_ref=recv.at[me, used],
                    send_sem=send_sem,
                    recv_sem=recv_sem.at[kind],
                    device_id=to,
                    device_id_type=pl.DeviceIdType.MESH,
                ).start()

    @pl.when(is_last)
    def _():
        open_with_near()

    high, low = split_in_kernel(cross[...])
    along_x = mm(
        jnp.concatenate([high, low], axis=1), jnp.concatenate([first[0], first[0]], axis=0)
    ) + mm(high, first[1])
    slot = lax.broadcasted_iota(jnp.int32, (area, 2 * plan.wide), 1) % 128 // plan.width
    along_x = [along_x[c * area : (c + 1) * area] for c in range(3)]
    along_x = jnp.where(slot == 0, along_x[0], jnp.where(slot == 1, along_x[1], along_x[2]))
    high = along_x.astype(jnp.bfloat16).astype(jnp.float32)
    low = along_x - high
    upper = lax.broadcasted_iota(jnp.int32, (plan.groups, plan.wide), 1) % plan.width // plan.block
    for z in range(zl):
        parts = []
        for part in (high, low):
            piece = part[z * yl : (z + 1) * yl]
            parts.append(
                jnp.concatenate([piece[:, : plan.wide], piece[:, plan.wide :]], axis=0)
            )
        stack = jnp.concatenate([parts[0], parts[1], parts[0]], axis=0).astype(jnp.bfloat16)
        planes = mm(second[...], stack)
        for k in range(2):
            total = None
            for i in range(plan.rows_ky):
                start = (k * plan.rows_ky + i) * plan.groups
                piece = planes[start : start + plan.groups]
                total = piece if total is None else jnp.where(upper == i, piece, total)
            for s in range(plan.slabs):
                rows = pl.ds(s * plan.groups * 8 + 2 * z + k, plan.groups, stride=8)
                send[rows, :] = total[:, s * 128 : (s + 1) * 128]

    for load in late_loads:
        load.start()

    @pl.when(jnp.logical_not(is_last))
    def _():
        open_with_near()

    for to in plan.order[plan.slabs :]:

        @pl.when(me != place(to))
        def _(to=to):
            pltpu.make_async_remote_copy(
                src_ref=send.at[pl.ds(slot_of(to[2], to[0] * plan.pens + to[1]), plan.rows)],
                dst_ref=recv.at[me, used],
                send_sem=send_sem,
                recv_sem=recv_sem.at[kind],
                device_id=to,
                device_id_type=pl.DeviceIdType.MESH,
            ).start()

    own = pl.multiple_of(slot_of(slab, group), 8)
    recv[me, 0 : plan.rows] = send[pl.ds(own, plan.rows)]

    bm, ky_n, width = plan.block, plan.rows_ky, plan.width

    row = lax.broadcasted_iota(jnp.int32, (width, keep), 0)
    kx = signed(row % bm + slab * bm)
    ky = signed(row // bm + group * ky_n)
    kz = signed(lax.broadcasted_iota(jnp.int32, (width, keep), 1))
    limit = -(keep // 2)
    mask = ((kx != limit) & (ky != limit) & (kz != limit)).astype(jnp.float32)
    waves = [k.astype(jnp.float32) for k in (kx, ky, kz)]
    ksq = waves[0] * waves[0] + waves[1] * waves[1] + waves[2] * waves[2]
    inverse = 1.0 / jnp.maximum(ksq, 1.0)
    damp = (0.5 / (keep // 2) ** 2) * ksq
    for load in late_loads:
        load.wait()
    damped = [
        [
            jnp.concatenate([modes[c, i, k] for i in range(ky_n)], axis=0) * damp
            for k in range(2)
        ]
        for c in range(3)
    ]

    def landed(messages, sem):
        part = recv.at[pl.ds(0, messages), used]
        pltpu.make_async_copy(part, part, sem).wait()

    early = plan.count - plan.slabs

    @pl.when(is_last)
    def _():
        landed(early, recv_sem.at[0])

    @pl.when(jnp.logical_not(is_last))
    def _():
        landed(early - 1, recv_sem.at[0])

    got = split_in_kernel(recv[0:early].reshape(early * 8, 128))
    out = mm(third[0], jnp.concatenate(got, axis=1))
    out = out[:, :128] + out[:, 128:] + mm(third[1], got[0])

    @pl.when(is_last)
    def _():
        if plan.slabs > 1:
            landed(plan.slabs - 1, recv_sem.at[1])

    @pl.when(jnp.logical_not(is_last))
    def _():
        landed(plan.slabs, recv_sem.at[1])

    tail = recv[early]
    for s in range(1, plan.slabs):
        tail = tail + recv[early + s]
    for r in range(plan.rows):
        out = out + final[r] * tail[r : r + 1]
    for k in range(2):
        turned = jnp.transpose(out[k * keep : (k + 1) * keep])
        comp = [turned[c * width : (c + 1) * width] for c in range(3)]
        inner = (waves[0] * comp[0] + waves[1] * comp[1] + waves[2] * comp[2]) * inverse
        for c in range(3):
            result = (comp[c] - waves[c] * inner) * mask - damped[c][k]
            for i in range(ky_n):
                out_ref[c, i, k] = result[i * bm : (i + 1) * bm]
    landed(plan.count - 1, send_sem)


def direct(plan, tables, velocity, vorticity, velocity_modes):
    modes = jnp.transpose(velocity_modes, (0, 2, 3, 4, 1))
    third, final = tables
    hbm = pl.BlockSpec(memory_space=pltpu.HBM)
    out = pl.pallas_call(
        functools.partial(kernel, plan),
        out_shape=pltpu.VMEM(modes.shape, jnp.float32),
        in_specs=[hbm] * 5,
        out_specs=pl.BlockSpec(memory_space=pltpu.VMEM),
        scratch_shapes=[
            pltpu.VMEM((2,) + velocity.shape, jnp.float32),
            pltpu.VMEM(modes.shape, jnp.float32),
            pltpu.VMEM((2, 128, 2 * plan.wide), jnp.bfloat16),
            pltpu.VMEM((2 * plan.keep, 6 * plan.y_rows), jnp.bfloat16),
            pltpu.VMEM(third.shape, jnp.bfloat16),
            pltpu.VMEM((plan.rows_ky, 2, plan.y_rows, 128), jnp.float32),
            pltpu.VMEM(final.shape, jnp.float32),
            pltpu.VMEM((3 * plan.z_rows * plan.y_rows, 128), jnp.float32),
            pltpu.VMEM((plan.slabs * 8, 128), jnp.float32),
            pltpu.VMEM((plan.slabs * plan.groups * 8, 128), jnp.float32),
            pltpu.VMEM((plan.count, 8, 128), jnp.float32),
            pltpu.SemaphoreType.DMA,
            pltpu.SemaphoreType.DMA((3,)),
            pltpu.SemaphoreType.DMA,
            pltpu.SemaphoreType.DMA((2,)),
        ],
        compiler_params=pltpu.CompilerParams(collective_id=0, has_side_effects=True),
    )(velocity, vorticity, modes, third, final)
    return jnp.transpose(out, (0, 4, 1, 2, 3))


def solution(mesh):
    sizes = dict(mesh.shape)
    order = by_distance(mesh.devices)

    def run(velocity, vorticity, velocity_modes):
        _, z_rows, y_rows, cells = velocity.shape
        plan = Plan(sizes, order, cells, velocity_modes.shape[1], z_rows, y_rows)
        if not plan.fits():
            return per_device(velocity, vorticity, velocity_modes)
        return direct(plan, plan.tables(), velocity, vorticity, velocity_modes)

    return jax.shard_map(
        run,
        mesh=mesh,
        in_specs=(
            P(None, ("section", "pen"), "slab", None),
            P(None, ("section", "pen"), "slab", None),
            P(None, None, ("section", "pen"), None, "slab"),
        ),
        out_specs=P(None, None, ("section", "pen"), None, "slab"),
        check_vma=False,
    )
```

```python
import functools
import math

import jax
import jax.numpy as jnp
import numpy as np
from jax import lax
from jax.experimental import pallas as pl
from jax.experimental.pallas import tpu as pltpu
from jax.sharding import PartitionSpec as P

AXES = ("section", "pen", "slab")
highest = lax.Precision.HIGHEST


def signed_modes(index, count):
    return jnp.where(index < count // 2, index, index - count)


def discrete_fourier_tables(length, keep_count):
    modes = signed_modes(jnp.arange(keep_count, dtype=jnp.int32), keep_count)
    mode_positions = jnp.arange(length, dtype=jnp.int32)
    phase = jnp.remainder(modes[:, None] * mode_positions[None, :], length).astype(jnp.float32)
    angles = 2.0 * math.pi / length * phase
    factor = 1.0 / math.sqrt(length)
    return (jnp.cos(angles) * factor, jnp.sin(angles) * factor)


def complex_apply(form, cosine, sine, real_part, imag_part):
    out_real = jnp.einsum(form, cosine, real_part, precision=highest) + jnp.einsum(
        form, sine, imag_part, precision=highest
    )
    out_imag = jnp.einsum(form, cosine, imag_part, precision=highest) - jnp.einsum(
        form, sine, real_part, precision=highest
    )
    return (out_real, out_imag)


def per_device(velocity, vorticity, velocity_modes):
    grid_cells = velocity.shape[3]
    keep_count = velocity_modes.shape[1]
    cross_product = jnp.stack(
        [
            velocity[1] * vorticity[2] - velocity[2] * vorticity[1],
            velocity[2] * vorticity[0] - velocity[0] * vorticity[2],
            velocity[0] * vorticity[1] - velocity[1] * vorticity[0],
        ]
    )
    slabs = lax.axis_size("slab")
    block_modes = keep_count // slabs
    cosine_table, sine_table = discrete_fourier_tables(grid_cells, keep_count)
    cols_real = cosine_table.T.reshape(grid_cells, slabs, block_modes)
    cols_imag = (-sine_table).T.reshape(grid_cells, slabs, block_modes)
    column_table = jnp.stack([cols_real, cols_imag], axis=2).reshape(grid_cells, 2 * keep_count)
    first_pass = jnp.einsum("czyx,xj->czyj", cross_product, column_table, precision=highest)
    block = lax.all_to_all(first_pass, "slab", split_axis=3, concat_axis=2, tiled=True)
    out_real, out_imag = complex_apply(
        "ky,czyj->czkj",
        cosine_table,
        sine_table,
        block[..., :block_modes],
        block[..., block_modes:],
    )
    second_pass = jnp.concatenate([out_real, out_imag], axis=-1)
    halves = lax.axis_size("section")
    pens = lax.axis_size("pen")
    rows_ky = keep_count // (halves * pens)
    block = lax.all_to_all(second_pass, ("section", "pen"), split_axis=2, concat_axis=1, tiled=True)
    out_real, out_imag = complex_apply(
        "kz,czyj->ckyj",
        cosine_table,
        sine_table,
        block[..., :block_modes],
        block[..., block_modes:],
    )
    third_pass = jnp.concatenate([out_real, out_imag], axis=-1)
    group_index = lax.axis_index("section") * pens + lax.axis_index("pen")
    modes_z = signed_modes(jnp.arange(keep_count, dtype=jnp.int32), keep_count)[:, None, None]
    modes_y = signed_modes(
        group_index * rows_ky + jnp.arange(rows_ky, dtype=jnp.int32), keep_count
    )[None, :, None]
    modes_x = signed_modes(
        lax.axis_index("slab") * block_modes + jnp.arange(block_modes, dtype=jnp.int32), keep_count
    )[None, None, :]
    limit = -(keep_count // 2)
    keep_mask = ((modes_x != limit) & (modes_y != limit) & (modes_z != limit)).astype(jnp.float32)
    waves = (modes_x.astype(jnp.float32), modes_y.astype(jnp.float32), modes_z.astype(jnp.float32))
    ksq = waves[0] * waves[0] + waves[1] * waves[1] + waves[2] * waves[2]
    denom = jnp.maximum(ksq, 1.0)
    parts = []
    for which in range(2):
        chosen = third_pass[..., which * block_modes : (which + 1) * block_modes]
        comp = [chosen[c] for c in range(3)]
        inner = (waves[0] * comp[0] + waves[1] * comp[1] + waves[2] * comp[2]) / denom
        parts.append(jnp.stack([comp[c] - waves[c] * inner for c in range(3)]))
    projected = jnp.stack(parts, axis=3)
    visc = 0.5 / (keep_count // 2) ** 2
    return (
        projected * keep_mask[None, :, :, None, :]
        - visc * ksq[None, :, :, None, :] * velocity_modes
    )


def split_bf16(table):
    high = table.astype(jnp.bfloat16)
    low = (table - high.astype(np.float32)).astype(jnp.bfloat16)
    return high, low


def split_in_kernel(value):
    high = value.astype(jnp.bfloat16)
    low = (value - high.astype(jnp.float32)).astype(jnp.bfloat16)
    return high, low


def mm(a, b):
    return lax.dot_general(a, b, (((1,), (0,)), ((), ())), preferred_element_type=jnp.float32)


def split_dot(a, b):
    return mm(a[0], b[0]) + mm(a[1], b[0]) + mm(a[0], b[1])


def wave_numbers(count):
    index = np.arange(count)
    return np.where(index < count // 2, index, index - count)


def host_tables(cells, keep):
    phase = np.remainder(wave_numbers(keep)[:, None] * np.arange(cells)[None, :], cells)
    angles = 2.0 * np.pi / cells * phase
    factor = 1.0 / np.sqrt(cells)
    return np.cos(angles) * factor, np.sin(angles) * factor


def by_distance(devices):
    origin = getattr(devices.flat[0], "coords", ())

    def hops(index):
        return [abs(a - b) for a, b in zip(getattr(devices[index], "coords", ()), origin)]

    every = list(np.ndindex(devices.shape))
    spans = [max(far) for far in zip(*map(hops, every))]

    def key(index):
        far = hops(index)
        if sum(far) == 0:
            return -1, 0, index
        return (far[spans.index(max(spans))], -sum(far), index) if far else (0, 0, index)

    order = sorted(every, key=key)

    def greeting(index):
        far = sum(hops(index))
        return order.index(index) >= len(order) // 2, far == 0, -far, index

    return order, sorted(every, key=greeting)


class Plan:
    def __init__(self, mesh_shape, orders, cells, keep, z_rows, y_rows):
        self.order, self.greeted = orders
        self.cells, self.keep, self.z_rows, self.y_rows = cells, keep, z_rows, y_rows
        self.halves, self.pens, self.slabs = (mesh_shape[a] for a in AXES)
        self.groups = self.halves * self.pens
        self.count = self.groups * self.slabs
        self.rows_ky = keep // self.groups
        self.block = keep // self.slabs
        self.width = self.rows_ky * self.block
        self.rows = 2 * z_rows
        self.wide = self.slabs * 128

    def fits(self):
        return (
            self.rows_ky * self.groups == self.keep
            and self.block * self.slabs == self.keep
            and 3 * self.width <= 128
            and 128 % self.width == 0
            and self.rows <= 8
            and self.cells <= 128
            and self.cells % 16 == 0
            and self.y_rows % 8 == 0
            and 6 * self.y_rows <= 256
            and self.groups % 8 == 0
            and self.keep % 8 == 0
            and self.block % 8 == 0
            and 3 * self.z_rows * self.y_rows <= 512
            and 2 <= self.count <= 64
        )

    def tables(self):
        cos, sin = host_tables(self.cells, self.keep)
        g, zl = self.groups, self.z_rows
        table = np.zeros((2, self.keep, g, self.slabs, 8), np.float32)
        for z in range(zl):
            c, n = cos[:, z::zl][:, :, None], sin[:, z::zl][:, :, None]
            table[0, :, :, :, 2 * z], table[0, :, :, :, 2 * z + 1] = c, n
            table[1, :, :, :, 2 * z], table[1, :, :, :, 2 * z + 1] = -n, c
        early = table[:, :, : g - 1].reshape(2 * self.keep, (g - 1) * self.slabs * 8)
        last = table[:, :, g - 1, 0, : self.rows].reshape(2 * self.keep, self.rows).T
        last = np.broadcast_to(last[:, :, None], (*last.shape, 128))
        return np.stack(split_bf16(early)), np.ascontiguousarray(last)


def kernel(
    plan, vel_hbm, vort_hbm, modes_hbm, third_hbm, final_hbm, out_ref,
    fields, modes, first, second, third, near, final, cross, quick, send, recv,
    field_sem, late_sem, send_sem, recv_sem,
):
    sec, pen, slab = (lax.axis_index(a) for a in AXES)
    group = sec * plan.pens + pen
    me = group * plan.slabs + slab
    kind = group // (plan.groups - 1)
    is_last = kind == 1
    cells, keep = plan.cells, plan.keep
    for i, source in enumerate((vel_hbm, vort_hbm)):
        for c in range(3):
            pltpu.make_async_copy(source.at[c], fields.at[i, c], field_sem).start()
    late_loads = [
        pltpu.make_async_copy(third_hbm, third, late_sem.at[0]),
        pltpu.make_async_copy(modes_hbm, modes, late_sem.at[1]),
        pltpu.make_async_copy(final_hbm, final, late_sem.at[2]),
    ]

    barrier = pltpu.get_barrier_semaphore()

    def signed(index):
        return jnp.where(index < keep // 2, index, index - keep)

    def place(to):
        return (to[0] * plan.pens + to[1]) * plan.slabs + to[2]

    for to in plan.greeted:

        @pl.when(me != place(to))
        def _(to=to):
            pl.semaphore_signal(
                barrier, inc=1, device_id=to, device_id_type=pl.DeviceIdType.MESH
            )

    if plan.rows < 8:
        recv[:, plan.rows : 8] = jnp.zeros((plan.count, 8 - plan.rows, 128), jnp.float32)
    cross[...] = jnp.zeros_like(cross)
    scale = 1.0 / math.sqrt(cells)

    def turn(wave, cell):
        product = wave * cell
        product = product - cells * jnp.floor(product * (1.0 / cells) + 0.5)
        angle = product * (2.0 * math.pi / cells)
        return jnp.cos(angle) * scale, jnp.sin(angle) * scale

    def ramp(shape, axis):
        return lax.broadcasted_iota(jnp.int32, shape, axis)

    kept = plan.order[0][0] * plan.pens + plan.order[0][1]
    line = (ramp((plan.y_rows, 128), 0) + slab * plan.y_rows).astype(jnp.float32)
    waves_near = [float(wave_numbers(keep)[kept * plan.rows_ky + i]) for i in range(plan.rows_ky)]
    for i in range(plan.rows_ky):
        if waves_near[i] != 0:
            near[i, 0], near[i, 1] = turn(waves_near[i], line)
    lane = ramp((cells, 128), 1)
    line = ramp((cells, 128), 0).astype(jnp.float32)
    for s in range(plan.slabs):
        wave = signed(lane % plan.block + s * plan.block).astype(jnp.float32)
        cosine, sine = turn(wave, line)
        for k, table in enumerate((cosine, -sine)):
            table = split_in_kernel(jnp.where(lane < 3 * plan.width, table, 0.0))
            start = k * plan.wide + s * 128
            for i in range(2):
                first[i, 0:cells, start : start + 128] = table[i]
    shape = (keep, 6 * plan.y_rows)
    row = ramp(shape, 0)
    wave = signed(row % plan.groups * plan.rows_ky + row // plan.groups).astype(jnp.float32)
    line = ramp(shape, 1).astype(jnp.float32)
    part = jnp.floor((line + 0.5) * (1.0 / plan.y_rows))
    line = line - part * plan.y_rows
    cosine, sine = turn(wave, line + (slab * plan.y_rows).astype(jnp.float32))
    real = (part == 0) | (part == 2) | (part == 4)
    for k, table in enumerate((jnp.where(real, cosine, sine), jnp.where(real, -sine, cosine))):
        table_high = table.astype(jnp.bfloat16).astype(jnp.float32)
        table = jnp.where(part < 4, table_high, table - table_high)
        second[k * keep : (k + 1) * keep] = table.astype(jnp.bfloat16)
    if cells < 128:
        for i in range(2):
            first[i, cells:128] = jnp.zeros((128 - cells, first.shape[2]), jnp.bfloat16)

    pltpu.make_async_copy(fields, fields, field_sem).wait()
    zl, yl = plan.z_rows, plan.y_rows
    area = zl * yl
    v, w = ([fields[i, c].reshape(area, cells) for c in range(3)] for i in range(2))
    for c in range(3):
        p, q = (c + 1) % 3, (c + 2) % 3
        cross[c * area : (c + 1) * area, 0:cells] = v[p] * w[q] - v[q] * w[p]
    sub = lax.broadcasted_iota(jnp.int32, (8, 128), 0)

    def folded(terms):
        part = terms[0:8]
        for r in range(8, yl, 8):
            part = part + terms[r : r + 8]
        return part

    blocks = []
    for i in range(plan.rows_ky):
        for c in range(3):
            sums = []
            for z in range(zl):
                start = (c * zl + z) * yl
                line = cross[start : start + yl]
                if waves_near[i] == 0:
                    part = folded(line)
                    part = part + pltpu.roll(part, 4, 0)
                else:
                    pair = [folded(line * near[i, k]) for k in range(2)]
                    part = jnp.where(sub < 4, pair[0], pair[1]) + pltpu.roll(
                        jnp.where(sub < 4, pair[1], pair[0]), 4, 0
                    )
                sums.append(part + pltpu.roll(part, 2 if z // 2 % 2 else 6, 0))
            even, odd = None, None
            for z in range(0, zl, 2):
                even = sums[z] if even is None else jnp.where(sub % 4 < 2, even, sums[z])
            for z in range(1, zl, 2):
                odd = sums[z] if odd is None else jnp.where(sub % 4 < 2, odd, sums[z])
            block = even + pltpu.roll(even, 7, 0)
            if odd is not None:
                block = jnp.where(sub % 2 == 0, block, odd + pltpu.roll(odd, 1, 0))
            if waves_near[i] == 0:
                block = jnp.where(sub < 4, block * scale, 0.0)
            blocks.append(block)
    high, low = split_in_kernel(jnp.concatenate(blocks, axis=0))
    planes = mm(
        jnp.concatenate([high, low, high], axis=1),
        jnp.concatenate([first[0], first[0], first[1]], axis=0),
    )
    cell = lax.broadcasted_iota(jnp.int32, (8, 2 * plan.wide), 1) % 128 // plan.block
    total = planes[0:8]
    for i in range(plan.rows_ky):
        for c in range(3):
            start = (i * 3 + c) * 8
            total = jnp.where(cell == c * plan.rows_ky + i, planes[start : start + 8], total)
    real, imag = total[:, : plan.wide], total[:, plan.wide :]
    parts = (real + pltpu.roll(imag, 4, 0), imag - pltpu.roll(real, 4, 0))
    for k in range(2):
        for s in range(plan.slabs):
            quick[pl.ds(s * 8 + k, zl, stride=2), :] = parts[k][0:zl, s * 128 : (s + 1) * 128]

    used = pl.ds(0, plan.rows)

    def slot_of(s, g):
        return (s * plan.groups + g) * 8

    def open_with_near():
        pl.semaphore_wait(barrier, plan.count - 1)
        for s in range(plan.slabs):
            to = (*plan.order[0][:2], s)

            @pl.when(me != place(to))
            def _(to=to):
                pltpu.make_async_remote_copy(
                    src_ref=quick.at[pl.ds(to[2] * 8, plan.rows)],
                    dst_ref=recv.at[me, used],
                    send_sem=send_sem,
                    recv_sem=recv_sem.at[kind],
                    device_id=to,
                    device_id_type=pl.DeviceIdType.MESH,
                ).start()

    @pl.when(is_last)
    def _():
        open_with_near()

    high, low = split_in_kernel(cross[...])
    along_x = mm(
        jnp.concatenate([high, low], axis=1), jnp.concatenate([first[0], first[0]], axis=0)
    ) + mm(high, first[1])
    slot = lax.broadcasted_iota(jnp.int32, (area, 2 * plan.wide), 1) % 128 // plan.width
    along_x = [along_x[c * area : (c + 1) * area] for c in range(3)]
    along_x = jnp.where(slot == 0, along_x[0], jnp.where(slot == 1, along_x[1], along_x[2]))
    high = along_x.astype(jnp.bfloat16).astype(jnp.float32)
    low = along_x - high
    upper = lax.broadcasted_iota(jnp.int32, (plan.groups, plan.wide), 1) % plan.width // plan.block
    for z in range(zl):
        parts = []
        for part in (high, low):
            piece = part[z * yl : (z + 1) * yl]
            parts.append(
                jnp.concatenate([piece[:, : plan.wide], piece[:, plan.wide :]], axis=0)
            )
        stack = jnp.concatenate([parts[0], parts[1], parts[0]], axis=0).astype(jnp.bfloat16)
        planes = mm(second[...], stack)
        for k in range(2):
            total = None
            for i in range(plan.rows_ky):
                start = (k * plan.rows_ky + i) * plan.groups
                piece = planes[start : start + plan.groups]
                total = piece if total is None else jnp.where(upper == i, piece, total)
            for s in range(plan.slabs):
                rows = pl.ds(s * plan.groups * 8 + 2 * z + k, plan.groups, stride=8)
                send[rows, :] = total[:, s * 128 : (s + 1) * 128]

    for load in late_loads:
        load.start()

    @pl.when(jnp.logical_not(is_last))
    def _():
        open_with_near()

    for to in plan.order[plan.slabs :]:

        @pl.when(me != place(to))
        def _(to=to):
            pltpu.make_async_remote_copy(
                src_ref=send.at[pl.ds(slot_of(to[2], to[0] * plan.pens + to[1]), plan.rows)],
                dst_ref=recv.at[me, used],
                send_sem=send_sem,
                recv_sem=recv_sem.at[kind],
                device_id=to,
                device_id_type=pl.DeviceIdType.MESH,
            ).start()

    own = pl.multiple_of(slot_of(slab, group), 8)
    recv[me, 0 : plan.rows] = send[pl.ds(own, plan.rows)]

    bm, ky_n, width = plan.block, plan.rows_ky, plan.width

    row = lax.broadcasted_iota(jnp.int32, (width, keep), 0)
    kx = signed(row % bm + slab * bm)
    ky = signed(row // bm + group * ky_n)
    kz = signed(lax.broadcasted_iota(jnp.int32, (width, keep), 1))
    limit = -(keep // 2)
    mask = ((kx != limit) & (ky != limit) & (kz != limit)).astype(jnp.float32)
    waves = [k.astype(jnp.float32) for k in (kx, ky, kz)]
    ksq = waves[0] * waves[0] + waves[1] * waves[1] + waves[2] * waves[2]
    inverse = 1.0 / jnp.maximum(ksq, 1.0)
    damp = (0.5 / (keep // 2) ** 2) * ksq
    for load in late_loads:
        load.wait()
    damped = [
        [
            jnp.concatenate([modes[c, i, k] for i in range(ky_n)], axis=0) * damp
            for k in range(2)
        ]
        for c in range(3)
    ]

    def landed(messages, sem):
        part = recv.at[pl.ds(0, messages), used]
        pltpu.make_async_copy(part, part, sem).wait()

    early = plan.count - plan.slabs

    @pl.when(is_last)
    def _():
        landed(early, recv_sem.at[0])

    @pl.when(jnp.logical_not(is_last))
    def _():
        landed(early - 1, recv_sem.at[0])

    got = split_in_kernel(recv[0:early].reshape(early * 8, 128))
    out = mm(third[0], jnp.concatenate(got, axis=1))
    out = out[:, :128] + out[:, 128:] + mm(third[1], got[0])

    @pl.when(is_last)
    def _():
        if plan.slabs > 1:
            landed(plan.slabs - 1, recv_sem.at[1])

    @pl.when(jnp.logical_not(is_last))
    def _():
        landed(plan.slabs, recv_sem.at[1])

    tail = recv[early]
    for s in range(1, plan.slabs):
        tail = tail + recv[early + s]
    for r in range(plan.rows):
        out = out + final[r] * tail[r : r + 1]
    for k in range(2):
        turned = jnp.transpose(out[k * keep : (k + 1) * keep])
        comp = [turned[c * width : (c + 1) * width] for c in range(3)]
        inner = (waves[0] * comp[0] + waves[1] * comp[1] + waves[2] * comp[2]) * inverse
        for c in range(3):
            result = (comp[c] - waves[c] * inner) * mask - damped[c][k]
            for i in range(ky_n):
                out_ref[c, i, k] = result[i * bm : (i + 1) * bm]
    landed(plan.count - 1, send_sem)


def direct(plan, tables, velocity, vorticity, velocity_modes):
    modes = jnp.transpose(velocity_modes, (0, 2, 3, 4, 1))
    third, final = tables
    hbm = pl.BlockSpec(memory_space=pltpu.HBM)
    out = pl.pallas_call(
        functools.partial(kernel, plan),
        out_shape=pltpu.VMEM(modes.shape, jnp.float32),
        in_specs=[hbm] * 5,
        out_specs=pl.BlockSpec(memory_space=pltpu.VMEM),
        scratch_shapes=[
            pltpu.VMEM((2,) + velocity.shape, jnp.float32),
            pltpu.VMEM(modes.shape, jnp.float32),
            pltpu.VMEM((2, 128, 2 * plan.wide), jnp.bfloat16),
            pltpu.VMEM((2 * plan.keep, 6 * plan.y_rows), jnp.bfloat16),
            pltpu.VMEM(third.shape, jnp.bfloat16),
            pltpu.VMEM((plan.rows_ky, 2, plan.y_rows, 128), jnp.float32),
            pltpu.VMEM(final.shape, jnp.float32),
            pltpu.VMEM((3 * plan.z_rows * plan.y_rows, 128), jnp.float32),
            pltpu.VMEM((plan.slabs * 8, 128), jnp.float32),
            pltpu.VMEM((plan.slabs * plan.groups * 8, 128), jnp.float32),
            pltpu.VMEM((plan.count, 8, 128), jnp.float32),
            pltpu.SemaphoreType.DMA,
            pltpu.SemaphoreType.DMA((3,)),
            pltpu.SemaphoreType.DMA,
            pltpu.SemaphoreType.DMA((2,)),
        ],
        compiler_params=pltpu.CompilerParams(collective_id=0, has_side_effects=True),
    )(velocity, vorticity, modes, third, final)
    return jnp.transpose(out, (0, 4, 1, 2, 3))


def solution(mesh):
    sizes = dict(mesh.shape)
    orders = by_distance(mesh.devices)

    def run(velocity, vorticity, velocity_modes):
        _, z_rows, y_rows, cells = velocity.shape
        plan = Plan(sizes, orders, cells, velocity_modes.shape[1], z_rows, y_rows)
        if not plan.fits():
            return per_device(velocity, vorticity, velocity_modes)
        return direct(plan, plan.tables(), velocity, vorticity, velocity_modes)

    return jax.shard_map(
        run,
        mesh=mesh,
        in_specs=(
            P(None, ("section", "pen"), "slab", None),
            P(None, ("section", "pen"), "slab", None),
            P(None, None, ("section", "pen"), None, "slab"),
        ),
        out_specs=P(None, None, ("section", "pen"), None, "slab"),
        check_vma=False,
    )
```

```python
import functools
import math

import jax
import jax.numpy as jnp
import numpy as np
from jax import lax
from jax.experimental import pallas as pl
from jax.experimental.pallas import tpu as pltpu
from jax.sharding import PartitionSpec as P

AXES = ("section", "pen", "slab")
highest = lax.Precision.HIGHEST


def signed_modes(index, count):
    return jnp.where(index < count // 2, index, index - count)


def discrete_fourier_tables(length, keep_count):
    modes = signed_modes(jnp.arange(keep_count, dtype=jnp.int32), keep_count)
    mode_positions = jnp.arange(length, dtype=jnp.int32)
    phase = jnp.remainder(modes[:, None] * mode_positions[None, :], length).astype(jnp.float32)
    angles = 2.0 * math.pi / length * phase
    factor = 1.0 / math.sqrt(length)
    return (jnp.cos(angles) * factor, jnp.sin(angles) * factor)


def complex_apply(form, cosine, sine, real_part, imag_part):
    out_real = jnp.einsum(form, cosine, real_part, precision=highest) + jnp.einsum(
        form, sine, imag_part, precision=highest
    )
    out_imag = jnp.einsum(form, cosine, imag_part, precision=highest) - jnp.einsum(
        form, sine, real_part, precision=highest
    )
    return (out_real, out_imag)


def per_device(velocity, vorticity, velocity_modes):
    grid_cells = velocity.shape[3]
    keep_count = velocity_modes.shape[1]
    cross_product = jnp.stack(
        [
            velocity[1] * vorticity[2] - velocity[2] * vorticity[1],
            velocity[2] * vorticity[0] - velocity[0] * vorticity[2],
            velocity[0] * vorticity[1] - velocity[1] * vorticity[0],
        ]
    )
    slabs = lax.axis_size("slab")
    block_modes = keep_count // slabs
    cosine_table, sine_table = discrete_fourier_tables(grid_cells, keep_count)
    cols_real = cosine_table.T.reshape(grid_cells, slabs, block_modes)
    cols_imag = (-sine_table).T.reshape(grid_cells, slabs, block_modes)
    column_table = jnp.stack([cols_real, cols_imag], axis=2).reshape(grid_cells, 2 * keep_count)
    first_pass = jnp.einsum("czyx,xj->czyj", cross_product, column_table, precision=highest)
    block = lax.all_to_all(first_pass, "slab", split_axis=3, concat_axis=2, tiled=True)
    out_real, out_imag = complex_apply(
        "ky,czyj->czkj",
        cosine_table,
        sine_table,
        block[..., :block_modes],
        block[..., block_modes:],
    )
    second_pass = jnp.concatenate([out_real, out_imag], axis=-1)
    halves = lax.axis_size("section")
    pens = lax.axis_size("pen")
    rows_ky = keep_count // (halves * pens)
    block = lax.all_to_all(second_pass, ("section", "pen"), split_axis=2, concat_axis=1, tiled=True)
    out_real, out_imag = complex_apply(
        "kz,czyj->ckyj",
        cosine_table,
        sine_table,
        block[..., :block_modes],
        block[..., block_modes:],
    )
    third_pass = jnp.concatenate([out_real, out_imag], axis=-1)
    group_index = lax.axis_index("section") * pens + lax.axis_index("pen")
    modes_z = signed_modes(jnp.arange(keep_count, dtype=jnp.int32), keep_count)[:, None, None]
    modes_y = signed_modes(
        group_index * rows_ky + jnp.arange(rows_ky, dtype=jnp.int32), keep_count
    )[None, :, None]
    modes_x = signed_modes(
        lax.axis_index("slab") * block_modes + jnp.arange(block_modes, dtype=jnp.int32), keep_count
    )[None, None, :]
    limit = -(keep_count // 2)
    keep_mask = ((modes_x != limit) & (modes_y != limit) & (modes_z != limit)).astype(jnp.float32)
    waves = (modes_x.astype(jnp.float32), modes_y.astype(jnp.float32), modes_z.astype(jnp.float32))
    ksq = waves[0] * waves[0] + waves[1] * waves[1] + waves[2] * waves[2]
    denom = jnp.maximum(ksq, 1.0)
    parts = []
    for which in range(2):
        chosen = third_pass[..., which * block_modes : (which + 1) * block_modes]
        comp = [chosen[c] for c in range(3)]
        inner = (waves[0] * comp[0] + waves[1] * comp[1] + waves[2] * comp[2]) / denom
        parts.append(jnp.stack([comp[c] - waves[c] * inner for c in range(3)]))
    projected = jnp.stack(parts, axis=3)
    visc = 0.5 / (keep_count // 2) ** 2
    return (
        projected * keep_mask[None, :, :, None, :]
        - visc * ksq[None, :, :, None, :] * velocity_modes
    )


def split_bf16(table):
    high = table.astype(jnp.bfloat16)
    low = (table - high.astype(np.float32)).astype(jnp.bfloat16)
    return high, low


def split_in_kernel(value):
    high = value.astype(jnp.bfloat16)
    low = (value - high.astype(jnp.float32)).astype(jnp.bfloat16)
    return high, low


def mm(a, b):
    return lax.dot_general(a, b, (((1,), (0,)), ((), ())), preferred_element_type=jnp.float32)


def split_dot(a, b):
    return mm(a[0], b[0]) + mm(a[1], b[0]) + mm(a[0], b[1])


def wave_numbers(count):
    index = np.arange(count)
    return np.where(index < count // 2, index, index - count)


def host_tables(cells, keep):
    phase = np.remainder(wave_numbers(keep)[:, None] * np.arange(cells)[None, :], cells)
    angles = 2.0 * np.pi / cells * phase
    factor = 1.0 / np.sqrt(cells)
    return np.cos(angles) * factor, np.sin(angles) * factor


def by_distance(devices):
    origin = getattr(devices.flat[0], "coords", ())

    def hops(index):
        return [abs(a - b) for a, b in zip(getattr(devices[index], "coords", ()), origin)]

    every = list(np.ndindex(devices.shape))
    spans = [max(far) for far in zip(*map(hops, every))]

    def key(index):
        far = hops(index)
        if sum(far) == 0:
            return -1, 0, index
        return (far[spans.index(max(spans))], -sum(far), index) if far else (0, 0, index)

    order = sorted(every, key=key)

    def greeting(index):
        far = sum(hops(index))
        return order.index(index) >= len(order) // 2, far == 0, -far, index

    return order, sorted(every, key=greeting)


class Plan:
    def __init__(self, mesh_shape, orders, cells, keep, z_rows, y_rows):
        self.order, self.greeted = orders
        self.cells, self.keep, self.z_rows, self.y_rows = cells, keep, z_rows, y_rows
        self.halves, self.pens, self.slabs = (mesh_shape[a] for a in AXES)
        self.groups = self.halves * self.pens
        self.count = self.groups * self.slabs
        self.rows_ky = keep // self.groups
        self.block = keep // self.slabs
        self.width = self.rows_ky * self.block
        self.rows = 2 * z_rows
        self.wide = self.slabs * 128

    def fits(self):
        return (
            self.rows_ky * self.groups == self.keep
            and self.block * self.slabs == self.keep
            and 3 * self.width <= 128
            and 128 % self.width == 0
            and self.rows <= 8
            and self.cells <= 128
            and self.cells % 16 == 0
            and self.y_rows % 8 == 0
            and 6 * self.y_rows <= 256
            and self.groups % 8 == 0
            and self.keep % 8 == 0
            and self.block % 8 == 0
            and 3 * self.z_rows * self.y_rows <= 512
            and 2 <= self.count <= 64
        )

    def tables(self):
        cos, sin = host_tables(self.cells, self.keep)
        g, zl = self.groups, self.z_rows
        table = np.zeros((2, self.keep, g, self.slabs, 8), np.float32)
        for z in range(zl):
            c, n = cos[:, z::zl][:, :, None], sin[:, z::zl][:, :, None]
            table[0, :, :, :, 2 * z], table[0, :, :, :, 2 * z + 1] = c, n
            table[1, :, :, :, 2 * z], table[1, :, :, :, 2 * z + 1] = -n, c
        early = table[:, :, : g - 1].reshape(2 * self.keep, (g - 1) * self.slabs * 8)
        last = table[:, :, g - 1, 0, : self.rows].reshape(2 * self.keep, self.rows).T
        last = np.broadcast_to(last[:, :, None], (*last.shape, 128))
        return np.stack(split_bf16(early)), np.ascontiguousarray(last)


def kernel(
    plan, vel_hbm, vort_hbm, modes_hbm, third_hbm, final_hbm, out_ref,
    fields, modes, first, second, third, near, final, cross, quick, send, recv,
    field_sem, late_sem, send_sem, recv_sem,
):
    sec, pen, slab = (lax.axis_index(a) for a in AXES)
    group = sec * plan.pens + pen
    me = group * plan.slabs + slab
    kind = group // (plan.groups - 1)
    is_last = kind == 1
    cells, keep = plan.cells, plan.keep
    for i, source in enumerate((vel_hbm, vort_hbm)):
        for c in range(3):
            pltpu.make_async_copy(source.at[c], fields.at[i, c], field_sem).start(priority=i)
    late_loads = [
        pltpu.make_async_copy(third_hbm, third, late_sem.at[0]),
        pltpu.make_async_copy(modes_hbm, modes, late_sem.at[1]),
        pltpu.make_async_copy(final_hbm, final, late_sem.at[2]),
    ]

    barrier = pltpu.get_barrier_semaphore()

    def signed(index):
        return jnp.where(index < keep // 2, index, index - keep)

    def place(to):
        return (to[0] * plan.pens + to[1]) * plan.slabs + to[2]

    for to in plan.greeted:

        @pl.when(me != place(to))
        def _(to=to):
            pl.semaphore_signal(
                barrier, inc=1, device_id=to, device_id_type=pl.DeviceIdType.MESH
            )

    if plan.rows < 8:
        recv[:, plan.rows : 8] = jnp.zeros((plan.count, 8 - plan.rows, 128), jnp.float32)
    cross[...] = jnp.zeros_like(cross)
    scale = 1.0 / math.sqrt(cells)

    def turn(wave, cell):
        product = wave * cell
        product = product - cells * jnp.floor(product * (1.0 / cells) + 0.5)
        angle = product * (2.0 * math.pi / cells)
        return jnp.cos(angle) * scale, jnp.sin(angle) * scale

    def ramp(shape, axis):
        return lax.broadcasted_iota(jnp.int32, shape, axis)

    kept = plan.order[0][0] * plan.pens + plan.order[0][1]
    line = (ramp((plan.y_rows, 128), 0) + slab * plan.y_rows).astype(jnp.float32)
    waves_near = [float(wave_numbers(keep)[kept * plan.rows_ky + i]) for i in range(plan.rows_ky)]
    for i in range(plan.rows_ky):
        if waves_near[i] != 0:
            near[i, 0], near[i, 1] = turn(waves_near[i], line)
    lane = ramp((cells, 128), 1)
    line = ramp((cells, 128), 0).astype(jnp.float32)
    for s in range(plan.slabs):
        wave = signed(lane % plan.block + s * plan.block).astype(jnp.float32)
        cosine, sine = turn(wave, line)
        for k, table in enumerate((cosine, -sine)):
            table = split_in_kernel(jnp.where(lane < 3 * plan.width, table, 0.0))
            start = k * plan.wide + s * 128
            for i in range(2):
                first[i, 0:cells, start : start + 128] = table[i]
    shape = (keep, 6 * plan.y_rows)
    row = ramp(shape, 0)
    wave = signed(row % plan.groups * plan.rows_ky + row // plan.groups).astype(jnp.float32)
    line = ramp(shape, 1).astype(jnp.float32)
    part = jnp.floor((line + 0.5) * (1.0 / plan.y_rows))
    line = line - part * plan.y_rows
    cosine, sine = turn(wave, line + (slab * plan.y_rows).astype(jnp.float32))
    real = (part == 0) | (part == 2) | (part == 4)
    for k, table in enumerate((jnp.where(real, cosine, sine), jnp.where(real, -sine, cosine))):
        table_high = table.astype(jnp.bfloat16).astype(jnp.float32)
        table = jnp.where(part < 4, table_high, table - table_high)
        second[k * keep : (k + 1) * keep] = table.astype(jnp.bfloat16)
    if cells < 128:
        for i in range(2):
            first[i, cells:128] = jnp.zeros((128 - cells, first.shape[2]), jnp.bfloat16)

    pltpu.make_async_copy(fields, fields, field_sem).wait()
    zl, yl = plan.z_rows, plan.y_rows
    area = zl * yl
    v, w = ([fields[i, c].reshape(area, cells) for c in range(3)] for i in range(2))
    for c in range(3):
        p, q = (c + 1) % 3, (c + 2) % 3
        cross[c * area : (c + 1) * area, 0:cells] = v[p] * w[q] - v[q] * w[p]
    sub = lax.broadcasted_iota(jnp.int32, (8, 128), 0)

    def folded(terms):
        part = terms[0:8]
        for r in range(8, yl, 8):
            part = part + terms[r : r + 8]
        return part

    blocks = []
    for i in range(plan.rows_ky):
        for c in range(3):
            sums = []
            for z in range(zl):
                start = (c * zl + z) * yl
                line = cross[start : start + yl]
                if waves_near[i] == 0:
                    part = folded(line)
                    part = part + pltpu.roll(part, 4, 0)
                else:
                    pair = [folded(line * near[i, k]) for k in range(2)]
                    part = jnp.where(sub < 4, pair[0], pair[1]) + pltpu.roll(
                        jnp.where(sub < 4, pair[1], pair[0]), 4, 0
                    )
                sums.append(part + pltpu.roll(part, 2 if z // 2 % 2 else 6, 0))
            even, odd = None, None
            for z in range(0, zl, 2):
                even = sums[z] if even is None else jnp.where(sub % 4 < 2, even, sums[z])
            for z in range(1, zl, 2):
                odd = sums[z] if odd is None else jnp.where(sub % 4 < 2, odd, sums[z])
            block = even + pltpu.roll(even, 7, 0)
            if odd is not None:
                block = jnp.where(sub % 2 == 0, block, odd + pltpu.roll(odd, 1, 0))
            if waves_near[i] == 0:
                block = jnp.where(sub < 4, block * scale, 0.0)
            blocks.append(block)
    high, low = split_in_kernel(jnp.concatenate(blocks, axis=0))
    planes = mm(
        jnp.concatenate([high, low, high], axis=1),
        jnp.concatenate([first[0], first[0], first[1]], axis=0),
    )
    cell = lax.broadcasted_iota(jnp.int32, (8, 2 * plan.wide), 1) % 128 // plan.block
    total = planes[0:8]
    for i in range(plan.rows_ky):
        for c in range(3):
            start = (i * 3 + c) * 8
            total = jnp.where(cell == c * plan.rows_ky + i, planes[start : start + 8], total)
    real, imag = total[:, : plan.wide], total[:, plan.wide :]
    parts = (real + pltpu.roll(imag, 4, 0), imag - pltpu.roll(real, 4, 0))
    for k in range(2):
        for s in range(plan.slabs):
            quick[pl.ds(s * 8 + k, zl, stride=2), :] = parts[k][0:zl, s * 128 : (s + 1) * 128]

    used = pl.ds(0, plan.rows)

    def slot_of(s, g):
        return (s * plan.groups + g) * 8

    def open_with_near():
        pl.semaphore_wait(barrier, plan.count - 1)
        for s in range(plan.slabs):
            to = (*plan.order[0][:2], s)

            @pl.when(me != place(to))
            def _(to=to):
                pltpu.make_async_remote_copy(
                    src_ref=quick.at[pl.ds(to[2] * 8, plan.rows)],
                    dst_ref=recv.at[me, used],
                    send_sem=send_sem,
                    recv_sem=recv_sem.at[kind],
                    device_id=to,
                    device_id_type=pl.DeviceIdType.MESH,
                ).start()

    @pl.when(is_last)
    def _():
        open_with_near()

    high, low = split_in_kernel(cross[...])
    along_x = mm(
        jnp.concatenate([high, low], axis=1), jnp.concatenate([first[0], first[0]], axis=0)
    ) + mm(high, first[1])
    slot = lax.broadcasted_iota(jnp.int32, (area, 2 * plan.wide), 1) % 128 // plan.width
    along_x = [along_x[c * area : (c + 1) * area] for c in range(3)]
    along_x = jnp.where(slot == 0, along_x[0], jnp.where(slot == 1, along_x[1], along_x[2]))
    high = along_x.astype(jnp.bfloat16).astype(jnp.float32)
    low = along_x - high
    upper = lax.broadcasted_iota(jnp.int32, (plan.groups, plan.wide), 1) % plan.width // plan.block
    for z in range(zl):
        parts = []
        for part in (high, low):
            piece = part[z * yl : (z + 1) * yl]
            parts.append(
                jnp.concatenate([piece[:, : plan.wide], piece[:, plan.wide :]], axis=0)
            )
        stack = jnp.concatenate([parts[0], parts[1], parts[0]], axis=0).astype(jnp.bfloat16)
        planes = mm(second[...], stack)
        for k in range(2):
            total = None
            for i in range(plan.rows_ky):
                start = (k * plan.rows_ky + i) * plan.groups
                piece = planes[start : start + plan.groups]
                total = piece if total is None else jnp.where(upper == i, piece, total)
            for s in range(plan.slabs):
                rows = pl.ds(s * plan.groups * 8 + 2 * z + k, plan.groups, stride=8)
                send[rows, :] = total[:, s * 128 : (s + 1) * 128]

    for load in late_loads:
        load.start()

    @pl.when(jnp.logical_not(is_last))
    def _():
        open_with_near()

    for to in plan.order[plan.slabs :]:

        @pl.when(me != place(to))
        def _(to=to):
            pltpu.make_async_remote_copy(
                src_ref=send.at[pl.ds(slot_of(to[2], to[0] * plan.pens + to[1]), plan.rows)],
                dst_ref=recv.at[me, used],
                send_sem=send_sem,
                recv_sem=recv_sem.at[kind],
                device_id=to,
                device_id_type=pl.DeviceIdType.MESH,
            ).start()

    own = pl.multiple_of(slot_of(slab, group), 8)
    recv[me, 0 : plan.rows] = send[pl.ds(own, plan.rows)]

    bm, ky_n, width = plan.block, plan.rows_ky, plan.width

    row = lax.broadcasted_iota(jnp.int32, (width, keep), 0)
    kx = signed(row % bm + slab * bm)
    ky = signed(row // bm + group * ky_n)
    kz = signed(lax.broadcasted_iota(jnp.int32, (width, keep), 1))
    limit = -(keep // 2)
    mask = ((kx != limit) & (ky != limit) & (kz != limit)).astype(jnp.float32)
    waves = [k.astype(jnp.float32) for k in (kx, ky, kz)]
    ksq = waves[0] * waves[0] + waves[1] * waves[1] + waves[2] * waves[2]
    inverse = 1.0 / jnp.maximum(ksq, 1.0)
    damp = (0.5 / (keep // 2) ** 2) * ksq
    for load in late_loads:
        load.wait()
    damped = [
        [
            jnp.concatenate([modes[c, i, k] for i in range(ky_n)], axis=0) * damp
            for k in range(2)
        ]
        for c in range(3)
    ]

    def landed(messages, sem):
        part = recv.at[pl.ds(0, messages), used]
        pltpu.make_async_copy(part, part, sem).wait()

    early = plan.count - plan.slabs

    @pl.when(is_last)
    def _():
        landed(early, recv_sem.at[0])

    @pl.when(jnp.logical_not(is_last))
    def _():
        landed(early - 1, recv_sem.at[0])

    got = split_in_kernel(recv[0:early].reshape(early * 8, 128))
    out = mm(third[0], jnp.concatenate(got, axis=1))
    out = out[:, :128] + out[:, 128:] + mm(third[1], got[0])

    @pl.when(is_last)
    def _():
        if plan.slabs > 1:
            landed(plan.slabs - 1, recv_sem.at[1])

    @pl.when(jnp.logical_not(is_last))
    def _():
        landed(plan.slabs, recv_sem.at[1])

    tail = recv[early]
    for s in range(1, plan.slabs):
        tail = tail + recv[early + s]
    for r in range(plan.rows):
        out = out + final[r] * tail[r : r + 1]
    for k in range(2):
        turned = jnp.transpose(out[k * keep : (k + 1) * keep])
        comp = [turned[c * width : (c + 1) * width] for c in range(3)]
        inner = (waves[0] * comp[0] + waves[1] * comp[1] + waves[2] * comp[2]) * inverse
        for c in range(3):
            result = (comp[c] - waves[c] * inner) * mask - damped[c][k]
            for i in range(ky_n):
                out_ref[c, i, k] = result[i * bm : (i + 1) * bm]
    landed(plan.count - 1, send_sem)


def direct(plan, tables, velocity, vorticity, velocity_modes):
    modes = jnp.transpose(velocity_modes, (0, 2, 3, 4, 1))
    third, final = tables
    hbm = pl.BlockSpec(memory_space=pltpu.HBM)
    out = pl.pallas_call(
        functools.partial(kernel, plan),
        out_shape=pltpu.VMEM(modes.shape, jnp.float32),
        in_specs=[hbm] * 5,
        out_specs=pl.BlockSpec(memory_space=pltpu.VMEM),
        scratch_shapes=[
            pltpu.VMEM((2,) + velocity.shape, jnp.float32),
            pltpu.VMEM(modes.shape, jnp.float32),
            pltpu.VMEM((2, 128, 2 * plan.wide), jnp.bfloat16),
            pltpu.VMEM((2 * plan.keep, 6 * plan.y_rows), jnp.bfloat16),
            pltpu.VMEM(third.shape, jnp.bfloat16),
            pltpu.VMEM((plan.rows_ky, 2, plan.y_rows, 128), jnp.float32),
            pltpu.VMEM(final.shape, jnp.float32),
            pltpu.VMEM((3 * plan.z_rows * plan.y_rows, 128), jnp.float32),
            pltpu.VMEM((plan.slabs * 8, 128), jnp.float32),
            pltpu.VMEM((plan.slabs * plan.groups * 8, 128), jnp.float32),
            pltpu.VMEM((plan.count, 8, 128), jnp.float32),
            pltpu.SemaphoreType.DMA,
            pltpu.SemaphoreType.DMA((3,)),
            pltpu.SemaphoreType.DMA,
            pltpu.SemaphoreType.DMA((2,)),
        ],
        compiler_params=pltpu.CompilerParams(collective_id=0, has_side_effects=True),
    )(velocity, vorticity, modes, third, final)
    return jnp.transpose(out, (0, 4, 1, 2, 3))


def solution(mesh):
    sizes = dict(mesh.shape)
    orders = by_distance(mesh.devices)

    def run(velocity, vorticity, velocity_modes):
        _, z_rows, y_rows, cells = velocity.shape
        plan = Plan(sizes, orders, cells, velocity_modes.shape[1], z_rows, y_rows)
        if not plan.fits():
            return per_device(velocity, vorticity, velocity_modes)
        return direct(plan, plan.tables(), velocity, vorticity, velocity_modes)

    return jax.shard_map(
        run,
        mesh=mesh,
        in_specs=(
            P(None, ("section", "pen"), "slab", None),
            P(None, ("section", "pen"), "slab", None),
            P(None, None, ("section", "pen"), None, "slab"),
        ),
        out_specs=P(None, None, ("section", "pen"), None, "slab"),
        check_vma=False,
    )
```

```python
import functools
import math

import jax
import jax.numpy as jnp
import numpy as np
from jax import lax
from jax.experimental import pallas as pl
from jax.experimental.pallas import tpu as pltpu
from jax.sharding import PartitionSpec as P

AXES = ("section", "pen", "slab")
highest = lax.Precision.HIGHEST


def signed_modes(index, count):
    return jnp.where(index < count // 2, index, index - count)


def discrete_fourier_tables(length, keep_count):
    modes = signed_modes(jnp.arange(keep_count, dtype=jnp.int32), keep_count)
    mode_positions = jnp.arange(length, dtype=jnp.int32)
    phase = jnp.remainder(modes[:, None] * mode_positions[None, :], length).astype(jnp.float32)
    angles = 2.0 * math.pi / length * phase
    factor = 1.0 / math.sqrt(length)
    return (jnp.cos(angles) * factor, jnp.sin(angles) * factor)


def complex_apply(form, cosine, sine, real_part, imag_part):
    out_real = jnp.einsum(form, cosine, real_part, precision=highest) + jnp.einsum(
        form, sine, imag_part, precision=highest
    )
    out_imag = jnp.einsum(form, cosine, imag_part, precision=highest) - jnp.einsum(
        form, sine, real_part, precision=highest
    )
    return (out_real, out_imag)


def per_device(velocity, vorticity, velocity_modes):
    grid_cells = velocity.shape[3]
    keep_count = velocity_modes.shape[1]
    cross_product = jnp.stack(
        [
            velocity[1] * vorticity[2] - velocity[2] * vorticity[1],
            velocity[2] * vorticity[0] - velocity[0] * vorticity[2],
            velocity[0] * vorticity[1] - velocity[1] * vorticity[0],
        ]
    )
    slabs = lax.axis_size("slab")
    block_modes = keep_count // slabs
    cosine_table, sine_table = discrete_fourier_tables(grid_cells, keep_count)
    cols_real = cosine_table.T.reshape(grid_cells, slabs, block_modes)
    cols_imag = (-sine_table).T.reshape(grid_cells, slabs, block_modes)
    column_table = jnp.stack([cols_real, cols_imag], axis=2).reshape(grid_cells, 2 * keep_count)
    first_pass = jnp.einsum("czyx,xj->czyj", cross_product, column_table, precision=highest)
    block = lax.all_to_all(first_pass, "slab", split_axis=3, concat_axis=2, tiled=True)
    out_real, out_imag = complex_apply(
        "ky,czyj->czkj",
        cosine_table,
        sine_table,
        block[..., :block_modes],
        block[..., block_modes:],
    )
    second_pass = jnp.concatenate([out_real, out_imag], axis=-1)
    halves = lax.axis_size("section")
    pens = lax.axis_size("pen")
    rows_ky = keep_count // (halves * pens)
    block = lax.all_to_all(second_pass, ("section", "pen"), split_axis=2, concat_axis=1, tiled=True)
    out_real, out_imag = complex_apply(
        "kz,czyj->ckyj",
        cosine_table,
        sine_table,
        block[..., :block_modes],
        block[..., block_modes:],
    )
    third_pass = jnp.concatenate([out_real, out_imag], axis=-1)
    group_index = lax.axis_index("section") * pens + lax.axis_index("pen")
    modes_z = signed_modes(jnp.arange(keep_count, dtype=jnp.int32), keep_count)[:, None, None]
    modes_y = signed_modes(
        group_index * rows_ky + jnp.arange(rows_ky, dtype=jnp.int32), keep_count
    )[None, :, None]
    modes_x = signed_modes(
        lax.axis_index("slab") * block_modes + jnp.arange(block_modes, dtype=jnp.int32), keep_count
    )[None, None, :]
    limit = -(keep_count // 2)
    keep_mask = ((modes_x != limit) & (modes_y != limit) & (modes_z != limit)).astype(jnp.float32)
    waves = (modes_x.astype(jnp.float32), modes_y.astype(jnp.float32), modes_z.astype(jnp.float32))
    ksq = waves[0] * waves[0] + waves[1] * waves[1] + waves[2] * waves[2]
    denom = jnp.maximum(ksq, 1.0)
    parts = []
    for which in range(2):
        chosen = third_pass[..., which * block_modes : (which + 1) * block_modes]
        comp = [chosen[c] for c in range(3)]
        inner = (waves[0] * comp[0] + waves[1] * comp[1] + waves[2] * comp[2]) / denom
        parts.append(jnp.stack([comp[c] - waves[c] * inner for c in range(3)]))
    projected = jnp.stack(parts, axis=3)
    visc = 0.5 / (keep_count // 2) ** 2
    return (
        projected * keep_mask[None, :, :, None, :]
        - visc * ksq[None, :, :, None, :] * velocity_modes
    )


def split_bf16(table):
    high = table.astype(jnp.bfloat16)
    low = (table - high.astype(np.float32)).astype(jnp.bfloat16)
    return high, low


def split_in_kernel(value):
    high = value.astype(jnp.bfloat16)
    low = (value - high.astype(jnp.float32)).astype(jnp.bfloat16)
    return high, low


def mm(a, b):
    return lax.dot_general(a, b, (((1,), (0,)), ((), ())), preferred_element_type=jnp.float32)


def split_dot(a, b):
    return mm(a[0], b[0]) + mm(a[1], b[0]) + mm(a[0], b[1])


def wave_numbers(count):
    index = np.arange(count)
    return np.where(index < count // 2, index, index - count)


def host_tables(cells, keep):
    phase = np.remainder(wave_numbers(keep)[:, None] * np.arange(cells)[None, :], cells)
    angles = 2.0 * np.pi / cells * phase
    factor = 1.0 / np.sqrt(cells)
    return np.cos(angles) * factor, np.sin(angles) * factor


def by_distance(devices):
    origin = getattr(devices.flat[0], "coords", ())

    def hops(index):
        return [abs(a - b) for a, b in zip(getattr(devices[index], "coords", ()), origin)]

    every = list(np.ndindex(devices.shape))
    spans = [max(far) for far in zip(*map(hops, every))]

    def key(index):
        far = hops(index)
        if sum(far) == 0:
            return -1, 0, index
        return (far[spans.index(max(spans))], -sum(far), index) if far else (0, 0, index)

    order = sorted(every, key=key)

    def greeting(index):
        far = sum(hops(index))
        return order.index(index) >= len(order) // 2, far == 0, -far, index

    return order, sorted(every, key=greeting)


class Plan:
    def __init__(self, mesh_shape, orders, cells, keep, z_rows, y_rows):
        self.order, self.greeted = orders
        self.cells, self.keep, self.z_rows, self.y_rows = cells, keep, z_rows, y_rows
        self.halves, self.pens, self.slabs = (mesh_shape[a] for a in AXES)
        self.groups = self.halves * self.pens
        self.count = self.groups * self.slabs
        self.rows_ky = keep // self.groups
        self.block = keep // self.slabs
        self.width = self.rows_ky * self.block
        self.rows = 2 * z_rows
        self.wide = self.slabs * 128

    def fits(self):
        return (
            self.rows_ky * self.groups == self.keep
            and self.block * self.slabs == self.keep
            and 3 * self.width <= 128
            and 128 % self.width == 0
            and self.rows <= 8
            and self.cells <= 128
            and self.cells % 16 == 0
            and self.y_rows % 8 == 0
            and 6 * self.y_rows <= 256
            and self.groups % 8 == 0
            and self.keep % 8 == 0
            and self.block % 8 == 0
            and 3 * self.z_rows * self.y_rows <= 512
            and 2 <= self.count <= 64
        )

    def tables(self):
        cos, sin = host_tables(self.cells, self.keep)
        g, zl = self.groups, self.z_rows
        table = np.zeros((2, self.keep, g, self.slabs, 8), np.float32)
        for z in range(zl):
            c, n = cos[:, z::zl][:, :, None], sin[:, z::zl][:, :, None]
            table[0, :, :, :, 2 * z], table[0, :, :, :, 2 * z + 1] = c, n
            table[1, :, :, :, 2 * z], table[1, :, :, :, 2 * z + 1] = -n, c
        early = table[:, :, : g - 1].reshape(2 * self.keep, (g - 1) * self.slabs * 8)
        last = table[:, :, g - 1, 0, : self.rows].reshape(2 * self.keep, self.rows).T
        last = np.broadcast_to(last[:, :, None], (*last.shape, 128))
        return np.stack(split_bf16(early)), np.ascontiguousarray(last)


def kernel(
    plan, vel_hbm, vort_hbm, modes_hbm, third_hbm, final_hbm, out_ref,
    fields, modes, first, second, third, near, final, cross, quick, send, recv,
    field_sem, late_sem, send_sem, recv_sem,
):
    sec, pen, slab = (lax.axis_index(a) for a in AXES)
    group = sec * plan.pens + pen
    me = group * plan.slabs + slab
    kind = group // (plan.groups - 1)
    is_last = kind == 1
    cells, keep = plan.cells, plan.keep
    for i, source in enumerate((vel_hbm, vort_hbm)):
        for c in range(3):
            pltpu.make_async_copy(source.at[c], fields.at[i, c], field_sem).start(priority=i)
    late_loads = [
        pltpu.make_async_copy(third_hbm, third, late_sem.at[0]),
        pltpu.make_async_copy(modes_hbm, modes, late_sem.at[1]),
        pltpu.make_async_copy(final_hbm, final, late_sem.at[2]),
    ]

    barrier = pltpu.get_barrier_semaphore()

    def signed(index):
        return jnp.where(index < keep // 2, index, index - keep)

    def place(to):
        return (to[0] * plan.pens + to[1]) * plan.slabs + to[2]

    for to in plan.greeted:

        @pl.when(me != place(to))
        def _(to=to):
            pl.semaphore_signal(
                barrier, inc=1, device_id=to, device_id_type=pl.DeviceIdType.MESH
            )

    if plan.rows < 8:
        recv[:, plan.rows : 8] = jnp.zeros((plan.count, 8 - plan.rows, 128), jnp.float32)
    cross[...] = jnp.zeros_like(cross)
    scale = 1.0 / math.sqrt(cells)

    def turn(wave, cell):
        product = wave * cell
        product = product - cells * jnp.floor(product * (1.0 / cells) + 0.5)
        angle = product * (2.0 * math.pi / cells)
        return jnp.cos(angle) * scale, jnp.sin(angle) * scale

    def ramp(shape, axis):
        return lax.broadcasted_iota(jnp.int32, shape, axis)

    kept = plan.order[0][0] * plan.pens + plan.order[0][1]
    line = (ramp((plan.y_rows, 128), 0) + slab * plan.y_rows).astype(jnp.float32)
    waves_near = [float(wave_numbers(keep)[kept * plan.rows_ky + i]) for i in range(plan.rows_ky)]
    for i in range(plan.rows_ky):
        if waves_near[i] != 0:
            near[i, 0], near[i, 1] = turn(waves_near[i], line)
    lane = ramp((cells, 128), 1)
    line = ramp((cells, 128), 0).astype(jnp.float32)
    for s in range(plan.slabs):
        wave = signed(lane % plan.block + s * plan.block).astype(jnp.float32)
        cosine, sine = turn(wave, line)
        for k, table in enumerate((cosine, -sine)):
            table = split_in_kernel(jnp.where(lane < 3 * plan.width, table, 0.0))
            start = k * plan.wide + s * 128
            for i in range(2):
                first[i, 0:cells, start : start + 128] = table[i]
    shape = (keep, 6 * plan.y_rows)
    row = ramp(shape, 0)
    wave = signed(row % plan.groups * plan.rows_ky + row // plan.groups).astype(jnp.float32)
    line = ramp(shape, 1).astype(jnp.float32)
    part = jnp.floor((line + 0.5) * (1.0 / plan.y_rows))
    line = line - part * plan.y_rows
    cosine, sine = turn(wave, line + (slab * plan.y_rows).astype(jnp.float32))
    real = (part == 0) | (part == 2) | (part == 4)
    for k, table in enumerate((jnp.where(real, cosine, sine), jnp.where(real, -sine, cosine))):
        table_high = table.astype(jnp.bfloat16).astype(jnp.float32)
        table = jnp.where(part < 4, table_high, table - table_high)
        second[k * keep : (k + 1) * keep] = table.astype(jnp.bfloat16)
    if cells < 128:
        for i in range(2):
            first[i, cells:128] = jnp.zeros((128 - cells, first.shape[2]), jnp.bfloat16)

    pltpu.make_async_copy(fields, fields, field_sem).wait()
    zl, yl = plan.z_rows, plan.y_rows
    area = zl * yl
    v, w = ([fields[i, c].reshape(area, cells) for c in range(3)] for i in range(2))
    for c in range(3):
        p, q = (c + 1) % 3, (c + 2) % 3
        cross[c * area : (c + 1) * area, 0:cells] = v[p] * w[q] - v[q] * w[p]
    sub = lax.broadcasted_iota(jnp.int32, (8, 128), 0)

    def folded(terms):
        part = terms[0:8]
        for r in range(8, yl, 8):
            part = part + terms[r : r + 8]
        return part

    blocks = []
    for i in range(plan.rows_ky):
        for c in range(3):
            sums = []
            for z in range(zl):
                start = (c * zl + z) * yl
                line = cross[start : start + yl]
                if waves_near[i] == 0:
                    part = folded(line)
                    part = part + pltpu.roll(part, 4, 0)
                else:
                    pair = [folded(line * near[i, k]) for k in range(2)]
                    part = jnp.where(sub < 4, pair[0], pair[1]) + pltpu.roll(
                        jnp.where(sub < 4, pair[1], pair[0]), 4, 0
                    )
                sums.append(part + pltpu.roll(part, 2 if z // 2 % 2 else 6, 0))
            even, odd = None, None
            for z in range(0, zl, 2):
                even = sums[z] if even is None else jnp.where(sub % 4 < 2, even, sums[z])
            for z in range(1, zl, 2):
                odd = sums[z] if odd is None else jnp.where(sub % 4 < 2, odd, sums[z])
            block = even + pltpu.roll(even, 7, 0)
            if odd is not None:
                block = jnp.where(sub % 2 == 0, block, odd + pltpu.roll(odd, 1, 0))
            if waves_near[i] == 0:
                block = jnp.where(sub < 4, block * scale, 0.0)
            blocks.append(block)
    high, low = split_in_kernel(jnp.concatenate(blocks, axis=0))
    planes = mm(
        jnp.concatenate([high, low, high], axis=1),
        jnp.concatenate([first[0], first[0], first[1]], axis=0),
    )
    cell = lax.broadcasted_iota(jnp.int32, (8, 2 * plan.wide), 1) % 128 // plan.block
    total = planes[0:8]
    for i in range(plan.rows_ky):
        for c in range(3):
            start = (i * 3 + c) * 8
            total = jnp.where(cell == c * plan.rows_ky + i, planes[start : start + 8], total)
    real, imag = total[:, : plan.wide], total[:, plan.wide :]
    parts = (real + pltpu.roll(imag, 4, 0), imag - pltpu.roll(real, 4, 0))
    for k in range(2):
        for s in range(plan.slabs):
            quick[pl.ds(s * 8 + k, zl, stride=2), :] = parts[k][0:zl, s * 128 : (s + 1) * 128]

    used = pl.ds(0, plan.rows)

    def slot_of(s, g):
        return (s * plan.groups + g) * 8

    def open_with_near():
        pl.semaphore_wait(barrier, plan.count - 1)
        for s in range(plan.slabs):
            to = (*plan.order[0][:2], s)

            @pl.when(me != place(to))
            def _(to=to):
                pltpu.make_async_remote_copy(
                    src_ref=quick.at[pl.ds(to[2] * 8, plan.rows)],
                    dst_ref=recv.at[me, used],
                    send_sem=send_sem,
                    recv_sem=recv_sem.at[kind],
                    device_id=to,
                    device_id_type=pl.DeviceIdType.MESH,
                ).start()

    @pl.when(is_last)
    def _():
        open_with_near()

    high, low = split_in_kernel(cross[...])
    along_x = mm(
        jnp.concatenate([high, low], axis=1), jnp.concatenate([first[0], first[0]], axis=0)
    ) + mm(high, first[1])
    slot = lax.broadcasted_iota(jnp.int32, (area, 2 * plan.wide), 1) % 128 // plan.width
    along_x = [along_x[c * area : (c + 1) * area] for c in range(3)]
    along_x = jnp.where(slot == 0, along_x[0], jnp.where(slot == 1, along_x[1], along_x[2]))
    high = along_x.astype(jnp.bfloat16).astype(jnp.float32)
    low = along_x - high
    upper = lax.broadcasted_iota(jnp.int32, (plan.groups, plan.wide), 1) % plan.width // plan.block
    for z in range(zl):
        parts = []
        for part in (high, low):
            piece = part[z * yl : (z + 1) * yl]
            parts.append(
                jnp.concatenate([piece[:, : plan.wide], piece[:, plan.wide :]], axis=0)
            )
        stack = jnp.concatenate([parts[0], parts[1], parts[0]], axis=0).astype(jnp.bfloat16)
        planes = mm(second[...], stack)
        for k in range(2):
            total = None
            for i in range(plan.rows_ky):
                start = (k * plan.rows_ky + i) * plan.groups
                piece = planes[start : start + plan.groups]
                total = piece if total is None else jnp.where(upper == i, piece, total)
            for s in range(plan.slabs):
                rows = pl.ds(s * plan.groups * 8 + 2 * z + k, plan.groups, stride=8)
                send[rows, :] = total[:, s * 128 : (s + 1) * 128]

    for load in late_loads:
        load.start(priority=1)

    @pl.when(jnp.logical_not(is_last))
    def _():
        open_with_near()

    for to in plan.order[plan.slabs :]:

        @pl.when(me != place(to))
        def _(to=to):
            pltpu.make_async_remote_copy(
                src_ref=send.at[pl.ds(slot_of(to[2], to[0] * plan.pens + to[1]), plan.rows)],
                dst_ref=recv.at[me, used],
                send_sem=send_sem,
                recv_sem=recv_sem.at[kind],
                device_id=to,
                device_id_type=pl.DeviceIdType.MESH,
            ).start()

    own = pl.multiple_of(slot_of(slab, group), 8)
    recv[me, 0 : plan.rows] = send[pl.ds(own, plan.rows)]

    bm, ky_n, width = plan.block, plan.rows_ky, plan.width

    row = lax.broadcasted_iota(jnp.int32, (width, keep), 0)
    kx = signed(row % bm + slab * bm)
    ky = signed(row // bm + group * ky_n)
    kz = signed(lax.broadcasted_iota(jnp.int32, (width, keep), 1))
    limit = -(keep // 2)
    mask = ((kx != limit) & (ky != limit) & (kz != limit)).astype(jnp.float32)
    waves = [k.astype(jnp.float32) for k in (kx, ky, kz)]
    ksq = waves[0] * waves[0] + waves[1] * waves[1] + waves[2] * waves[2]
    inverse = 1.0 / jnp.maximum(ksq, 1.0)
    damp = (0.5 / (keep // 2) ** 2) * ksq
    for load in late_loads:
        load.wait()
    damped = [
        [
            jnp.concatenate([modes[c, i, k] for i in range(ky_n)], axis=0) * damp
            for k in range(2)
        ]
        for c in range(3)
    ]

    def landed(messages, sem):
        part = recv.at[pl.ds(0, messages), used]
        pltpu.make_async_copy(part, part, sem).wait()

    early = plan.count - plan.slabs

    @pl.when(is_last)
    def _():
        landed(early, recv_sem.at[0])

    @pl.when(jnp.logical_not(is_last))
    def _():
        landed(early - 1, recv_sem.at[0])

    got = split_in_kernel(recv[0:early].reshape(early * 8, 128))
    out = mm(third[0], jnp.concatenate(got, axis=1))
    out = out[:, :128] + out[:, 128:] + mm(third[1], got[0])

    @pl.when(is_last)
    def _():
        if plan.slabs > 1:
            landed(plan.slabs - 1, recv_sem.at[1])

    @pl.when(jnp.logical_not(is_last))
    def _():
        landed(plan.slabs, recv_sem.at[1])

    tail = recv[early]
    for s in range(1, plan.slabs):
        tail = tail + recv[early + s]
    for r in range(plan.rows):
        out = out + final[r] * tail[r : r + 1]
    for k in range(2):
        turned = jnp.transpose(out[k * keep : (k + 1) * keep])
        comp = [turned[c * width : (c + 1) * width] for c in range(3)]
        inner = (waves[0] * comp[0] + waves[1] * comp[1] + waves[2] * comp[2]) * inverse
        for c in range(3):
            result = (comp[c] - waves[c] * inner) * mask - damped[c][k]
            for i in range(ky_n):
                out_ref[c, i, k] = result[i * bm : (i + 1) * bm]
    landed(plan.count - 1, send_sem)


def direct(plan, tables, velocity, vorticity, velocity_modes):
    modes = jnp.transpose(velocity_modes, (0, 2, 3, 4, 1))
    third, final = tables
    hbm = pl.BlockSpec(memory_space=pltpu.HBM)
    out = pl.pallas_call(
        functools.partial(kernel, plan),
        out_shape=pltpu.VMEM(modes.shape, jnp.float32),
        in_specs=[hbm] * 5,
        out_specs=pl.BlockSpec(memory_space=pltpu.VMEM),
        scratch_shapes=[
            pltpu.VMEM((2,) + velocity.shape, jnp.float32),
            pltpu.VMEM(modes.shape, jnp.float32),
            pltpu.VMEM((2, 128, 2 * plan.wide), jnp.bfloat16),
            pltpu.VMEM((2 * plan.keep, 6 * plan.y_rows), jnp.bfloat16),
            pltpu.VMEM(third.shape, jnp.bfloat16),
            pltpu.VMEM((plan.rows_ky, 2, plan.y_rows, 128), jnp.float32),
            pltpu.VMEM(final.shape, jnp.float32),
            pltpu.VMEM((3 * plan.z_rows * plan.y_rows, 128), jnp.float32),
            pltpu.VMEM((plan.slabs * 8, 128), jnp.float32),
            pltpu.VMEM((plan.slabs * plan.groups * 8, 128), jnp.float32),
            pltpu.VMEM((plan.count, 8, 128), jnp.float32),
            pltpu.SemaphoreType.DMA,
            pltpu.SemaphoreType.DMA((3,)),
            pltpu.SemaphoreType.DMA,
            pltpu.SemaphoreType.DMA((2,)),
        ],
        compiler_params=pltpu.CompilerParams(collective_id=0, has_side_effects=True),
    )(velocity, vorticity, modes, third, final)
    return jnp.transpose(out, (0, 4, 1, 2, 3))


def solution(mesh):
    sizes = dict(mesh.shape)
    orders = by_distance(mesh.devices)

    def run(velocity, vorticity, velocity_modes):
        _, z_rows, y_rows, cells = velocity.shape
        plan = Plan(sizes, orders, cells, velocity_modes.shape[1], z_rows, y_rows)
        if not plan.fits():
            return per_device(velocity, vorticity, velocity_modes)
        return direct(plan, plan.tables(), velocity, vorticity, velocity_modes)

    return jax.shard_map(
        run,
        mesh=mesh,
        in_specs=(
            P(None, ("section", "pen"), "slab", None),
            P(None, ("section", "pen"), "slab", None),
            P(None, None, ("section", "pen"), None, "slab"),
        ),
        out_specs=P(None, None, ("section", "pen"), None, "slab"),
        check_vma=False,
    )
```
